8 devices in a mesh: dp: 2 (over z, y), tp: 4 (over x, core).
Axes of the slice: x: 2, y: 2, z: 1, core: 2. Of those that a mesh axis runs over, the one named last changes fastest.
Arguments:
- x_in: bfloat16 [1024, 1536], P('dp'), parts along dimension 0
- tok_pos: int32 [1024], P('dp'), parts along dimension 0
- self_k: bfloat16 [1024, 128, 16, 64], P('dp', None, 'tp'), parts along dimension 0
- self_v: bfloat16 [1024, 128, 16, 64], P('dp', None, 'tp'), parts along dimension 0
- cross_k: bfloat16 [1024, 64, 16, 64], P('dp', None, 'tp'), parts along dimension 0
- cross_v: bfloat16 [1024, 64, 16, 64], P('dp', None, 'tp'), parts along dimension 0
- enc_mask: int32 [1024, 64], P('dp'), parts along dimension 0
- rel_bias: float32 [32, 16], P(None, 'tp')
- w_q: bfloat16 [1536, 1024], P(None, 'tp')
- w_k: bfloat16 [1536, 1024], P(None, 'tp')
- w_v: bfloat16 [1536, 1024], P(None, 'tp')
- w_o: bfloat16 [1024, 1536], P('tp')
- cross_q: bfloat16 [1536, 1024], P(None, 'tp')
- cross_o: bfloat16 [1024, 1536], P('tp')
- w_gate: bfloat16 [1536, 3840], P(None, 'tp')
- w_up: bfloat16 [1536, 3840], P(None, 'tp')
- w_down: bfloat16 [3840, 1536], P('tp')
- norm_self: bfloat16 [1536], replicated
- norm_cross: bfloat16 [1536], replicated
- norm_mlp: bfloat16 [1536], replicated
Outputs:
- output 1: bfloat16 [1024, 1536], P('dp'), parts along dimension 0
- output 2: bfloat16 [1024, 128, 16, 64], P('dp', None, 'tp'), parts along dimension 0
- output 3: bfloat16 [1024, 128, 16, 64], P('dp', None, 'tp'), parts along dimension 0
There are 2 independent parts. The reference program is written for one: setup_inputs(seed, part) draws one part's arguments, and reference() takes and returns one part's arrays. A program takes and returns all parts, laid end to end along the dimension named above; an argument that names none is the same for every part.
All inputs are finite; a program needn't handle non-finite values.
Results may differ from the reference program's by a relative error of at most 0.0172771.
Values are sent between devices in bfloat16 or wider.
A program may use at most 1 GiB of HBM per device.

```python
import math
import jax
import jax.numpy as jnp
from jax import lax

BATCH_ROWS = 512
T_MAX = 128
SRC_LEN = 64
D_MODEL = 1536
N_HEADS = 16
D_HEAD = 64
D_FF = 3840

INNER_DIM = N_HEADS * D_HEAD
BUCKET_EDGES = tuple(int(math.ceil(16.0 * 8.0 ** (bucket_step / 16.0))) for bucket_step in range(1, 16))
NEG_FILL = -1e30


def draw_ends(rng_key, low_end, high_end):
    key_list = jax.random.split(rng_key, 3)
    drawn_vals = jax.random.randint(key_list[0], (BATCH_ROWS,), low_end, high_end + 1)
    high_row = jax.random.randint(key_list[1], (), 0, BATCH_ROWS)
    low_row = (high_row + jax.random.randint(key_list[2], (), 1, BATCH_ROWS)) % BATCH_ROWS
    return drawn_vals.at[high_row].set(high_end).at[low_row].set(low_end).astype(jnp.int32)


def normal_bf16(rng_key, array_shape, std_dev):
    return (std_dev * jax.random.normal(rng_key, array_shape, jnp.float32)).astype(jnp.bfloat16)


def setup_inputs(seed: int = 0, part: int = 0) -> dict:
    part_keys = jax.random.split(jax.random.fold_in(jax.random.key(seed), part), 8)
    shared_keys = jax.random.split(jax.random.key(seed + 1), 16)
    cache_shape = (BATCH_ROWS, T_MAX, N_HEADS, D_HEAD)
    cross_shape = (BATCH_ROWS, SRC_LEN, N_HEADS, D_HEAD)
    src_lens = draw_ends(part_keys[2], SRC_LEN // 4, SRC_LEN)
    bias_draw = 0.7 * jax.random.normal(shared_keys[0], (32, N_HEADS), jnp.float32)
    q_scale = (D_MODEL * D_HEAD) ** -0.5
    in_scale = D_MODEL ** -0.5
    out_scale = INNER_DIM ** -0.5
    return {
        'x_in': normal_bf16(part_keys[0], (BATCH_ROWS, D_MODEL), 1.0),
        'tok_pos': draw_ends(part_keys[1], T_MAX // 8, T_MAX - 1),
        'self_k': normal_bf16(part_keys[3], cache_shape, 1.0),
        'self_v': normal_bf16(part_keys[4], cache_shape, 1.0),
        'cross_k': normal_bf16(part_keys[5], cross_shape, 1.0),
        'cross_v': normal_bf16(part_keys[6], cross_shape, 1.0),
        'enc_mask': (jnp.arange(SRC_LEN)[None, :] < src_lens[:, None]).astype(jnp.int32),
        'rel_bias': bias_draw.at[0].add(0.5 * math.log(T_MAX) - 1.0),
        'w_q': normal_bf16(shared_keys[1], (D_MODEL, INNER_DIM), q_scale),
        'w_k': normal_bf16(shared_keys[2], (D_MODEL, INNER_DIM), in_scale),
        'w_v': normal_bf16(shared_keys[3], (D_MODEL, INNER_DIM), in_scale),
        'w_o': normal_bf16(shared_keys[4], (INNER_DIM, D_MODEL), 0.4 * math.sqrt(T_MAX) * out_scale),
        'cross_q': normal_bf16(shared_keys[5], (D_MODEL, INNER_DIM), q_scale),
        'cross_o': normal_bf16(shared_keys[6], (INNER_DIM, D_MODEL), 0.5 * math.sqrt(SRC_LEN) * out_scale),
        'w_gate': normal_bf16(shared_keys[7], (D_MODEL, D_FF), in_scale),
        'w_up': normal_bf16(shared_keys[8], (D_MODEL, D_FF), in_scale),
        'w_down': normal_bf16(shared_keys[9], (D_FF, D_MODEL), 1.5 * D_FF ** -0.5),
        'norm_self': (1.0 + 0.25 * jax.random.normal(shared_keys[10], (D_MODEL,), jnp.float32)).astype(jnp.bfloat16),
        'norm_cross': (1.0 + 0.25 * jax.random.normal(shared_keys[11], (D_MODEL,), jnp.float32)).astype(jnp.bfloat16),
        'norm_mlp': (1.0 + 0.25 * jax.random.normal(shared_keys[12], (D_MODEL,), jnp.float32)).astype(jnp.bfloat16),
    }


def rms_norm(values, norm_scale):
    inv_rms = lax.rsqrt(jnp.mean(values * values, axis=-1, keepdims=True) + 1e-6)
    return (values * inv_rms * norm_scale.astype(jnp.float32)).astype(jnp.bfloat16)


def project(normed, weight):
    return jnp.dot(normed, weight, preferred_element_type=jnp.float32).astype(jnp.bfloat16)


def rel_bucket(distance):
    bucket_edges = jnp.array(BUCKET_EDGES, dtype=jnp.int32)
    far_bucket = 16 + jnp.sum((distance[..., None] >= bucket_edges).astype(jnp.int32), axis=-1)
    return jnp.where(distance < 16, distance, far_bucket)


def attend(queries, keys_all, values_all, extra):
    def one_row(operands):
        row_q, row_k, row_v, row_extra = operands
        scores = jnp.einsum('hk,thk->ht', row_q.astype(jnp.float32), row_k.astype(jnp.float32)) + row_extra
        probs_bf = jax.nn.softmax(scores, axis=-1).astype(jnp.bfloat16)
        mixed_out = jnp.einsum('ht,thk->hk', probs_bf.astype(jnp.float32), row_v.astype(jnp.float32))
        return mixed_out.astype(jnp.bfloat16)
    return lax.map(one_row, (queries, keys_all, values_all, extra))


def reference(x_in, tok_pos, self_k, self_v, cross_k, cross_v, enc_mask, rel_bias, w_q, w_k, w_v, w_o, cross_q, cross_o, w_gate, w_up, w_down, norm_self, norm_cross, norm_mlp):
    row_count = x_in.shape[0]
    head_shape = (row_count, N_HEADS, D_HEAD)
    residual = x_in.astype(jnp.float32)
    normed = rms_norm(residual, norm_self)
    queries = project(normed, w_q).reshape(head_shape)
    new_keys = project(normed, w_k).reshape(head_shape)
    new_values = project(normed, w_v).reshape(head_shape)
    key_index = jnp.arange(T_MAX)
    at_pos = (key_index[None, :] == tok_pos[:, None])[:, :, None, None]
    new_self_k = jnp.where(at_pos, new_keys[:, None], self_k)
    new_self_v = jnp.where(at_pos, new_values[:, None], self_v)
    distance = jnp.maximum(tok_pos[:, None] - key_index[None, :], 0)
    bias_rows = jnp.swapaxes(jnp.take(rel_bias, rel_bucket(distance), axis=0), 1, 2)
    causal = (key_index[None, :] <= tok_pos[:, None])[:, None, :]
    self_extra = jnp.where(causal, bias_rows, NEG_FILL)
    mixed_self = attend(queries, new_self_k, new_self_v, self_extra)
    residual = residual + jnp.dot(mixed_self.reshape(row_count, INNER_DIM), w_o, preferred_element_type=jnp.float32)
    normed = rms_norm(residual, norm_cross)
    cross_queries = project(normed, cross_q).reshape(head_shape)
    cross_extra = jnp.where(enc_mask[:, None, :] != 0, 0.0, NEG_FILL)
    mixed_cross = attend(cross_queries, cross_k, cross_v, cross_extra)
    residual = residual + jnp.dot(mixed_cross.reshape(row_count, INNER_DIM), cross_o, preferred_element_type=jnp.float32)
    normed = rms_norm(residual, norm_mlp)
    gate_pre = jnp.dot(normed, w_gate, preferred_element_type=jnp.float32)
    up_pre = jnp.dot(normed, w_up, preferred_element_type=jnp.float32)
    hidden = (jax.nn.gelu(gate_pre, approximate=True) * up_pre).astype(jnp.bfloat16)
    residual = residual + jnp.dot(hidden, w_down, preferred_element_type=jnp.float32)
    return (residual.astype(jnp.bfloat16), new_self_k, new_self_v)
```

```python
import functools
import math
import jax
import jax.numpy as jnp
from jax import lax
from jax.experimental import pallas as pl
from jax.experimental.pallas import tpu as pltpu
from jax.sharding import PartitionSpec as P

BUCKET_EDGES = tuple(int(math.ceil(16.0 * 8.0 ** (bucket_step / 16.0))) for bucket_step in range(1, 16))
NEG_FILL = -1e30
STEP_ROWS = 32
LANES = 128
F32 = jnp.float32
BF16 = jnp.bfloat16


def rms_norm(values, norm_scale):
    inv_rms = lax.rsqrt(jnp.mean(values * values, axis=-1, keepdims=True) + 1e-6)
    return (values * inv_rms * norm_scale.astype(F32)).astype(BF16)


def dot(a, b):
    return jnp.dot(a, b, preferred_element_type=F32)


def dot_nt(a, b):
    return lax.dot_general(a, b, (((1,), (1,)), ((), ())), preferred_element_type=F32)


def iota(shape, axis):
    return lax.broadcasted_iota(jnp.int32, shape, axis)


def self_kernel(heads, head_dim, pos_ref, bias_ref, x_ref, wq_ref, wk_ref, wv_ref, norm_ref, k_ref, v_ref,
                mixed_ref, ko_ref, vo_ref, q_s, kt_s, vt_s, table_s, score_s, out_s):
    step = pl.program_id(0)
    flat = heads * head_dim
    rows_total = x_ref.shape[0]

    @pl.when(step == 0)
    def _():
        lane = iota((4 * heads, LANES), 1)
        head_of = lax.rem(iota((4 * heads, LANES), 0), heads)
        far = jnp.full_like(lane, 16)
        for edge in BUCKET_EDGES:
            far = far + jnp.where(lane >= edge, 1, 0)
        bucket = jnp.where(lane < 16, lane, far)
        table = jnp.zeros((4 * heads, LANES), F32)
        for b in range(32):
            here = jnp.zeros((4 * heads, LANES), F32)
            for h in range(heads):
                here = jnp.where(head_of == h, bias_ref[h, b], here)
            table = jnp.where(bucket == b, here, table)
        table_s[...] = table

        @pl.loop(0, rows_total // LANES)
        def _(g):
            rows = pl.ds(pl.multiple_of(g * LANES, LANES), LANES)
            normed = rms_norm(x_ref[rows, :].astype(F32), norm_ref[...])
            q_s[rows, :] = dot(normed, wq_ref[...]).astype(BF16)
            kt_s[g] = dot(normed, wk_ref[...]).astype(BF16).astype(F32).T
            vt_s[g] = dot(normed, wv_ref[...]).astype(BF16).astype(F32).T

    n = STEP_ROWS
    first = pl.multiple_of(step * n, n)
    per = LANES // n
    group, part = step // per, lax.rem(step, per)
    shift = lax.rem(LANES - part * n, LANES)
    k_new = pltpu.roll(kt_s[group], shift, 1)
    v_new = pltpu.roll(vt_s[group], shift, 1)

    spread = jnp.where(iota((n * heads, n), 0) // heads == iota((n * heads, n), 1), 1.0, 0.0).astype(BF16)
    own_head = iota((n * heads, flat), 1) // head_dim == lax.rem(iota((n * heads, flat), 0), heads)
    q_rows = jnp.where(own_head, dot(spread, q_s[pl.ds(first, n), :]), 0.0).astype(BF16)

    lane_bf = iota((flat, LANES), 1).astype(F32).astype(BF16)
    quad_row = iota((4 * heads, LANES), 0)
    table = table_s[...]

    def update(cache_ref, new_cols, out_ref, b):
        at_pos = lane_bf == pos_ref[first + b].astype(F32).astype(BF16)
        col = jnp.broadcast_to(new_cols[:, b:b + 1], (flat, LANES)).astype(BF16)
        updated = jnp.where(at_pos, col, cache_ref[b])
        out_ref[b] = updated
        return updated

    for g in range(n // 4):
        lhs = q_rows[4 * heads * g:4 * heads * (g + 1), :]
        picked = None
        distance = None
        for half in range(2):
            b = 4 * g + 2 * half
            pair = jnp.concatenate([update(k_ref, k_new, ko_ref, b), update(k_ref, k_new, ko_ref, b + 1)], axis=1)
            both = dot(lhs, pair)
            for j in range(2):
                mine = both[:, LANES * j:LANES * (j + 1)]
                at = 2 * half + j
                pos = pos_ref[first + 4 * g + at]
                picked = mine if picked is None else jnp.where(quad_row >= heads * at, mine, picked)
                distance = jnp.full((4 * heads, LANES), pos, jnp.int32) if distance is None else jnp.where(quad_row >= heads * at, pos, distance)
        distance = distance - iota((4 * heads, LANES), 1)
        bias = jnp.take_along_axis(table, jnp.maximum(distance, 0), axis=1)
        score_s[4 * heads * g:4 * heads * (g + 1), :] = jnp.where(distance >= 0, picked + bias, NEG_FILL)

    scores = score_s[...]
    exps = jnp.exp(scores - jnp.max(scores, axis=1, keepdims=True))
    probs = exps * pl.reciprocal(jnp.sum(exps, axis=1, keepdims=True))

    for g in range(n // 4):
        quad = probs[4 * heads * g:4 * heads * (g + 1), :]
        picked = None
        for half in range(2):
            b = 4 * g + 2 * half
            pair = jnp.concatenate([update(v_ref, v_new, vo_ref, b), update(v_ref, v_new, vo_ref, b + 1)], axis=1)
            low = jnp.where(quad_row // heads == 2 * half, quad, 0.0)
            high = jnp.where(quad_row // heads == 2 * half + 1, quad, 0.0)
            lhs = jnp.concatenate([low, high], axis=1).astype(BF16)
            both = dot_nt(lhs, pair)
            picked = both if half == 0 else jnp.where(iota(both.shape, 0) >= 2 * heads, both, picked)
        out_s[4 * heads * g:4 * heads * (g + 1), :] = picked
    gather = jnp.where(iota((n, n * heads), 1) // heads == iota((n, n * heads), 0), 1.0, 0.0).astype(BF16)
    mixed_ref[...] = dot(gather, jnp.where(own_head, out_s[...], 0.0).astype(BF16)).astype(BF16)


def self_attention(tok_pos, bias_t, x_in, w_q, w_k, w_v, norm_self, keys, values, heads):
    rows, flat, t_len = keys.shape
    d_model = x_in.shape[1]
    n = STEP_ROWS
    smem = pl.BlockSpec(memory_space=pltpu.SMEM)
    whole = lambda *shape: pl.BlockSpec(shape, lambda i: (0,) * len(shape))
    cache = pl.BlockSpec((n, flat, t_len), lambda i: (i, 0, 0))
    cache_shape = jax.ShapeDtypeStruct(keys.shape, BF16)
    return pl.pallas_call(
        functools.partial(self_kernel, heads, flat // heads),
        grid=(rows // n,),
        in_specs=[smem, smem, whole(rows, d_model), whole(d_model, flat), whole(d_model, flat), whole(d_model, flat),
                  whole(1, d_model), cache, cache],
        out_specs=[pl.BlockSpec((n, flat), lambda i: (i, 0)), cache, cache],
        out_shape=[jax.ShapeDtypeStruct((rows, flat), BF16), cache_shape, cache_shape],
        scratch_shapes=[
            pltpu.VMEM((rows, flat), BF16),
            pltpu.VMEM((rows // LANES, flat, LANES), F32),
            pltpu.VMEM((rows // LANES, flat, LANES), F32),
            pltpu.VMEM((4 * heads, LANES), F32),
            pltpu.VMEM((n * heads, LANES), F32),
            pltpu.VMEM((n * heads, flat), F32),
        ],
        compiler_params=pltpu.CompilerParams(dimension_semantics=('arbitrary',), vmem_limit_bytes=48 * 1024 * 1024),
        cost_estimate=pl.CostEstimate(flops=4 * rows * flat * t_len * 16 + 6 * rows * d_model * flat, bytes_accessed=8 * rows * flat * t_len, transcendentals=rows * heads * t_len),
        name='self_attention',
    )(tok_pos, bias_t, x_in, w_q, w_k, w_v, norm_self.reshape(1, d_model), keys, values)


def attend(queries, keys_all, values_all, extra):
    scores = jnp.einsum('bhk,bthk->bht', queries, keys_all, preferred_element_type=jnp.float32) + extra
    probs_bf = jax.nn.softmax(scores, axis=-1).astype(jnp.bfloat16)
    mixed_out = jnp.einsum('bht,bthk->bhk', probs_bf, values_all, preferred_element_type=jnp.float32)
    return mixed_out.astype(jnp.bfloat16)


def solution(mesh):
    def tp_sum(partial_out):
        return lax.psum(partial_out.astype(jnp.bfloat16), 'tp').astype(jnp.float32)

    def local_layer(x_in, tok_pos, self_k, self_v, cross_k, cross_v, enc_mask, rel_bias, w_q, w_k, w_v, w_o, cross_q, cross_o, w_gate, w_up, w_down, norm_self, norm_cross, norm_mlp):
        rows, t_len, heads, head_dim = self_k.shape
        flat = heads * head_dim
        head_shape = (rows, heads, head_dim)
        to_kernel = lambda c: jnp.transpose(c, (0, 2, 3, 1)).reshape(rows, flat, t_len)
        from_kernel = lambda c: jnp.transpose(c.reshape(rows, heads, head_dim, t_len), (0, 3, 1, 2))
        mixed_self, new_k, new_v = self_attention(tok_pos, rel_bias.T, x_in, w_q, w_k, w_v, norm_self, to_kernel(self_k), to_kernel(self_v), heads)
        residual = x_in.astype(F32)
        residual = residual + tp_sum(dot(mixed_self, w_o))
        normed = rms_norm(residual, norm_cross)
        cross_queries = dot(normed, cross_q).astype(BF16).reshape(head_shape)
        cross_extra = jnp.where(enc_mask[:, None, :] != 0, 0.0, NEG_FILL)
        mixed_cross = attend(cross_queries, cross_k, cross_v, cross_extra)
        residual = residual + tp_sum(dot(mixed_cross.reshape(rows, flat), cross_o))
        normed = rms_norm(residual, norm_mlp)
        gate_pre = dot(normed, w_gate)
        up_pre = dot(normed, w_up)
        hidden = (jax.nn.gelu(gate_pre, approximate=True) * up_pre).astype(BF16)
        residual = residual + tp_sum(dot(hidden, w_down))
        return residual.astype(BF16), from_kernel(new_k), from_kernel(new_v)

    cache_spec = P('dp', None, 'tp', None)
    split_cols = P(None, 'tp')
    split_rows = P('tp', None)
    in_specs = (P('dp', None), P('dp'), cache_spec, cache_spec, cache_spec, cache_spec, P('dp', None), split_cols, split_cols, split_cols, split_cols, split_rows, split_cols, split_rows, split_cols, split_cols, split_rows, P(None), P(None), P(None))
    out_specs = (P('dp', None), cache_spec, cache_spec)
    return jax.shard_map(local_layer, mesh=mesh, in_specs=in_specs, out_specs=out_specs, check_vma=False)
```

```python
import functools
import math
import jax
import jax.numpy as jnp
from jax import lax
from jax.experimental import pallas as pl
from jax.experimental.pallas import tpu as pltpu
from jax.sharding import PartitionSpec as P

BUCKET_EDGES = tuple(int(math.ceil(16.0 * 8.0 ** (bucket_step / 16.0))) for bucket_step in range(1, 16))
NEG_FILL = -1e30
STEP_ROWS = 32
LANES = 128
F32 = jnp.float32
BF16 = jnp.bfloat16


def rms_norm(values, norm_scale):
    inv_rms = lax.rsqrt(jnp.mean(values * values, axis=-1, keepdims=True) + 1e-6)
    return (values * inv_rms * norm_scale.astype(F32)).astype(BF16)


def dot(a, b):
    return jnp.dot(a, b, preferred_element_type=F32)


def dot_nt(a, b):
    return lax.dot_general(a, b, (((1,), (1,)), ((), ())), preferred_element_type=F32)


def iota(shape, axis):
    return lax.broadcasted_iota(jnp.int32, shape, axis)


def self_kernel(heads, head_dim, pos_ref, bias_ref, x_ref, wq_ref, wk_ref, wv_ref, norm_ref, k_ref, v_ref,
                mixed_ref, ko_ref, vo_ref, q_s, kt_s, vt_s, table_s, score_s, out_s):
    step = pl.program_id(0)
    flat = heads * head_dim
    rows_total = x_ref.shape[0]

    @pl.when(step == 0)
    def _():
        lane = iota((4 * heads, LANES), 1)
        head_of = lax.rem(iota((4 * heads, LANES), 0), heads)
        far = jnp.full_like(lane, 16)
        for edge in BUCKET_EDGES:
            far = far + jnp.where(lane >= edge, 1, 0)
        bucket = jnp.where(lane < 16, lane, far)
        table = jnp.zeros((4 * heads, LANES), F32)
        for b in range(32):
            here = jnp.zeros((4 * heads, LANES), F32)
            for h in range(heads):
                here = jnp.where(head_of == h, bias_ref[h, b], here)
            table = jnp.where(bucket == b, here, table)
        table_s[...] = table

        @pl.loop(0, rows_total // LANES)
        def _(g):
            rows = pl.ds(pl.multiple_of(g * LANES, LANES), LANES)
            normed = rms_norm(x_ref[rows, :].astype(F32), norm_ref[...])
            q_s[rows, :] = dot(normed, wq_ref[...]).astype(BF16)
            kt_s[g] = dot(normed, wk_ref[...]).astype(BF16).astype(F32).T
            vt_s[g] = dot(normed, wv_ref[...]).astype(BF16).astype(F32).T

    n = STEP_ROWS
    first = pl.multiple_of(step * n, n)
    per = LANES // n
    group, part = step // per, lax.rem(step, per)
    shift = lax.rem(LANES - part * n, LANES)
    k_new = pltpu.roll(kt_s[group], shift, 1)
    v_new = pltpu.roll(vt_s[group], shift, 1)

    spread = jnp.where(iota((n * heads, n), 0) // heads == iota((n * heads, n), 1), 1.0, 0.0).astype(BF16)
    own_head = iota((n * heads, flat), 1) // head_dim == lax.rem(iota((n * heads, flat), 0), heads)
    q_rows = jnp.where(own_head, dot(spread, q_s[pl.ds(first, n), :]), 0.0).astype(BF16)

    lane_bf = iota((flat, LANES), 1).astype(F32).astype(BF16)
    quad_row = iota((4 * heads, LANES), 0)
    table = table_s[...]

    def update(cache_ref, new_cols, out_ref, b):
        at_pos = lane_bf == pos_ref[first + b].astype(F32).astype(BF16)
        col = jnp.broadcast_to(new_cols[:, b:b + 1], (flat, LANES)).astype(BF16)
        updated = jnp.where(at_pos, col, cache_ref[b])
        out_ref[b] = updated
        return updated

    for g in range(n // 4):
        lhs = q_rows[4 * heads * g:4 * heads * (g + 1), :]
        picked = None
        distance = None
        for half in range(2):
            b = 4 * g + 2 * half
            pair = jnp.concatenate([update(k_ref, k_new, ko_ref, b), update(k_ref, k_new, ko_ref, b + 1)], axis=1)
            both = dot(lhs, pair)
            for j in range(2):
                mine = both[:, LANES * j:LANES * (j + 1)]
                at = 2 * half + j
                pos = pos_ref[first + 4 * g + at]
                picked = mine if picked is None else jnp.where(quad_row >= heads * at, mine, picked)
                distance = jnp.full((4 * heads, LANES), pos, jnp.int32) if distance is None else jnp.where(quad_row >= heads * at, pos, distance)
        distance = distance - iota((4 * heads, LANES), 1)
        bias = jnp.take_along_axis(table, jnp.maximum(distance, 0), axis=1)
        score_s[4 * heads * g:4 * heads * (g + 1), :] = jnp.where(distance >= 0, picked + bias, NEG_FILL)

    scores = score_s[...]
    exps = jnp.exp(scores - jnp.max(scores, axis=1, keepdims=True))
    probs = exps * pl.reciprocal(jnp.sum(exps, axis=1, keepdims=True))

    for g in range(n // 4):
        quad = probs[4 * heads * g:4 * heads * (g + 1), :]
        picked = None
        for half in range(2):
            b = 4 * g + 2 * half
            pair = jnp.concatenate([update(v_ref, v_new, vo_ref, b), update(v_ref, v_new, vo_ref, b + 1)], axis=1)
            low = jnp.where(quad_row // heads == 2 * half, quad, 0.0)
            high = jnp.where(quad_row // heads == 2 * half + 1, quad, 0.0)
            lhs = jnp.concatenate([low, high], axis=1).astype(BF16)
            both = dot_nt(lhs, pair)
            picked = both if half == 0 else jnp.where(iota(both.shape, 0) >= 2 * heads, both, picked)
        out_s[4 * heads * g:4 * heads * (g + 1), :] = picked
    gather = jnp.where(iota((n, n * heads), 1) // heads == iota((n, n * heads), 0), 1.0, 0.0).astype(BF16)
    mixed_ref[...] = dot(gather, jnp.where(own_head, out_s[...], 0.0).astype(BF16)).astype(BF16)


def self_attention(tok_pos, bias_t, x_in, w_q, w_k, w_v, norm_self, keys, values, heads):
    rows, flat, t_len = keys.shape
    d_model = x_in.shape[1]
    n = STEP_ROWS
    smem = pl.BlockSpec(memory_space=pltpu.SMEM)
    whole = lambda *shape: pl.BlockSpec(shape, lambda i: (0,) * len(shape))
    cache = pl.BlockSpec((n, flat, t_len), lambda i: (i, 0, 0))
    cache_shape = jax.ShapeDtypeStruct(keys.shape, BF16)
    return pl.pallas_call(
        functools.partial(self_kernel, heads, flat // heads),
        grid=(rows // n,),
        in_specs=[smem, smem, whole(rows, d_model), whole(d_model, flat), whole(d_model, flat), whole(d_model, flat),
                  whole(1, d_model), cache, cache],
        out_specs=[pl.BlockSpec((n, flat), lambda i: (i, 0)), cache, cache],
        out_shape=[jax.ShapeDtypeStruct((rows, flat), BF16), cache_shape, cache_shape],
        scratch_shapes=[
            pltpu.VMEM((rows, flat), BF16),
            pltpu.VMEM((rows // LANES, flat, LANES), F32),
            pltpu.VMEM((rows // LANES, flat, LANES), F32),
            pltpu.VMEM((4 * heads, LANES), F32),
            pltpu.VMEM((n * heads, LANES), F32),
            pltpu.VMEM((n * heads, flat), F32),
        ],
        compiler_params=pltpu.CompilerParams(dimension_semantics=('arbitrary',), vmem_limit_bytes=63 * 1024 * 1024),
        cost_estimate=pl.CostEstimate(flops=4 * rows * flat * t_len * 16 + 6 * rows * d_model * flat, bytes_accessed=8 * rows * flat * t_len, transcendentals=rows * heads * t_len),
        name='self_attention',
    )(tok_pos, bias_t, x_in, w_q, w_k, w_v, norm_self.reshape(1, d_model), keys, values)


CHUNK = 128
MESH = pl.DeviceIdType.MESH


def rest_kernel(heads, n_cross_slots,
                x_ref, mixed_ref, wo_ref, wox_ref, co_ref, cox_ref, cq_ref, gate_ref, up_ref, down_ref, norm_c_ref, norm_m_ref,
                mask_ref, ck_ref, cv_ref, out_ref,
                x_s, res_s, mix_s, cmix_s, wo_s, co_s, cq_s, gate_s, up_s, down_s, k_s, v_s, mask_s,
                qt_s, score_s, hid_s, part_s, near_s, chip_s, far_s, done_s,
                ag_send, ag_recv, w_send, w_recv, sum_send, sum_recv, load_sem, cross_sem, out_sem):
    me = lax.axis_index('tp')
    core = lax.rem(me, 2)
    mate = me + 1 - 2 * core
    over = lax.rem(me + 2, 4)
    cater = lax.rem(mate + 2, 4)
    rows_total, d_model = x_ref.shape
    flat = mixed_ref.shape[1]
    head_dim = flat // heads
    src_len = ck_ref.shape[0]
    d_ff = gate_ref.shape[0]
    chunks = rows_total // CHUNK
    half = CHUNK // 2

    def remote(src, dst, send_sem, recv_sem, to):
        return pltpu.make_async_remote_copy(src_ref=src, dst_ref=dst, send_sem=send_sem, recv_sem=recv_sem,
                                            device_id={'tp': to}, device_id_type=MESH)

    def block(buf, who, c):
        return buf.at[who, pl.ds(CHUNK * c, CHUNK), :]

    def shard(buf, who):
        return buf.at[pl.ds(pl.multiple_of(who * flat, flat), flat), :]

    loads = []

    def load(src, dst):
        copy = pltpu.make_async_copy(src, dst, load_sem.at[len(loads)])
        copy.start()
        loads.append(copy)
        return copy

    def cross_load(c):
        slot = c % n_cross_slots
        cols = pl.ds(CHUNK * c, CHUNK)
        return (pltpu.make_async_copy(ck_ref.at[:, :, cols], k_s.at[slot], cross_sem.at[0, slot]),
                pltpu.make_async_copy(cv_ref.at[:, :, cols], v_s.at[slot], cross_sem.at[1, slot]))

    own_mixed = load(mixed_ref, mix_s.at[me])
    x_load = load(x_ref, x_s)
    own_wo = (load(wo_ref, shard(wo_s, me)), load(wox_ref, shard(wo_s, over)))
    q_load = load(cq_ref, cq_s)
    mask_load = load(mask_ref, mask_s)
    first_cross = cross_load(0)
    for copy in first_cross:
        copy.start()
    own_co = (load(co_ref, shard(co_s, me)), load(cox_ref, shard(co_s, over)))
    mlp_loads = (load(gate_ref, gate_s), load(up_ref, up_s), load(down_ref, down_s))
    for c in range(1, n_cross_slots):
        for copy in cross_load(c):
            copy.start()

    barrier = pltpu.get_barrier_semaphore()
    for peer in (mate, over):
        pl.semaphore_signal(barrier, inc=1, device_id={'tp': peer}, device_id_type=MESH)
    pl.semaphore_wait(barrier, 2)

    sends = []

    def send(copy):
        copy.start()
        sends.append(copy)

    def gather_send(stage, src, buf, c):
        send(remote(src, block(buf, me, c), ag_send.at[stage, 0, c], ag_recv.at[stage, 0, c], over))
        send(remote(src, block(buf, me, c), ag_send.at[stage, 1, c], ag_recv.at[stage, 1, c], mate))

    def gather_relay(stage, buf, c):
        remote(block(buf, over, c), block(buf, over, c), ag_send.at[stage, 0, c], ag_recv.at[stage, 0, c], over).wait_recv()
        send(remote(block(buf, over, c), block(buf, over, c), ag_send.at[stage, 2, c], ag_recv.at[stage, 2, c], mate))

    def gather_wait(stage, buf, c):
        remote(block(buf, mate, c), block(buf, mate, c), ag_send.at[stage, 1, c], ag_recv.at[stage, 1, c], mate).wait_recv()
        remote(block(buf, cater, c), block(buf, cater, c), ag_send.at[stage, 2, c], ag_recv.at[stage, 2, c], mate).wait_recv()

    def weight_send(which, ref, ref_x, buf):
        send(remote(ref, shard(buf, me), w_send.at[which, 0], w_recv.at[which, 0], mate))
        send(remote(ref_x, shard(buf, over), w_send.at[which, 1], w_recv.at[which, 1], mate))

    def weight_wait(which, buf):
        remote(shard(buf, mate), shard(buf, mate), w_send.at[which, 0], w_recv.at[which, 0], mate).wait_recv()
        remote(shard(buf, cater), shard(buf, cater), w_send.at[which, 1], w_recv.at[which, 1], mate).wait_recv()

    for c in range(chunks):
        gather_send(0, mixed_ref.at[pl.ds(CHUNK * c, CHUNK), :], mix_s, c)
    weight_send(0, wo_ref, wox_ref, wo_s)

    def project_heads(buf, weight, c, add_to):
        lhs = jnp.concatenate([buf[i, CHUNK * c:CHUNK * (c + 1), :] for i in range(4)], axis=1)
        for n in range(0, d_model, 512):
            res_s[CHUNK * c:CHUNK * (c + 1), n:n + 512] = add_to[CHUNK * c:CHUNK * (c + 1), n:n + 512].astype(F32) + dot(lhs, weight[:, n:n + 512])

    def cross_query(c):
        if c == 0:
            own_mixed.wait()
            x_load.wait()
            for copy in own_wo:
                copy.wait()
        gather_wait(0, mix_s, c)
        if c == 0:
            weight_wait(0, wo_s)
            q_load.wait()
        project_heads(mix_s, wo_s, c, x_s)
        normed = rms_norm(res_s[CHUNK * c:CHUNK * (c + 1), :], norm_c_ref[...])
        qt_s[...] = dot(normed, cq_s[...]).astype(BF16).astype(F32).T

    def cross_attend(c):
        slot = c % n_cross_slots
        for copy in cross_load(c):
            copy.wait()
        if c == 0:
            mask_load.wait()
        step = 8

        @pl.loop(0, src_len // step)
        def _(i):
            at = pl.ds(pl.multiple_of(i * step, step), step)
            for h in range(heads):
                d = slice(head_dim * h, head_dim * (h + 1))
                score_s[h, at, :] = jnp.sum(k_s[slot, at, d, :].astype(F32) * qt_s[d, :][None], axis=1)

        valid = mask_s[:, CHUNK * c:CHUNK * (c + 1)] != 0
        for h in range(heads):
            scores = jnp.where(valid, score_s[h], NEG_FILL)
            exps = jnp.exp(scores - jnp.max(scores, axis=0, keepdims=True))
            probs = exps * pl.reciprocal(jnp.sum(exps, axis=0, keepdims=True))
            score_s[h] = probs.astype(BF16).astype(F32)

        def mix(i, acc):
            acc = list(acc)
            for j in range(step):
                s = i * step + j
                for h in range(heads):
                    d = slice(head_dim * h, head_dim * (h + 1))
                    acc[h] = acc[h] + v_s[slot, s, d, :].astype(F32) * score_s[h, pl.ds(s, 1), :]
            return tuple(acc)

        zero = jnp.zeros((head_dim, CHUNK), F32)
        acc = lax.fori_loop(0, src_len // step, mix, (zero,) * heads)
        cmix_s[me, CHUNK * c:CHUNK * (c + 1), :] = jnp.concatenate(acc, axis=0).T.astype(BF16)
        gather_send(1, block(cmix_s, me, c), cmix_s, c)
        if c + n_cross_slots < chunks:
            for copy in cross_load(c + n_cross_slots):
                copy.start()

    def mlp(c):
        if c == 0:
            for copy in own_co:
                copy.wait()
            weight_wait(1, co_s)
        gather_wait(1, cmix_s, c)
        project_heads(cmix_s, co_s, c, res_s)
        if c == 0:
            for copy in mlp_loads:
                copy.wait()
        normed = rms_norm(res_s[CHUNK * c:CHUNK * (c + 1), :], norm_m_ref[...])
        for n in range(0, d_ff, 256):
            end = min(d_ff, n + 256)
            gate = dot_nt(normed, gate_s[n:end, :])
            up = dot_nt(normed, up_s[n:end, :])
            hid_s[:, n:end] = (jax.nn.gelu(gate, approximate=True) * up).astype(BF16)
        hidden = hid_s[...]
        for n in range(0, d_model, 512):
            part_s[c, :, n:n + 512] = dot(hidden, down_s[:, n:n + 512]).astype(BF16)
        give = pl.ds(pl.multiple_of((1 - core) * half, half), half)
        send(remote(part_s.at[c, give, :], near_s.at[c], sum_send.at[0, c], sum_recv.at[0, c], mate))

    keep = pl.ds(pl.multiple_of(core * half, half), half)

    def chip_sum(c):
        remote(near_s.at[c], near_s.at[c], sum_send.at[0, c], sum_recv.at[0, c], mate).wait_recv()
        chip_s[c] = (part_s[c, keep, :].astype(F32) + near_s[c].astype(F32)).astype(BF16)
        send(remote(chip_s.at[c], far_s.at[c], sum_send.at[1, c], sum_recv.at[1, c], over))

    def full_sum(c):
        remote(far_s.at[c], far_s.at[c], sum_send.at[1, c], sum_recv.at[1, c], over).wait_recv()
        mine = pl.ds(pl.multiple_of(CHUNK * c + core * half, half), half)
        done_s[mine, :] = (res_s[mine, :] + (chip_s[c].astype(F32) + far_s[c].astype(F32))).astype(BF16)
        send(remote(done_s.at[mine, :], done_s.at[mine, :], sum_send.at[2, c], sum_recv.at[2, c], mate))

    def store(c):
        other = pl.ds(pl.multiple_of(CHUNK * c + (1 - core) * half, half), half)
        remote(done_s.at[other, :], done_s.at[other, :], sum_send.at[2, c], sum_recv.at[2, c], mate).wait_recv()
        rows = pl.ds(CHUNK * c, CHUNK)
        copy = pltpu.make_async_copy(done_s.at[rows, :], out_ref.at[rows, :], out_sem.at[c])
        copy.start()
        return copy

    for c in range(chunks):
        gather_relay(0, mix_s, c)
        if c == 0:
            cross_query(0)
    weight_send(1, co_ref, cox_ref, co_s)
    cross_attend(0)
    cross_query(1)
    gather_relay(1, cmix_s, 0)
    cross_attend(1)
    mlp(0)
    cross_query(2)
    gather_relay(1, cmix_s, 1)
    chip_sum(0)
    cross_attend(2)
    mlp(1)
    cross_query(3)
    gather_relay(1, cmix_s, 2)
    chip_sum(1)
    cross_attend(3)
    mlp(2)
    full_sum(0)
    gather_relay(1, cmix_s, 3)
    chip_sum(2)
    mlp(3)
    full_sum(1)
    stores = [store(0)]
    chip_sum(3)
    full_sum(2)
    stores.append(store(1))
    full_sum(3)
    stores.append(store(2))
    stores.append(store(3))
    for copy in stores:
        copy.wait()
    for copy in sends:
        copy.wait_send()


def rest_of_layer(x_in, mixed, w_o, w_o_over, cross_o, cross_o_over, cross_q, gate_t, up_t, w_down, norm_cross, norm_mlp, mask_t, cross_k, cross_v, heads):
    rows, d_model = x_in.shape
    flat = mixed.shape[1]
    d_ff = gate_t.shape[0]
    src_len = cross_k.shape[0]
    chunks = rows // CHUNK
    slots = 3
    anywhere = pl.BlockSpec(memory_space=pl.ANY)
    vmem = pl.BlockSpec(memory_space=pltpu.VMEM)
    dma = pltpu.SemaphoreType.DMA
    return pl.pallas_call(
        functools.partial(rest_kernel, heads, slots),
        in_specs=[anywhere] * 10 + [vmem, vmem] + [anywhere] * 3,
        out_specs=anywhere,
        out_shape=jax.ShapeDtypeStruct((rows, d_model), BF16),
        scratch_shapes=[
            pltpu.VMEM((rows, d_model), BF16),
            pltpu.VMEM((rows, d_model), F32),
            pltpu.VMEM((4, rows, flat), BF16),
            pltpu.VMEM((4, rows, flat), BF16),
            pltpu.VMEM((4 * flat, d_model), BF16),
            pltpu.VMEM((4 * flat, d_model), BF16),
            pltpu.VMEM((d_model, flat), BF16),
            pltpu.VMEM((d_ff, d_model), BF16),
            pltpu.VMEM((d_ff, d_model), BF16),
            pltpu.VMEM((d_ff, d_model), BF16),
            pltpu.VMEM((slots, src_len, flat, CHUNK), BF16),
            pltpu.VMEM((slots, src_len, flat, CHUNK), BF16),
            pltpu.VMEM((src_len, rows), jnp.int32),
            pltpu.VMEM((flat, CHUNK), F32),
            pltpu.VMEM((heads, src_len, CHUNK), F32),
            pltpu.VMEM((CHUNK, d_ff), BF16),
            pltpu.VMEM((chunks, CHUNK, d_model), BF16),
            pltpu.VMEM((chunks, CHUNK // 2, d_model), BF16),
            pltpu.VMEM((chunks, CHUNK // 2, d_model), BF16),
            pltpu.VMEM((chunks, CHUNK // 2, d_model), BF16),
            pltpu.VMEM((rows, d_model), BF16),
            dma((2, 3, chunks)), dma((2, 3, chunks)),
            dma((2, 2)), dma((2, 2)),
            dma((3, chunks)), dma((3, chunks)),
            dma((16,)), dma((2, slots)), dma((chunks,)),
        ],
        compiler_params=pltpu.CompilerParams(collective_id=0, has_side_effects=True, vmem_limit_bytes=63 * 1024 * 1024),
        cost_estimate=pl.CostEstimate(flops=2 * rows * d_model * (8 * flat + flat + 3 * d_ff), bytes_accessed=50_000_000, transcendentals=rows * d_ff),
        name='rest_of_layer',
    )(x_in, mixed, w_o, w_o_over, cross_o, cross_o_over, cross_q, gate_t, up_t, w_down, norm_cross.reshape(1, d_model), norm_mlp.reshape(1, d_model), mask_t, cross_k, cross_v)


def solution(mesh):
    def local_layer(x_in, tok_pos, self_k, self_v, cross_k, cross_v, enc_mask, rel_bias, w_q, w_k, w_v, w_o, cross_q, cross_o, w_gate, w_up, w_down, norm_self, norm_cross, norm_mlp):
        rows, t_len, heads, head_dim = self_k.shape
        flat = heads * head_dim
        to_kernel = lambda c: jnp.transpose(c, (0, 2, 3, 1)).reshape(rows, flat, t_len)
        from_kernel = lambda c: jnp.transpose(c.reshape(rows, heads, head_dim, t_len), (0, 3, 1, 2))
        cross_view = lambda c: jnp.transpose(c, (1, 2, 3, 0)).reshape(c.shape[1], flat, rows)
        swap = [(0, 2), (1, 3), (2, 0), (3, 1)]
        w_o_over = lax.ppermute(w_o, 'tp', swap)
        cross_o_over = lax.ppermute(cross_o, 'tp', swap)
        mixed_self, new_k, new_v = self_attention(tok_pos, rel_bias.T, x_in, w_q, w_k, w_v, norm_self, to_kernel(self_k), to_kernel(self_v), heads)
        x_out = rest_of_layer(x_in, mixed_self, w_o, w_o_over, cross_o, cross_o_over, cross_q, w_gate.T, w_up.T, w_down, norm_cross, norm_mlp,
                              enc_mask.T, cross_view(cross_k), cross_view(cross_v), heads)
        return x_out, from_kernel(new_k), from_kernel(new_v)

    cache_spec = P('dp', None, 'tp', None)
    split_cols = P(None, 'tp')
    split_rows = P('tp', None)
    in_specs = (P('dp', None), P('dp'), cache_spec, cache_spec, cache_spec, cache_spec, P('dp', None), split_cols, split_cols, split_cols, split_cols, split_rows, split_cols, split_rows, split_cols, split_cols, split_rows, P(None), P(None), P(None))
    out_specs = (P('dp', None), cache_spec, cache_spec)
    return jax.shard_map(local_layer, mesh=mesh, in_specs=in_specs, out_specs=out_specs, check_vma=False)
```

```python
import functools
import math
import jax
import jax.numpy as jnp
from jax import lax
from jax.experimental import pallas as pl
from jax.experimental.pallas import tpu as pltpu
from jax.sharding import PartitionSpec as P

BUCKET_EDGES = tuple(int(math.ceil(16.0 * 8.0 ** (bucket_step / 16.0))) for bucket_step in range(1, 16))
NEG_FILL = -1e30
STEP_ROWS = 32
SLOTS = 8
AHEAD = 4
VMEM_BYTES = 67043328
LANES = 128
F32 = jnp.float32
BF16 = jnp.bfloat16


def rms_norm(values, norm_scale):
    inv_rms = lax.rsqrt(jnp.mean(values * values, axis=-1, keepdims=True) + 1e-6)
    return (values * inv_rms * norm_scale.astype(F32)).astype(BF16)


def dot(a, b):
    return jnp.dot(a, b, preferred_element_type=F32)


def dot_nt(a, b):
    return lax.dot_general(a, b, (((1,), (1,)), ((), ())), preferred_element_type=F32)


def iota(shape, axis):
    return lax.broadcasted_iota(jnp.int32, shape, axis)


def self_kernel(heads, head_dim, pos_ref, bias_ref, x_ref, wq_ref, wk_ref, wv_ref, norm_ref, k_ref, v_ref,
                mixed_ref, ko_ref, vo_ref, x_s, wq_s, wk_s, wv_s, k_s, v_s, mixed_s, q_s, kt_s, vt_s, score_s, out_s,
                load_sem, in_sem, out_sem, mixed_sem):
    flat = heads * head_dim
    rows_total = x_ref.shape[0]
    n = STEP_ROWS
    steps = rows_total // n

    def rows_of(step):
        return pl.ds(pl.multiple_of(step * n, n), n)

    def fetch(step):
        slot = lax.rem(step, SLOTS)
        return (pltpu.make_async_copy(k_ref.at[rows_of(step)], k_s.at[slot], in_sem.at[0, slot]),
                pltpu.make_async_copy(v_ref.at[rows_of(step)], v_s.at[slot], in_sem.at[1, slot]))

    def write(step):
        slot = lax.rem(step, SLOTS)
        return (pltpu.make_async_copy(k_s.at[slot], ko_ref.at[rows_of(step)], out_sem.at[0, slot]),
                pltpu.make_async_copy(v_s.at[slot], vo_ref.at[rows_of(step)], out_sem.at[1, slot]))

    loads = [pltpu.make_async_copy(src, dst, load_sem.at[i])
             for i, (src, dst) in enumerate(((x_ref, x_s), (wq_ref, wq_s), (wk_ref, wk_s), (wv_ref, wv_s)))]
    for copy in loads:
        copy.start()
    for step in range(AHEAD):
        for copy in fetch(step):
            copy.start()

    lane = iota((4 * heads, LANES), 1)
    head_of = lax.rem(iota((4 * heads, LANES), 0), heads)
    far = jnp.full_like(lane, 16)
    for edge in BUCKET_EDGES:
        far = far + jnp.where(lane >= edge, 1, 0)
    bucket = jnp.where(lane < 16, lane, far)
    table = jnp.zeros((4 * heads, LANES), F32)
    for b in range(32):
        here = jnp.zeros((4 * heads, LANES), F32)
        for h in range(heads):
            here = jnp.where(head_of == h, bias_ref[h, b], here)
        table = jnp.where(bucket == b, here, table)

    for copy in loads:
        copy.wait()

    @pl.loop(0, rows_total // LANES)
    def _(g):
        rows = pl.ds(pl.multiple_of(g * LANES, LANES), LANES)
        normed = rms_norm(x_s[rows, :].astype(F32), norm_ref[...])
        q_s[rows, :] = dot(normed, wq_s[...]).astype(BF16)
        kt_s[g] = dot(normed, wk_s[...]).astype(BF16).astype(F32).T
        vt_s[g] = dot(normed, wv_s[...]).astype(BF16).astype(F32).T

    spread = jnp.where(iota((n * heads, n), 0) // heads == iota((n * heads, n), 1), 1.0, 0.0).astype(BF16)
    gather = jnp.where(iota((n, n * heads), 1) // heads == iota((n, n * heads), 0), 1.0, 0.0).astype(BF16)
    own_head = iota((n * heads, flat), 1) // head_dim == lax.rem(iota((n * heads, flat), 0), heads)
    lane_bf = iota((flat, LANES), 1).astype(F32).astype(BF16)
    quad_row = iota((4 * heads, LANES), 0)
    per = LANES // n

    @pl.loop(0, steps)
    def _(step):
        ahead = step + AHEAD

        @pl.when(ahead < steps)
        def _():
            @pl.when(ahead >= SLOTS)
            def _():
                for copy in write(ahead - SLOTS):
                    copy.wait()
            for copy in fetch(ahead):
                copy.start()

        first = pl.multiple_of(step * n, n)
        slot = lax.rem(step, SLOTS)
        group, part = step // per, lax.rem(step, per)
        shift = lax.rem(LANES - part * n, LANES)
        k_new = pltpu.roll(kt_s[group], shift, 1)
        v_new = pltpu.roll(vt_s[group], shift, 1)
        q_rows = jnp.where(own_head, dot(spread, q_s[pl.ds(first, n), :]), 0.0).astype(BF16)
        in_k, in_v = fetch(step)

        def update(cache, new_cols, b):
            at_pos = lane_bf == pos_ref[first + b].astype(F32).astype(BF16)
            col = jnp.broadcast_to(new_cols[:, b:b + 1], (flat, LANES)).astype(BF16)
            updated = jnp.where(at_pos, col, cache[slot, b])
            cache[slot, b] = updated
            return updated

        in_k.wait()
        for g in range(n // 4):
            lhs = q_rows[4 * heads * g:4 * heads * (g + 1), :]
            picked = None
            distance = None
            for half in range(2):
                b = 4 * g + 2 * half
                pair = jnp.concatenate([update(k_s, k_new, b), update(k_s, k_new, b + 1)], axis=1)
                both = dot(lhs, pair)
                for j in range(2):
                    mine = both[:, LANES * j:LANES * (j + 1)]
                    at = 2 * half + j
                    pos = pos_ref[first + 4 * g + at]
                    picked = mine if picked is None else jnp.where(quad_row >= heads * at, mine, picked)
                    distance = jnp.full((4 * heads, LANES), pos, jnp.int32) if distance is None else jnp.where(quad_row >= heads * at, pos, distance)
            distance = distance - iota((4 * heads, LANES), 1)
            bias = jnp.take_along_axis(table, jnp.maximum(distance, 0), axis=1)
            score_s[4 * heads * g:4 * heads * (g + 1), :] = jnp.where(distance >= 0, picked + bias, NEG_FILL)
        write(step)[0].start()

        scores = score_s[...]
        exps = jnp.exp(scores - jnp.max(scores, axis=1, keepdims=True))
        probs = exps * pl.reciprocal(jnp.sum(exps, axis=1, keepdims=True))

        in_v.wait()
        for g in range(n // 4):
            quad = probs[4 * heads * g:4 * heads * (g + 1), :]
            picked = None
            for half in range(2):
                b = 4 * g + 2 * half
                pair = jnp.concatenate([update(v_s, v_new, b), update(v_s, v_new, b + 1)], axis=1)
                low = jnp.where(quad_row // heads == 2 * half, quad, 0.0)
                high = jnp.where(quad_row // heads == 2 * half + 1, quad, 0.0)
                lhs = jnp.concatenate([low, high], axis=1).astype(BF16)
                both = dot_nt(lhs, pair)
                picked = both if half == 0 else jnp.where(iota(both.shape, 0) >= 2 * heads, both, picked)
            out_s[4 * heads * g:4 * heads * (g + 1), :] = picked
        write(step)[1].start()
        mixed_s[pl.ds(first, n), :] = dot(gather, jnp.where(own_head, out_s[...], 0.0).astype(BF16)).astype(BF16)

    mixed_copy = pltpu.make_async_copy(mixed_s, mixed_ref, mixed_sem)
    mixed_copy.start()
    for step in range(steps - SLOTS, steps):
        for copy in write(step):
            copy.wait()
    mixed_copy.wait()


def self_attention(tok_pos, bias_t, x_in, w_q, w_k, w_v, norm_self, keys, values, heads):
    rows, flat, t_len = keys.shape
    d_model = x_in.shape[1]
    n = STEP_ROWS
    smem = pl.BlockSpec(memory_space=pltpu.SMEM)
    anywhere = pl.BlockSpec(memory_space=pl.ANY)
    cache_shape = jax.ShapeDtypeStruct(keys.shape, BF16)
    return pl.pallas_call(
        functools.partial(self_kernel, heads, flat // heads),
        in_specs=[smem, smem] + [anywhere] * 4 + [pl.BlockSpec(memory_space=pltpu.VMEM)] + [anywhere] * 2,
        out_specs=[anywhere] * 3,
        out_shape=[jax.ShapeDtypeStruct((rows, flat), BF16), cache_shape, cache_shape],
        scratch_shapes=[
            pltpu.VMEM((rows, d_model), BF16),
            pltpu.VMEM((d_model, flat), BF16),
            pltpu.VMEM((d_model, flat), BF16),
            pltpu.VMEM((d_model, flat), BF16),
            pltpu.VMEM((SLOTS, n, flat, t_len), BF16),
            pltpu.VMEM((SLOTS, n, flat, t_len), BF16),
            pltpu.VMEM((rows, flat), BF16),
            pltpu.VMEM((rows, flat), BF16),
            pltpu.VMEM((rows // LANES, flat, LANES), F32),
            pltpu.VMEM((rows // LANES, flat, LANES), F32),
            pltpu.VMEM((n * heads, LANES), F32),
            pltpu.VMEM((n * heads, flat), F32),
            pltpu.SemaphoreType.DMA((4,)),
            pltpu.SemaphoreType.DMA((2, SLOTS)),
            pltpu.SemaphoreType.DMA((2, SLOTS)),
            pltpu.SemaphoreType.DMA,
        ],
        compiler_params=pltpu.CompilerParams(vmem_limit_bytes=VMEM_BYTES),
        cost_estimate=pl.CostEstimate(flops=4 * rows * flat * t_len * 16 + 6 * rows * d_model * flat, bytes_accessed=8 * rows * flat * t_len, transcendentals=rows * heads * t_len),
        name='self_attention',
    )(tok_pos, bias_t, x_in, w_q, w_k, w_v, norm_self, keys, values)


CHUNK = 128
MESH = pl.DeviceIdType.MESH


def rest_kernel(heads, n_cross_slots,
                x_ref, mixed_ref, wo_ref, wox_ref, co_ref, cox_ref, cq_ref, gate_ref, up_ref, down_ref, norm_c_ref, norm_m_ref,
                mask_ref, ck_ref, cv_ref, out_ref,
                x_s, res_s, mix_s, cmix_s, wo_s, co_s, cq_s, gate_s, up_s, down_s, k_s, v_s, mask_s,
                qt_s, score_s, hid_s, part_s, near_s, chip_s, far_s, done_s,
                ag_send, ag_recv, w_send, w_recv, sum_send, sum_recv, load_sem, cross_sem, out_sem):
    me = lax.axis_index('tp')
    core = lax.rem(me, 2)
    mate = me + 1 - 2 * core
    over = lax.rem(me + 2, 4)
    cater = lax.rem(mate + 2, 4)
    rows_total, d_model = x_ref.shape
    flat = mixed_ref.shape[1]
    head_dim = flat // heads
    src_len = ck_ref.shape[0]
    d_ff = gate_ref.shape[0]
    chunks = rows_total // CHUNK
    half = CHUNK // 2

    def remote(src, dst, send_sem, recv_sem, to):
        return pltpu.make_async_remote_copy(src_ref=src, dst_ref=dst, send_sem=send_sem, recv_sem=recv_sem,
                                            device_id={'tp': to}, device_id_type=MESH)

    def block(buf, who, c):
        return buf.at[who, pl.ds(CHUNK * c, CHUNK), :]

    def shard(buf, who):
        return buf.at[pl.ds(pl.multiple_of(who * flat, flat), flat), :]

    loads = []

    def load(src, dst):
        copy = pltpu.make_async_copy(src, dst, load_sem.at[len(loads)])
        copy.start()
        loads.append(copy)
        return copy

    def cross_load(c):
        slot = c % n_cross_slots
        cols = pl.ds(CHUNK * c, CHUNK)
        return (pltpu.make_async_copy(ck_ref.at[:, :, cols], k_s.at[slot], cross_sem.at[0, slot]),
                pltpu.make_async_copy(cv_ref.at[:, :, cols], v_s.at[slot], cross_sem.at[1, slot]))

    own_mixed = load(mixed_ref, mix_s.at[me])
    x_load = load(x_ref, x_s)
    own_wo = (load(wo_ref, shard(wo_s, me)), load(wox_ref, shard(wo_s, over)))
    q_load = load(cq_ref, cq_s)
    mask_load = load(mask_ref, mask_s)
    first_cross = cross_load(0)
    for copy in first_cross:
        copy.start()
    own_co = (load(co_ref, shard(co_s, me)), load(cox_ref, shard(co_s, over)))
    mlp_loads = (load(gate_ref, gate_s), load(up_ref, up_s), load(down_ref, down_s))
    for c in range(1, n_cross_slots):
        for copy in cross_load(c):
            copy.start()

    barrier = pltpu.get_barrier_semaphore()
    for peer in (mate, over):
        pl.semaphore_signal(barrier, inc=1, device_id={'tp': peer}, device_id_type=MESH)
    pl.semaphore_wait(barrier, 2)

    sends = []

    def send(copy):
        copy.start()
        sends.append(copy)

    def gather_send(stage, src, buf, c):
        send(remote(src, block(buf, me, c), ag_send.at[stage, 0, c], ag_recv.at[stage, 0, c], over))
        send(remote(src, block(buf, me, c), ag_send.at[stage, 1, c], ag_recv.at[stage, 1, c], mate))

    def gather_relay(stage, buf, c):
        remote(block(buf, over, c), block(buf, over, c), ag_send.at[stage, 0, c], ag_recv.at[stage, 0, c], over).wait_recv()
        send(remote(block(buf, over, c), block(buf, over, c), ag_send.at[stage, 2, c], ag_recv.at[stage, 2, c], mate))

    def gather_wait(stage, buf, c):
        remote(block(buf, mate, c), block(buf, mate, c), ag_send.at[stage, 1, c], ag_recv.at[stage, 1, c], mate).wait_recv()
        remote(block(buf, cater, c), block(buf, cater, c), ag_send.at[stage, 2, c], ag_recv.at[stage, 2, c], mate).wait_recv()

    def weight_send(which, ref, ref_x, buf):
        send(remote(ref, shard(buf, me), w_send.at[which, 0], w_recv.at[which, 0], mate))
        send(remote(ref_x, shard(buf, over), w_send.at[which, 1], w_recv.at[which, 1], mate))

    def weight_wait(which, buf):
        remote(shard(buf, mate), shard(buf, mate), w_send.at[which, 0], w_recv.at[which, 0], mate).wait_recv()
        remote(shard(buf, cater), shard(buf, cater), w_send.at[which, 1], w_recv.at[which, 1], mate).wait_recv()

    for c in range(chunks):
        gather_send(0, mixed_ref.at[pl.ds(CHUNK * c, CHUNK), :], mix_s, c)
    weight_send(0, wo_ref, wox_ref, wo_s)

    def project_heads(buf, weight, c, add_to):
        lhs = jnp.concatenate([buf[i, CHUNK * c:CHUNK * (c + 1), :] for i in range(4)], axis=1)
        for n in range(0, d_model, 512):
            res_s[CHUNK * c:CHUNK * (c + 1), n:n + 512] = add_to[CHUNK * c:CHUNK * (c + 1), n:n + 512].astype(F32) + dot(lhs, weight[:, n:n + 512])

    def cross_query(c):
        if c == 0:
            own_mixed.wait()
            x_load.wait()
            for copy in own_wo:
                copy.wait()
        gather_wait(0, mix_s, c)
        if c == 0:
            weight_wait(0, wo_s)
            q_load.wait()
        project_heads(mix_s, wo_s, c, x_s)
        normed = rms_norm(res_s[CHUNK * c:CHUNK * (c + 1), :], norm_c_ref[...])
        qt_s[...] = dot(normed, cq_s[...]).astype(BF16).astype(F32).T

    def cross_score(c):
        slot = c % n_cross_slots
        for copy in cross_load(c):
            copy.wait()
        if c == 0:
            mask_load.wait()
        step = 8

        @pl.loop(0, src_len // step)
        def _(i):
            at = pl.ds(pl.multiple_of(i * step, step), step)
            for h in range(heads):
                d = slice(head_dim * h, head_dim * (h + 1))
                score_s[h, at, :] = jnp.sum(k_s[slot, at, d, :].astype(F32) * qt_s[d, :][None], axis=1)

    def cross_mix(c):
        slot = c % n_cross_slots
        step = 8
        valid = mask_s[:, CHUNK * c:CHUNK * (c + 1)] != 0
        for h in range(heads):
            scores = jnp.where(valid, score_s[h], NEG_FILL)
            exps = jnp.exp(scores - jnp.max(scores, axis=0, keepdims=True))
            probs = exps * pl.reciprocal(jnp.sum(exps, axis=0, keepdims=True))
            score_s[h] = probs.astype(BF16).astype(F32)

        def mix(i, acc):
            acc = list(acc)
            for j in range(step):
                s = i * step + j
                for h in range(heads):
                    d = slice(head_dim * h, head_dim * (h + 1))
                    acc[h] = acc[h] + v_s[slot, s, d, :].astype(F32) * score_s[h, pl.ds(s, 1), :]
            return tuple(acc)

        zero = jnp.zeros((head_dim, CHUNK), F32)
        acc = lax.fori_loop(0, src_len // step, mix, (zero,) * heads)
        cmix_s[me, CHUNK * c:CHUNK * (c + 1), :] = jnp.concatenate(acc, axis=0).T.astype(BF16)
        gather_send(1, block(cmix_s, me, c), cmix_s, c)
        if c + n_cross_slots < chunks:
            for copy in cross_load(c + n_cross_slots):
                copy.start()

    def mlp(c):
        if c == 0:
            for copy in own_co:
                copy.wait()
            weight_wait(1, co_s)
        gather_wait(1, cmix_s, c)
        project_heads(cmix_s, co_s, c, res_s)
        if c == 0:
            for copy in mlp_loads:
                copy.wait()
        normed = rms_norm(res_s[CHUNK * c:CHUNK * (c + 1), :], norm_m_ref[...])
        for n in range(0, d_ff, 256):
            end = min(d_ff, n + 256)
            gate = dot_nt(normed, gate_s[n:end, :])
            up = dot_nt(normed, up_s[n:end, :])
            hid_s[:, n:end] = (jax.nn.gelu(gate, approximate=True) * up).astype(BF16)
        hidden = hid_s[...]
        for n in range(0, d_model, 512):
            part_s[c, :, n:n + 512] = dot(hidden, down_s[:, n:n + 512]).astype(BF16)
        give = pl.ds(pl.multiple_of((1 - core) * half, half), half)
        send(remote(part_s.at[c, give, :], near_s.at[c], sum_send.at[0, c], sum_recv.at[0, c], mate))

    keep = pl.ds(pl.multiple_of(core * half, half), half)

    def chip_sum(c):
        remote(near_s.at[c], near_s.at[c], sum_send.at[0, c], sum_recv.at[0, c], mate).wait_recv()
        chip_s[c] = (part_s[c, keep, :].astype(F32) + near_s[c].astype(F32)).astype(BF16)
        send(remote(chip_s.at[c], far_s.at[c], sum_send.at[1, c], sum_recv.at[1, c], over))

    def full_sum(c):
        remote(far_s.at[c], far_s.at[c], sum_send.at[1, c], sum_recv.at[1, c], over).wait_recv()
        mine = pl.ds(pl.multiple_of(CHUNK * c + core * half, half), half)
        done_s[mine, :] = (res_s[mine, :] + (chip_s[c].astype(F32) + far_s[c].astype(F32))).astype(BF16)
        send(remote(done_s.at[mine, :], done_s.at[mine, :], sum_send.at[2, c], sum_recv.at[2, c], mate))

    def store(c):
        other = pl.ds(pl.multiple_of(CHUNK * c + (1 - core) * half, half), half)
        remote(done_s.at[other, :], done_s.at[other, :], sum_send.at[2, c], sum_recv.at[2, c], mate).wait_recv()
        rows = pl.ds(CHUNK * c, CHUNK)
        copy = pltpu.make_async_copy(done_s.at[rows, :], out_ref.at[rows, :], out_sem.at[c])
        copy.start()
        return copy

    gather_relay(0, mix_s, 0)
    cross_query(0)
    for c in range(1, chunks):
        gather_relay(0, mix_s, c)
    weight_send(1, co_ref, cox_ref, co_s)
    cross_score(0)
    cross_mix(0)
    cross_query(1)
    cross_score(1)
    cross_mix(1)
    cross_query(2)
    cross_score(2)
    gather_relay(1, cmix_s, 0)
    cross_mix(2)
    mlp(0)
    gather_relay(1, cmix_s, 1)
    cross_query(3)
    cross_score(3)
    chip_sum(0)
    gather_relay(1, cmix_s, 2)
    cross_mix(3)
    mlp(1)
    mlp(2)
    chip_sum(1)
    chip_sum(2)
    full_sum(0)
    gather_relay(1, cmix_s, 3)
    mlp(3)
    stores = [store(0)]
    full_sum(1)
    chip_sum(3)
    stores.append(store(1))
    full_sum(2)
    stores.append(store(2))
    full_sum(3)
    stores.append(store(3))
    for copy in stores:
        copy.wait()
    for copy in sends:
        copy.wait_send()


def rest_of_layer(x_in, mixed, w_o, w_o_over, cross_o, cross_o_over, cross_q, gate_t, up_t, w_down, norm_cross, norm_mlp, mask_t, cross_k, cross_v, heads):
    rows, d_model = x_in.shape
    flat = mixed.shape[1]
    d_ff = gate_t.shape[0]
    src_len = cross_k.shape[0]
    chunks = rows // CHUNK
    slots = 3
    anywhere = pl.BlockSpec(memory_space=pl.ANY)
    vmem = pl.BlockSpec(memory_space=pltpu.VMEM)
    dma = pltpu.SemaphoreType.DMA
    return pl.pallas_call(
        functools.partial(rest_kernel, heads, slots),
        in_specs=[anywhere] * 10 + [vmem, vmem] + [anywhere] * 3,
        out_specs=anywhere,
        out_shape=jax.ShapeDtypeStruct((rows, d_model), BF16),
        scratch_shapes=[
            pltpu.VMEM((rows, d_model), BF16),
            pltpu.VMEM((rows, d_model), F32),
            pltpu.VMEM((4, rows, flat), BF16),
            pltpu.VMEM((4, rows, flat), BF16),
            pltpu.VMEM((4 * flat, d_model), BF16),
            pltpu.VMEM((4 * flat, d_model), BF16),
            pltpu.VMEM((d_model, flat), BF16),
            pltpu.VMEM((d_ff, d_model), BF16),
            pltpu.VMEM((d_ff, d_model), BF16),
            pltpu.VMEM((d_ff, d_model), BF16),
            pltpu.VMEM((slots, src_len, flat, CHUNK), BF16),
            pltpu.VMEM((slots, src_len, flat, CHUNK), BF16),
            pltpu.VMEM((src_len, rows), jnp.int32),
            pltpu.VMEM((flat, CHUNK), F32),
            pltpu.VMEM((heads, src_len, CHUNK), F32),
            pltpu.VMEM((CHUNK, d_ff), BF16),
            pltpu.VMEM((chunks, CHUNK, d_model), BF16),
            pltpu.VMEM((chunks, CHUNK // 2, d_model), BF16),
            pltpu.VMEM((chunks, CHUNK // 2, d_model), BF16),
            pltpu.VMEM((chunks, CHUNK // 2, d_model), BF16),
            pltpu.VMEM((rows, d_model), BF16),
            dma((2, 3, chunks)), dma((2, 3, chunks)),
            dma((2, 2)), dma((2, 2)),
            dma((3, chunks)), dma((3, chunks)),
            dma((16,)), dma((2, slots)), dma((chunks,)),
        ],
        compiler_params=pltpu.CompilerParams(collective_id=0, has_side_effects=True, vmem_limit_bytes=VMEM_BYTES),
        cost_estimate=pl.CostEstimate(flops=2 * rows * d_model * (8 * flat + flat + 3 * d_ff), bytes_accessed=50_000_000, transcendentals=rows * d_ff),
        name='rest_of_layer',
    )(x_in, mixed, w_o, w_o_over, cross_o, cross_o_over, cross_q, gate_t, up_t, w_down, norm_cross, norm_mlp, mask_t, cross_k, cross_v)


def solution(mesh):
    def local_layer(x_in, tok_pos, self_k, self_v, cross_k, cross_v, enc_mask, rel_bias, w_q, w_k, w_v, w_o, cross_q, cross_o, w_gate, w_up, w_down, norm_self, norm_cross, norm_mlp):
        rows, t_len, heads, head_dim = self_k.shape
        flat = heads * head_dim
        to_kernel = lambda c: jnp.transpose(c, (0, 2, 3, 1)).reshape(rows, flat, t_len)
        from_kernel = lambda c: jnp.transpose(c.reshape(rows, heads, head_dim, t_len), (0, 3, 1, 2))
        cross_view = lambda c: jnp.transpose(c, (1, 2, 3, 0)).reshape(c.shape[1], flat, rows)
        swap = [(0, 2), (1, 3), (2, 0), (3, 1)]
        w_o_over = lax.ppermute(w_o, 'tp', swap)
        cross_o_over = lax.ppermute(cross_o, 'tp', swap)
        mixed_self, new_k, new_v = self_attention(tok_pos, rel_bias.T, x_in, w_q, w_k, w_v, norm_self, to_kernel(self_k), to_kernel(self_v), heads)
        x_out = rest_of_layer(x_in, mixed_self, w_o, w_o_over, cross_o, cross_o_over, cross_q, w_gate.T, w_up.T, w_down, norm_cross, norm_mlp,
                              enc_mask.T, cross_view(cross_k), cross_view(cross_v), heads)
        return x_out, from_kernel(new_k), from_kernel(new_v)

    cache_spec = P('dp', None, 'tp', None)
    split_cols = P(None, 'tp')
    split_rows = P('tp', None)
    in_specs = (P('dp', None), P('dp'), cache_spec, cache_spec, cache_spec, cache_spec, P('dp', None), split_cols, split_cols, split_cols, split_cols, split_rows, split_cols, split_rows, split_cols, split_cols, split_rows, P(None), P(None), P(None))
    out_specs = (P('dp', None), cache_spec, cache_spec)
    return jax.shard_map(local_layer, mesh=mesh, in_specs=in_specs, out_specs=out_specs, check_vma=False)
```

```python
import functools
import math
import jax
import jax.numpy as jnp
from jax import lax
from jax.experimental import pallas as pl
from jax.experimental.pallas import tpu as pltpu
from jax.sharding import PartitionSpec as P

BUCKET_EDGES = tuple(int(math.ceil(16.0 * 8.0 ** (bucket_step / 16.0))) for bucket_step in range(1, 16))
NEG_FILL = -1e30
STEP_ROWS = 32
SLOTS = 8
AHEAD = 4
VMEM_BYTES = 67043328
LANES = 128
F32 = jnp.float32
BF16 = jnp.bfloat16


def rms_norm(values, norm_scale):
    inv_rms = lax.rsqrt(jnp.mean(values * values, axis=-1, keepdims=True) + 1e-6)
    return (values * inv_rms * norm_scale.astype(F32)).astype(BF16)


def dot(a, b):
    return jnp.dot(a, b, preferred_element_type=F32)


def dot_nt(a, b):
    return lax.dot_general(a, b, (((1,), (1,)), ((), ())), preferred_element_type=F32)


def iota(shape, axis):
    return lax.broadcasted_iota(jnp.int32, shape, axis)


def self_kernel(heads, head_dim, pos_ref, bias_ref, x_ref, wq_ref, wk_ref, wv_ref, norm_ref, k_ref, v_ref,
                mixed_ref, ko_ref, vo_ref, x_s, wq_s, wk_s, wv_s, k_s, v_s, mixed_s, q_s, kt_s, vt_s, score_s, out_s,
                load_sem, in_sem, out_sem, mixed_sem):
    flat = heads * head_dim
    rows_total = x_ref.shape[0]
    n = STEP_ROWS
    steps = rows_total // n

    def rows_of(step):
        return pl.ds(pl.multiple_of(step * n, n), n)

    def fetch(step):
        slot = lax.rem(step, SLOTS)
        return (pltpu.make_async_copy(k_ref.at[rows_of(step)], k_s.at[slot], in_sem.at[0, slot]),
                pltpu.make_async_copy(v_ref.at[rows_of(step)], v_s.at[slot], in_sem.at[1, slot]))

    def write(step):
        slot = lax.rem(step, SLOTS)
        return (pltpu.make_async_copy(k_s.at[slot], ko_ref.at[rows_of(step)], out_sem.at[0, slot]),
                pltpu.make_async_copy(v_s.at[slot], vo_ref.at[rows_of(step)], out_sem.at[1, slot]))

    loads = [pltpu.make_async_copy(src, dst, load_sem.at[i])
             for i, (src, dst) in enumerate(((x_ref, x_s), (wq_ref, wq_s), (wk_ref, wk_s), (wv_ref, wv_s)))]
    for copy in loads:
        copy.start()
    for step in range(AHEAD):
        for copy in fetch(step):
            copy.start()

    lane = iota((4 * heads, LANES), 1)
    head_of = lax.rem(iota((4 * heads, LANES), 0), heads)
    far = jnp.full_like(lane, 16)
    for edge in BUCKET_EDGES:
        far = far + jnp.where(lane >= edge, 1, 0)
    bucket = jnp.where(lane < 16, lane, far)
    table = jnp.zeros((4 * heads, LANES), F32)
    for b in range(32):
        here = jnp.zeros((4 * heads, LANES), F32)
        for h in range(heads):
            here = jnp.where(head_of == h, bias_ref[h, b], here)
        table = jnp.where(bucket == b, here, table)

    for copy in loads:
        copy.wait()

    @pl.loop(0, rows_total // LANES)
    def _(g):
        rows = pl.ds(pl.multiple_of(g * LANES, LANES), LANES)
        normed = rms_norm(x_s[rows, :].astype(F32), norm_ref[...])
        q_s[rows, :] = dot(normed, wq_s[...]).astype(BF16)
        kt_s[g] = dot(normed, wk_s[...]).astype(BF16).astype(F32).T
        vt_s[g] = dot(normed, wv_s[...]).astype(BF16).astype(F32).T

    spread = jnp.where(iota((n * heads, n), 0) // heads == iota((n * heads, n), 1), 1.0, 0.0).astype(BF16)
    gather = jnp.where(iota((n, n * heads), 1) // heads == iota((n, n * heads), 0), 1.0, 0.0).astype(BF16)
    own_head = iota((n * heads, flat), 1) // head_dim == lax.rem(iota((n * heads, flat), 0), heads)
    lane_bf = iota((flat, LANES), 1).astype(F32).astype(BF16)
    quad_row = iota((4 * heads, LANES), 0)
    per = LANES // n

    @pl.loop(0, steps)
    def _(step):
        ahead = step + AHEAD

        @pl.when(ahead < steps)
        def _():
            @pl.when(ahead >= SLOTS)
            def _():
                for copy in write(ahead - SLOTS):
                    copy.wait()
            for copy in fetch(ahead):
                copy.start()

        first = pl.multiple_of(step * n, n)
        slot = lax.rem(step, SLOTS)
        group, part = step // per, lax.rem(step, per)
        shift = lax.rem(LANES - part * n, LANES)
        k_new = pltpu.roll(kt_s[group], shift, 1)
        v_new = pltpu.roll(vt_s[group], shift, 1)
        q_rows = jnp.where(own_head, dot(spread, q_s[pl.ds(first, n), :]), 0.0).astype(BF16)
        in_k, in_v = fetch(step)

        def update(cache, new_cols, b):
            at_pos = lane_bf == pos_ref[first + b].astype(F32).astype(BF16)
            col = jnp.broadcast_to(new_cols[:, b:b + 1], (flat, LANES)).astype(BF16)
            updated = jnp.where(at_pos, col, cache[slot, b])
            cache[slot, b] = updated
            return updated

        in_k.wait()
        for g in range(n // 4):
            lhs = q_rows[4 * heads * g:4 * heads * (g + 1), :]
            picked = None
            distance = None
            for half in range(2):
                b = 4 * g + 2 * half
                pair = jnp.concatenate([update(k_s, k_new, b), update(k_s, k_new, b + 1)], axis=1)
                both = dot(lhs, pair)
                for j in range(2):
                    mine = both[:, LANES * j:LANES * (j + 1)]
                    at = 2 * half + j
                    pos = pos_ref[first + 4 * g + at]
                    picked = mine if picked is None else jnp.where(quad_row >= heads * at, mine, picked)
                    distance = jnp.full((4 * heads, LANES), pos, jnp.int32) if distance is None else jnp.where(quad_row >= heads * at, pos, distance)
            distance = distance - iota((4 * heads, LANES), 1)
            bias = jnp.take_along_axis(table, jnp.maximum(distance, 0), axis=1)
            score_s[4 * heads * g:4 * heads * (g + 1), :] = jnp.where(distance >= 0, picked + bias, NEG_FILL)
        write(step)[0].start()

        scores = score_s[...]
        exps = jnp.exp(scores - jnp.max(scores, axis=1, keepdims=True))
        probs = exps * pl.reciprocal(jnp.sum(exps, axis=1, keepdims=True))

        in_v.wait()
        for g in range(n // 4):
            quad = probs[4 * heads * g:4 * heads * (g + 1), :]
            picked = None
            for half in range(2):
                b = 4 * g + 2 * half
                pair = jnp.concatenate([update(v_s, v_new, b), update(v_s, v_new, b + 1)], axis=1)
                low = jnp.where(quad_row // heads == 2 * half, quad, 0.0)
                high = jnp.where(quad_row // heads == 2 * half + 1, quad, 0.0)
                lhs = jnp.concatenate([low, high], axis=1).astype(BF16)
                both = dot_nt(lhs, pair)
                picked = both if half == 0 else jnp.where(iota(both.shape, 0) >= 2 * heads, both, picked)
            out_s[4 * heads * g:4 * heads * (g + 1), :] = picked
        write(step)[1].start()
        mixed_s[pl.ds(first, n), :] = dot(gather, jnp.where(own_head, out_s[...], 0.0).astype(BF16)).astype(BF16)

    mixed_copy = pltpu.make_async_copy(mixed_s, mixed_ref, mixed_sem)
    mixed_copy.start()
    for step in range(steps - SLOTS, steps):
        for copy in write(step):
            copy.wait()
    mixed_copy.wait()


def self_attention(tok_pos, bias_t, x_in, w_q, w_k, w_v, norm_self, keys, values, heads):
    rows, flat, t_len = keys.shape
    d_model = x_in.shape[1]
    n = STEP_ROWS
    smem = pl.BlockSpec(memory_space=pltpu.SMEM)
    anywhere = pl.BlockSpec(memory_space=pl.ANY)
    cache_shape = jax.ShapeDtypeStruct(keys.shape, BF16)
    return pl.pallas_call(
        functools.partial(self_kernel, heads, flat // heads),
        in_specs=[smem, smem] + [anywhere] * 4 + [pl.BlockSpec(memory_space=pltpu.VMEM)] + [anywhere] * 2,
        out_specs=[anywhere] * 3,
        out_shape=[jax.ShapeDtypeStruct((rows, flat), BF16), cache_shape, cache_shape],
        scratch_shapes=[
            pltpu.VMEM((rows, d_model), BF16),
            pltpu.VMEM((d_model, flat), BF16),
            pltpu.VMEM((d_model, flat), BF16),
            pltpu.VMEM((d_model, flat), BF16),
            pltpu.VMEM((SLOTS, n, flat, t_len), BF16),
            pltpu.VMEM((SLOTS, n, flat, t_len), BF16),
            pltpu.VMEM((rows, flat), BF16),
            pltpu.VMEM((rows, flat), BF16),
            pltpu.VMEM((rows // LANES, flat, LANES), F32),
            pltpu.VMEM((rows // LANES, flat, LANES), F32),
            pltpu.VMEM((n * heads, LANES), F32),
            pltpu.VMEM((n * heads, flat), F32),
            pltpu.SemaphoreType.DMA((4,)),
            pltpu.SemaphoreType.DMA((2, SLOTS)),
            pltpu.SemaphoreType.DMA((2, SLOTS)),
            pltpu.SemaphoreType.DMA,
        ],
        compiler_params=pltpu.CompilerParams(vmem_limit_bytes=VMEM_BYTES),
        cost_estimate=pl.CostEstimate(flops=4 * rows * flat * t_len * 16 + 6 * rows * d_model * flat, bytes_accessed=8 * rows * flat * t_len, transcendentals=rows * heads * t_len),
        name='self_attention',
    )(tok_pos, bias_t, x_in, w_q, w_k, w_v, norm_self, keys, values)


CHUNK = 128
MESH = pl.DeviceIdType.MESH


def rest_kernel(heads, n_cross_slots,
                x_ref, mixed_ref, wo_ref, wox_ref, co_ref, cox_ref, cq_ref, gate_ref, up_ref, down_ref, norm_c_ref, norm_m_ref,
                mask_ref, ck_ref, cv_ref, out_ref,
                x_s, res_s, mix_s, cmix_s, wo_s, co_s, cq_s, gate_s, up_s, down_s, k_s, v_s, mask_s,
                qt_s, score_s, hid_s, part_s, near_s, chip_s, far_s, done_s,
                ag_send, ag_recv, w_send, w_recv, sum_send, sum_recv, load_sem, cross_sem, out_sem):
    me = lax.axis_index('tp')
    core = lax.rem(me, 2)
    mate = me + 1 - 2 * core
    over = lax.rem(me + 2, 4)
    cater = lax.rem(mate + 2, 4)
    rows_total, d_model = x_ref.shape
    flat = mixed_ref.shape[1]
    head_dim = flat // heads
    src_len = ck_ref.shape[0]
    d_ff = gate_ref.shape[0]
    chunks = rows_total // CHUNK
    half = CHUNK // 2

    def remote(src, dst, send_sem, recv_sem, to):
        return pltpu.make_async_remote_copy(src_ref=src, dst_ref=dst, send_sem=send_sem, recv_sem=recv_sem,
                                            device_id={'tp': to}, device_id_type=MESH)

    def block(buf, who, c):
        return buf.at[who, pl.ds(CHUNK * c, CHUNK), :]

    def shard(buf, who):
        return buf.at[pl.ds(pl.multiple_of(who * flat, flat), flat), :]

    loads = []

    def load(src, dst):
        copy = pltpu.make_async_copy(src, dst, load_sem.at[len(loads)])
        copy.start()
        loads.append(copy)
        return copy

    def cross_load(c):
        slot = c % n_cross_slots
        cols = pl.ds(CHUNK * c, CHUNK)
        return (pltpu.make_async_copy(ck_ref.at[:, :, cols], k_s.at[slot], cross_sem.at[0, slot]),
                pltpu.make_async_copy(cv_ref.at[:, :, cols], v_s.at[slot], cross_sem.at[1, slot]))

    def cross_start(c):
        for copy in cross_load(c):
            copy.start()

    barrier = pltpu.get_barrier_semaphore()
    for peer in (mate, over):
        pl.semaphore_signal(barrier, inc=1, device_id={'tp': peer}, device_id_type=MESH)
    pl.semaphore_wait(barrier, 2)

    sends = []

    def send(copy):
        copy.start()
        sends.append(copy)

    def gather_send(stage, src, buf, c):
        send(remote(src, block(buf, me, c), ag_send.at[stage, 0, c], ag_recv.at[stage, 0, c], over))
        send(remote(src, block(buf, me, c), ag_send.at[stage, 1, c], ag_recv.at[stage, 1, c], mate))

    def gather_relay(stage, buf, c):
        remote(block(buf, over, c), block(buf, over, c), ag_send.at[stage, 0, c], ag_recv.at[stage, 0, c], over).wait_recv()
        send(remote(block(buf, over, c), block(buf, over, c), ag_send.at[stage, 2, c], ag_recv.at[stage, 2, c], mate))

    def gather_wait(stage, buf, c):
        remote(block(buf, mate, c), block(buf, mate, c), ag_send.at[stage, 1, c], ag_recv.at[stage, 1, c], mate).wait_recv()
        remote(block(buf, cater, c), block(buf, cater, c), ag_send.at[stage, 2, c], ag_recv.at[stage, 2, c], mate).wait_recv()

    def weight_send(which, ref, ref_x, buf):
        send(remote(ref, shard(buf, me), w_send.at[which, 0], w_recv.at[which, 0], mate))
        send(remote(ref_x, shard(buf, over), w_send.at[which, 1], w_recv.at[which, 1], mate))

    def weight_wait(which, buf):
        remote(shard(buf, mate), shard(buf, mate), w_send.at[which, 0], w_recv.at[which, 0], mate).wait_recv()
        remote(shard(buf, cater), shard(buf, cater), w_send.at[which, 1], w_recv.at[which, 1], mate).wait_recv()

    for c in range(chunks):
        gather_send(0, mixed_ref.at[pl.ds(CHUNK * c, CHUNK), :], mix_s, c)
    own_mixed = load(mixed_ref, mix_s.at[me])
    own_wo = (load(wo_ref, shard(wo_s, me)), load(wox_ref, shard(wo_s, over)))
    x_load = load(x_ref, x_s)
    q_load = load(cq_ref, cq_s)
    mask_load = load(mask_ref, mask_s)
    weight_send(0, wo_ref, wox_ref, wo_s)
    cross_start(0)

    def project_heads(buf, weight, c, add_to):
        lhs = jnp.concatenate([buf[i, CHUNK * c:CHUNK * (c + 1), :] for i in range(4)], axis=1)
        for n in range(0, d_model, 512):
            res_s[CHUNK * c:CHUNK * (c + 1), n:n + 512] = add_to[CHUNK * c:CHUNK * (c + 1), n:n + 512].astype(F32) + dot(lhs, weight[:, n:n + 512])

    def cross_query(c):
        if c == 0:
            own_mixed.wait()
            x_load.wait()
            for copy in own_wo:
                copy.wait()
        gather_wait(0, mix_s, c)
        if c == 0:
            weight_wait(0, wo_s)
            q_load.wait()
        project_heads(mix_s, wo_s, c, x_s)
        normed = rms_norm(res_s[CHUNK * c:CHUNK * (c + 1), :], norm_c_ref[...])
        qt_s[...] = dot(normed, cq_s[...]).astype(BF16).astype(F32).T

    def cross_score(c):
        slot = c % n_cross_slots
        for copy in cross_load(c):
            copy.wait()
        if c == 0:
            mask_load.wait()
        step = 8

        @pl.loop(0, src_len // step)
        def _(i):
            at = pl.ds(pl.multiple_of(i * step, step), step)
            for h in range(heads):
                d = slice(head_dim * h, head_dim * (h + 1))
                score_s[h, at, :] = jnp.sum(k_s[slot, at, d, :].astype(F32) * qt_s[d, :][None], axis=1)

    def cross_mix(c):
        slot = c % n_cross_slots
        step = 8
        valid = mask_s[:, CHUNK * c:CHUNK * (c + 1)] != 0
        for h in range(heads):
            scores = jnp.where(valid, score_s[h], NEG_FILL)
            exps = jnp.exp(scores - jnp.max(scores, axis=0, keepdims=True))
            probs = exps * pl.reciprocal(jnp.sum(exps, axis=0, keepdims=True))
            score_s[h] = probs.astype(BF16).astype(F32)

        def mix(i, acc):
            acc = list(acc)
            for j in range(step):
                s = i * step + j
                for h in range(heads):
                    d = slice(head_dim * h, head_dim * (h + 1))
                    acc[h] = acc[h] + v_s[slot, s, d, :].astype(F32) * score_s[h, pl.ds(s, 1), :]
            return tuple(acc)

        zero = jnp.zeros((head_dim, CHUNK), F32)
        acc = lax.fori_loop(0, src_len // step, mix, (zero,) * heads)
        cmix_s[me, CHUNK * c:CHUNK * (c + 1), :] = jnp.concatenate(acc, axis=0).T.astype(BF16)
        gather_send(1, block(cmix_s, me, c), cmix_s, c)

    def mlp(c):
        if c == 0:
            for copy in own_co:
                copy.wait()
            weight_wait(1, co_s)
        gather_wait(1, cmix_s, c)
        project_heads(cmix_s, co_s, c, res_s)
        if c == 0:
            for copy in mlp_loads:
                copy.wait()
        normed = rms_norm(res_s[CHUNK * c:CHUNK * (c + 1), :], norm_m_ref[...])
        for n in range(0, d_ff, 256):
            end = min(d_ff, n + 256)
            gate = dot_nt(normed, gate_s[n:end, :])
            up = dot_nt(normed, up_s[n:end, :])
            hid_s[:, n:end] = (jax.nn.gelu(gate, approximate=True) * up).astype(BF16)
        hidden = hid_s[...]
        for n in range(0, d_model, 512):
            part_s[c, :, n:n + 512] = dot(hidden, down_s[:, n:n + 512]).astype(BF16)
        give = pl.ds(pl.multiple_of((1 - core) * half, half), half)
        send(remote(part_s.at[c, give, :], near_s.at[c], sum_send.at[0, c], sum_recv.at[0, c], mate))

    keep = pl.ds(pl.multiple_of(core * half, half), half)

    def chip_sum(c):
        remote(near_s.at[c], near_s.at[c], sum_send.at[0, c], sum_recv.at[0, c], mate).wait_recv()
        chip_s[c] = (part_s[c, keep, :].astype(F32) + near_s[c].astype(F32)).astype(BF16)
        send(remote(chip_s.at[c], far_s.at[c], sum_send.at[1, c], sum_recv.at[1, c], over))

    def full_sum(c):
        remote(far_s.at[c], far_s.at[c], sum_send.at[1, c], sum_recv.at[1, c], over).wait_recv()
        mine = pl.ds(pl.multiple_of(CHUNK * c + core * half, half), half)
        done_s[mine, :] = (res_s[mine, :] + (chip_s[c].astype(F32) + far_s[c].astype(F32))).astype(BF16)
        send(remote(done_s.at[mine, :], done_s.at[mine, :], sum_send.at[2, c], sum_recv.at[2, c], mate))

    def store(c):
        other = pl.ds(pl.multiple_of(CHUNK * c + (1 - core) * half, half), half)
        remote(done_s.at[other, :], done_s.at[other, :], sum_send.at[2, c], sum_recv.at[2, c], mate).wait_recv()
        rows = pl.ds(CHUNK * c, CHUNK)
        copy = pltpu.make_async_copy(done_s.at[rows, :], out_ref.at[rows, :], out_sem.at[c])
        copy.start()
        return copy

    gather_relay(0, mix_s, 0)
    cross_query(0)
    for c in range(1, chunks):
        gather_relay(0, mix_s, c)
    cross_start(1)
    cross_score(0)
    cross_mix(0)
    weight_send(1, co_ref, cox_ref, co_s)
    own_co = (load(co_ref, shard(co_s, me)), load(cox_ref, shard(co_s, over)))
    cross_start(2)
    cross_query(1)
    cross_score(1)
    cross_mix(1)
    mlp_loads = (load(gate_ref, gate_s), load(up_ref, up_s), load(down_ref, down_s))
    cross_query(2)
    cross_score(2)
    gather_relay(1, cmix_s, 0)
    cross_mix(2)
    cross_start(3)
    mlp(0)
    gather_relay(1, cmix_s, 1)
    cross_query(3)
    cross_score(3)
    chip_sum(0)
    gather_relay(1, cmix_s, 2)
    cross_mix(3)
    mlp(1)
    mlp(2)
    chip_sum(1)
    chip_sum(2)
    full_sum(0)
    gather_relay(1, cmix_s, 3)
    mlp(3)
    stores = [store(0)]
    full_sum(1)
    chip_sum(3)
    stores.append(store(1))
    full_sum(2)
    stores.append(store(2))
    full_sum(3)
    stores.append(store(3))
    for copy in stores:
        copy.wait()
    for copy in sends:
        copy.wait_send()


def rest_of_layer(x_in, mixed, w_o, w_o_over, cross_o, cross_o_over, cross_q, gate_t, up_t, w_down, norm_cross, norm_mlp, mask_t, cross_k, cross_v, heads):
    rows, d_model = x_in.shape
    flat = mixed.shape[1]
    d_ff = gate_t.shape[0]
    src_len = cross_k.shape[0]
    chunks = rows // CHUNK
    slots = 3
    anywhere = pl.BlockSpec(memory_space=pl.ANY)
    vmem = pl.BlockSpec(memory_space=pltpu.VMEM)
    dma = pltpu.SemaphoreType.DMA
    return pl.pallas_call(
        functools.partial(rest_kernel, heads, slots),
        in_specs=[anywhere] * 10 + [vmem, vmem] + [anywhere] * 3,
        out_specs=anywhere,
        out_shape=jax.ShapeDtypeStruct((rows, d_model), BF16),
        scratch_shapes=[
            pltpu.VMEM((rows, d_model), BF16),
            pltpu.VMEM((rows, d_model), F32),
            pltpu.VMEM((4, rows, flat), BF16),
            pltpu.VMEM((4, rows, flat), BF16),
            pltpu.VMEM((4 * flat, d_model), BF16),
            pltpu.VMEM((4 * flat, d_model), BF16),
            pltpu.VMEM((d_model, flat), BF16),
            pltpu.VMEM((d_ff, d_model), BF16),
            pltpu.VMEM((d_ff, d_model), BF16),
            pltpu.VMEM((d_ff, d_model), BF16),
            pltpu.VMEM((slots, src_len, flat, CHUNK), BF16),
            pltpu.VMEM((slots, src_len, flat, CHUNK), BF16),
            pltpu.VMEM((src_len, rows), jnp.int32),
            pltpu.VMEM((flat, CHUNK), F32),
            pltpu.VMEM((heads, src_len, CHUNK), F32),
            pltpu.VMEM((CHUNK, d_ff), BF16),
            pltpu.VMEM((chunks, CHUNK, d_model), BF16),
            pltpu.VMEM((chunks, CHUNK // 2, d_model), BF16),
            pltpu.VMEM((chunks, CHUNK // 2, d_model), BF16),
            pltpu.VMEM((chunks, CHUNK // 2, d_model), BF16),
            pltpu.VMEM((rows, d_model), BF16),
            dma((2, 3, chunks)), dma((2, 3, chunks)),
            dma((2, 2)), dma((2, 2)),
            dma((3, chunks)), dma((3, chunks)),
            dma((16,)), dma((2, slots)), dma((chunks,)),
        ],
        compiler_params=pltpu.CompilerParams(collective_id=0, has_side_effects=True, vmem_limit_bytes=VMEM_BYTES),
        cost_estimate=pl.CostEstimate(flops=2 * rows * d_model * (8 * flat + flat + 3 * d_ff), bytes_accessed=50_000_000, transcendentals=rows * d_ff),
        name='rest_of_layer',
    )(x_in, mixed, w_o, w_o_over, cross_o, cross_o_over, cross_q, gate_t, up_t, w_down, norm_cross, norm_mlp, mask_t, cross_k, cross_v)


def solution(mesh):
    def local_layer(x_in, tok_pos, self_k, self_v, cross_k, cross_v, enc_mask, rel_bias, w_q, w_k, w_v, w_o, cross_q, cross_o, w_gate, w_up, w_down, norm_self, norm_cross, norm_mlp):
        rows, t_len, heads, head_dim = self_k.shape
        flat = heads * head_dim
        to_kernel = lambda c: jnp.transpose(c, (0, 2, 3, 1)).reshape(rows, flat, t_len)
        from_kernel = lambda c: jnp.transpose(c.reshape(rows, heads, head_dim, t_len), (0, 3, 1, 2))
        cross_view = lambda c: jnp.transpose(c, (1, 2, 3, 0)).reshape(c.shape[1], flat, rows)
        swap = [(0, 2), (1, 3), (2, 0), (3, 1)]
        w_o_over = lax.ppermute(w_o, 'tp', swap)
        cross_o_over = lax.ppermute(cross_o, 'tp', swap)
        mixed_self, new_k, new_v = self_attention(tok_pos, rel_bias.T, x_in, w_q, w_k, w_v, norm_self, to_kernel(self_k), to_kernel(self_v), heads)
        x_out = rest_of_layer(x_in, mixed_self, w_o, w_o_over, cross_o, cross_o_over, cross_q, w_gate.T, w_up.T, w_down, norm_cross, norm_mlp,
                              enc_mask.T, cross_view(cross_k), cross_view(cross_v), heads)
        return x_out, from_kernel(new_k), from_kernel(new_v)

    cache_spec = P('dp', None, 'tp', None)
    split_cols = P(None, 'tp')
    split_rows = P('tp', None)
    in_specs = (P('dp', None), P('dp'), cache_spec, cache_spec, cache_spec, cache_spec, P('dp', None), split_cols, split_cols, split_cols, split_cols, split_rows, split_cols, split_rows, split_cols, split_cols, split_rows, P(None), P(None), P(None))
    out_specs = (P('dp', None), cache_spec, cache_spec)
    return jax.shard_map(local_layer, mesh=mesh, in_specs=in_specs, out_specs=out_specs, check_vma=False)
```

```python
import functools
import math
import jax
import jax.numpy as jnp
from jax import lax
from jax.experimental import pallas as pl
from jax.experimental.pallas import tpu as pltpu
from jax.sharding import PartitionSpec as P

BUCKET_EDGES = tuple(int(math.ceil(16.0 * 8.0 ** (bucket_step / 16.0))) for bucket_step in range(1, 16))
NEG_FILL = -1e30
STEP_ROWS = 16
SLOTS = 16
AHEAD = 8
VMEM_BYTES = 67043328
LANES = 128
F32 = jnp.float32
BF16 = jnp.bfloat16


def rms_norm(values, norm_scale):
    inv_rms = lax.rsqrt(jnp.mean(values * values, axis=-1, keepdims=True) + 1e-6)
    return (values * inv_rms * norm_scale.astype(F32)).astype(BF16)


def dot(a, b):
    return jnp.dot(a, b, preferred_element_type=F32)


def dot_nt(a, b):
    return lax.dot_general(a, b, (((1,), (1,)), ((), ())), preferred_element_type=F32)


def iota(shape, axis):
    return lax.broadcasted_iota(jnp.int32, shape, axis)


def self_kernel(heads, head_dim, pos_ref, bias_ref, x_ref, wq_ref, wk_ref, wv_ref, norm_ref, k_ref, v_ref,
                mixed_ref, ko_ref, vo_ref, x_s, wq_s, wk_s, wv_s, k_s, v_s, mixed_s, q_s, kt_s, vt_s, score_s, out_s,
                load_sem, in_sem, out_sem, mixed_sem):
    flat = heads * head_dim
    rows_total = x_ref.shape[0]
    n = STEP_ROWS
    steps = rows_total // n

    def rows_of(step):
        return pl.ds(pl.multiple_of(step * n, n), n)

    def fetch(step):
        slot = lax.rem(step, SLOTS)
        return (pltpu.make_async_copy(k_ref.at[rows_of(step)], k_s.at[slot], in_sem.at[0, slot]),
                pltpu.make_async_copy(v_ref.at[rows_of(step)], v_s.at[slot], in_sem.at[1, slot]))

    def write(step):
        slot = lax.rem(step, SLOTS)
        return (pltpu.make_async_copy(k_s.at[slot], ko_ref.at[rows_of(step)], out_sem.at[0, slot]),
                pltpu.make_async_copy(v_s.at[slot], vo_ref.at[rows_of(step)], out_sem.at[1, slot]))

    loads = [pltpu.make_async_copy(src, dst, load_sem.at[i])
             for i, (src, dst) in enumerate(((x_ref, x_s), (wq_ref, wq_s), (wk_ref, wk_s), (wv_ref, wv_s)))]
    for copy in loads:
        copy.start()
    for step in range(AHEAD):
        for copy in fetch(step):
            copy.start()

    lane = iota((4 * heads, LANES), 1)
    head_of = lax.rem(iota((4 * heads, LANES), 0), heads)
    far = jnp.full_like(lane, 16)
    for edge in BUCKET_EDGES:
        far = far + jnp.where(lane >= edge, 1, 0)
    bucket = jnp.where(lane < 16, lane, far)
    table = jnp.zeros((4 * heads, LANES), F32)
    for b in range(32):
        here = jnp.zeros((4 * heads, LANES), F32)
        for h in range(heads):
            here = jnp.where(head_of == h, bias_ref[h, b], here)
        table = jnp.where(bucket == b, here, table)

    for copy in loads:
        copy.wait()

    @pl.loop(0, rows_total // LANES)
    def _(g):
        rows = pl.ds(pl.multiple_of(g * LANES, LANES), LANES)
        normed = rms_norm(x_s[rows, :].astype(F32), norm_ref[...])
        q_s[rows, :] = dot(normed, wq_s[...]).astype(BF16)
        kt_s[g] = dot(normed, wk_s[...]).astype(BF16).astype(F32).T
        vt_s[g] = dot(normed, wv_s[...]).astype(BF16).astype(F32).T

    spread = jnp.where(iota((n * heads, n), 0) // heads == iota((n * heads, n), 1), 1.0, 0.0).astype(BF16)
    gather = jnp.where(iota((n, n * heads), 1) // heads == iota((n, n * heads), 0), 1.0, 0.0).astype(BF16)
    own_head = iota((n * heads, flat), 1) // head_dim == lax.rem(iota((n * heads, flat), 0), heads)
    lane_bf = iota((flat, LANES), 1).astype(F32).astype(BF16)
    quad_row = iota((4 * heads, LANES), 0)
    per = LANES // n

    @pl.loop(0, steps)
    def _(step):
        ahead = step + AHEAD

        @pl.when(ahead < steps)
        def _():
            @pl.when(ahead >= SLOTS)
            def _():
                for copy in write(ahead - SLOTS):
                    copy.wait()
            for copy in fetch(ahead):
                copy.start()

        first = pl.multiple_of(step * n, n)
        slot = lax.rem(step, SLOTS)
        group, part = step // per, lax.rem(step, per)
        shift = lax.rem(LANES - part * n, LANES)
        k_new = pltpu.roll(kt_s[group], shift, 1)
        v_new = pltpu.roll(vt_s[group], shift, 1)
        q_rows = jnp.where(own_head, dot(spread, q_s[pl.ds(first, n), :]), 0.0).astype(BF16)
        in_k, in_v = fetch(step)

        def update(cache, new_cols, b):
            at_pos = lane_bf == pos_ref[first + b].astype(F32).astype(BF16)
            col = jnp.broadcast_to(new_cols[:, b:b + 1], (flat, LANES)).astype(BF16)
            updated = jnp.where(at_pos, col, cache[slot, b])
            cache[slot, b] = updated
            return updated

        in_k.wait()
        for g in range(n // 4):
            lhs = q_rows[4 * heads * g:4 * heads * (g + 1), :]
            picked = None
            distance = None
            for half in range(2):
                b = 4 * g + 2 * half
                pair = jnp.concatenate([update(k_s, k_new, b), update(k_s, k_new, b + 1)], axis=1)
                both = dot(lhs, pair)
                for j in range(2):
                    mine = both[:, LANES * j:LANES * (j + 1)]
                    at = 2 * half + j
                    pos = pos_ref[first + 4 * g + at]
                    picked = mine if picked is None else jnp.where(quad_row >= heads * at, mine, picked)
                    distance = jnp.full((4 * heads, LANES), pos, jnp.int32) if distance is None else jnp.where(quad_row >= heads * at, pos, distance)
            distance = distance - iota((4 * heads, LANES), 1)
            bias = jnp.take_along_axis(table, jnp.maximum(distance, 0), axis=1)
            score_s[4 * heads * g:4 * heads * (g + 1), :] = jnp.where(distance >= 0, picked + bias, NEG_FILL)
        write(step)[0].start()

        scores = score_s[...]
        exps = jnp.exp(scores - jnp.max(scores, axis=1, keepdims=True))
        probs = exps * pl.reciprocal(jnp.sum(exps, axis=1, keepdims=True))

        in_v.wait()
        for g in range(n // 4):
            quad = probs[4 * heads * g:4 * heads * (g + 1), :]
            picked = None
            for half in range(2):
                b = 4 * g + 2 * half
                pair = jnp.concatenate([update(v_s, v_new, b), update(v_s, v_new, b + 1)], axis=1)
                low = jnp.where(quad_row // heads == 2 * half, quad, 0.0)
                high = jnp.where(quad_row // heads == 2 * half + 1, quad, 0.0)
                lhs = jnp.concatenate([low, high], axis=1).astype(BF16)
                both = dot_nt(lhs, pair)
                picked = both if half == 0 else jnp.where(iota(both.shape, 0) >= 2 * heads, both, picked)
            out_s[4 * heads * g:4 * heads * (g + 1), :] = picked
        write(step)[1].start()
        mixed_s[pl.ds(first, n), :] = dot(gather, jnp.where(own_head, out_s[...], 0.0).astype(BF16)).astype(BF16)

    mixed_copy = pltpu.make_async_copy(mixed_s, mixed_ref, mixed_sem)
    mixed_copy.start()
    for step in range(steps - SLOTS, steps):
        for copy in write(step):
            copy.wait()
    mixed_copy.wait()


def self_attention(tok_pos, bias_t, x_in, w_q, w_k, w_v, norm_self, keys, values, heads):
    rows, flat, t_len = keys.shape
    d_model = x_in.shape[1]
    n = STEP_ROWS
    smem = pl.BlockSpec(memory_space=pltpu.SMEM)
    anywhere = pl.BlockSpec(memory_space=pl.ANY)
    cache_shape = jax.ShapeDtypeStruct(keys.shape, BF16)
    return pl.pallas_call(
        functools.partial(self_kernel, heads, flat // heads),
        in_specs=[smem, smem] + [anywhere] * 4 + [pl.BlockSpec(memory_space=pltpu.VMEM)] + [anywhere] * 2,
        out_specs=[anywhere] * 3,
        out_shape=[jax.ShapeDtypeStruct((rows, flat), BF16), cache_shape, cache_shape],
        scratch_shapes=[
            pltpu.VMEM((rows, d_model), BF16),
            pltpu.VMEM((d_model, flat), BF16),
            pltpu.VMEM((d_model, flat), BF16),
            pltpu.VMEM((d_model, flat), BF16),
            pltpu.VMEM((SLOTS, n, flat, t_len), BF16),
            pltpu.VMEM((SLOTS, n, flat, t_len), BF16),
            pltpu.VMEM((rows, flat), BF16),
            pltpu.VMEM((rows, flat), BF16),
            pltpu.VMEM((rows // LANES, flat, LANES), F32),
            pltpu.VMEM((rows // LANES, flat, LANES), F32),
            pltpu.VMEM((n * heads, LANES), F32),
            pltpu.VMEM((n * heads, flat), F32),
            pltpu.SemaphoreType.DMA((4,)),
            pltpu.SemaphoreType.DMA((2, SLOTS)),
            pltpu.SemaphoreType.DMA((2, SLOTS)),
            pltpu.SemaphoreType.DMA,
        ],
        compiler_params=pltpu.CompilerParams(vmem_limit_bytes=VMEM_BYTES),
        cost_estimate=pl.CostEstimate(flops=4 * rows * flat * t_len * 16 + 6 * rows * d_model * flat, bytes_accessed=8 * rows * flat * t_len, transcendentals=rows * heads * t_len),
        name='self_attention',
    )(tok_pos, bias_t, x_in, w_q, w_k, w_v, norm_self, keys, values)


CHUNK = 128
MESH = pl.DeviceIdType.MESH


def rest_kernel(heads, n_cross_slots,
                x_ref, mixed_ref, wo_ref, wox_ref, co_ref, cox_ref, cq_ref, gate_ref, up_ref, down_ref, norm_c_ref, norm_m_ref,
                mask_ref, ck_ref, cv_ref, out_ref,
                x_s, res_s, mix_s, cmix_s, wo_s, co_s, cq_s, gate_s, up_s, gate_t, up_t, down_s, k_s, v_s, mask_s,
                qt_s, score_s, hid_s, part_s, near_s, chip_s, far_s, done_s,
                ag_send, ag_recv, w_send, w_recv, sum_send, sum_recv, load_sem, cross_sem, out_sem):
    me = lax.axis_index('tp')
    core = lax.rem(me, 2)
    mate = me + 1 - 2 * core
    over = lax.rem(me + 2, 4)
    cater = lax.rem(mate + 2, 4)
    rows_total, d_model = x_ref.shape
    flat = mixed_ref.shape[1]
    head_dim = flat // heads
    src_len = ck_ref.shape[0]
    d_ff = gate_ref.shape[0]
    chunks = rows_total // CHUNK
    half = CHUNK // 2

    def remote(src, dst, send_sem, recv_sem, to):
        return pltpu.make_async_remote_copy(src_ref=src, dst_ref=dst, send_sem=send_sem, recv_sem=recv_sem,
                                            device_id={'tp': to}, device_id_type=MESH)

    def block(buf, who, c):
        return buf.at[who, pl.ds(CHUNK * c, CHUNK), :]

    def shard(buf, who):
        return buf.at[pl.ds(pl.multiple_of(who * flat, flat), flat), :]

    loads = []

    def load(src, dst):
        copy = pltpu.make_async_copy(src, dst, load_sem.at[len(loads)])
        copy.start()
        loads.append(copy)
        return copy

    def cross_load(c):
        slot = c % n_cross_slots
        cols = pl.ds(CHUNK * c, CHUNK)
        return (pltpu.make_async_copy(ck_ref.at[:, :, cols], k_s.at[slot], cross_sem.at[0, slot]),
                pltpu.make_async_copy(cv_ref.at[:, :, cols], v_s.at[slot], cross_sem.at[1, slot]))

    def cross_start(c):
        for copy in cross_load(c):
            copy.start()

    barrier = pltpu.get_barrier_semaphore()
    for peer in (mate, over):
        pl.semaphore_signal(barrier, inc=1, device_id={'tp': peer}, device_id_type=MESH)
    pl.semaphore_wait(barrier, 2)

    sends = []

    def send(copy):
        copy.start()
        sends.append(copy)

    def gather_send(stage, src, buf, c):
        send(remote(src, block(buf, me, c), ag_send.at[stage, 0, c], ag_recv.at[stage, 0, c], over))
        send(remote(src, block(buf, me, c), ag_send.at[stage, 1, c], ag_recv.at[stage, 1, c], mate))

    def gather_relay(stage, buf, c):
        remote(block(buf, over, c), block(buf, over, c), ag_send.at[stage, 0, c], ag_recv.at[stage, 0, c], over).wait_recv()
        send(remote(block(buf, over, c), block(buf, over, c), ag_send.at[stage, 2, c], ag_recv.at[stage, 2, c], mate))

    def gather_wait(stage, buf, c):
        remote(block(buf, mate, c), block(buf, mate, c), ag_send.at[stage, 1, c], ag_recv.at[stage, 1, c], mate).wait_recv()
        remote(block(buf, cater, c), block(buf, cater, c), ag_send.at[stage, 2, c], ag_recv.at[stage, 2, c], mate).wait_recv()

    def weight_send(which, ref, ref_x, buf):
        send(remote(ref, shard(buf, me), w_send.at[which, 0], w_recv.at[which, 0], mate))
        send(remote(ref_x, shard(buf, over), w_send.at[which, 1], w_recv.at[which, 1], mate))

    def weight_wait(which, buf):
        remote(shard(buf, mate), shard(buf, mate), w_send.at[which, 0], w_recv.at[which, 0], mate).wait_recv()
        remote(shard(buf, cater), shard(buf, cater), w_send.at[which, 1], w_recv.at[which, 1], mate).wait_recv()

    for c in range(chunks):
        gather_send(0, mixed_ref.at[pl.ds(CHUNK * c, CHUNK), :], mix_s, c)
    own_mixed = load(mixed_ref, mix_s.at[me])
    own_wo = (load(wo_ref, shard(wo_s, me)), load(wox_ref, shard(wo_s, over)))
    x_load = load(x_ref, x_s)
    q_load = load(cq_ref, cq_s)
    mask_load = load(mask_ref, mask_s)
    weight_send(0, wo_ref, wox_ref, wo_s)
    gate_load = load(gate_ref, gate_s)
    up_load = load(up_ref, up_s)
    cross_start(0)

    def turn(wide, tall):
        @pl.loop(0, d_model // CHUNK)
        def _(i):
            at = pl.ds(pl.multiple_of(i * CHUNK, CHUNK), CHUNK)
            tall[at, :] = wide[:, at].T

    def project_heads(buf, weight, c, add_to):
        lhs = jnp.concatenate([buf[i, CHUNK * c:CHUNK * (c + 1), :] for i in range(4)], axis=1)
        for n in range(0, d_model, 512):
            res_s[CHUNK * c:CHUNK * (c + 1), n:n + 512] = add_to[CHUNK * c:CHUNK * (c + 1), n:n + 512].astype(F32) + dot(lhs, weight[:, n:n + 512])

    def cross_query(c):
        if c == 0:
            own_mixed.wait()
            x_load.wait()
            for copy in own_wo:
                copy.wait()
        gather_wait(0, mix_s, c)
        if c == 0:
            weight_wait(0, wo_s)
            q_load.wait()
        project_heads(mix_s, wo_s, c, x_s)
        normed = rms_norm(res_s[CHUNK * c:CHUNK * (c + 1), :], norm_c_ref[...])
        qt_s[...] = dot(normed, cq_s[...]).astype(BF16).astype(F32).T

    def cross_score(c):
        slot = c % n_cross_slots
        for copy in cross_load(c):
            copy.wait()
        if c == 0:
            mask_load.wait()
        step = 8

        @pl.loop(0, src_len // step)
        def _(i):
            at = pl.ds(pl.multiple_of(i * step, step), step)
            for h in range(heads):
                d = slice(head_dim * h, head_dim * (h + 1))
                score_s[h, at, :] = jnp.sum(k_s[slot, at, d, :].astype(F32) * qt_s[d, :][None], axis=1)

    def cross_mix(c):
        slot = c % n_cross_slots
        step = 8
        valid = mask_s[:, CHUNK * c:CHUNK * (c + 1)] != 0
        for h in range(heads):
            scores = jnp.where(valid, score_s[h], NEG_FILL)
            exps = jnp.exp(scores - jnp.max(scores, axis=0, keepdims=True))
            probs = exps * pl.reciprocal(jnp.sum(exps, axis=0, keepdims=True))
            score_s[h] = probs.astype(BF16).astype(F32)

        def mix(i, acc):
            acc = list(acc)
            for j in range(step):
                s = i * step + j
                for h in range(heads):
                    d = slice(head_dim * h, head_dim * (h + 1))
                    acc[h] = acc[h] + v_s[slot, s, d, :].astype(F32) * score_s[h, pl.ds(s, 1), :]
            return tuple(acc)

        zero = jnp.zeros((head_dim, CHUNK), F32)
        acc = lax.fori_loop(0, src_len // step, mix, (zero,) * heads)
        cmix_s[me, CHUNK * c:CHUNK * (c + 1), :] = jnp.concatenate(acc, axis=0).T.astype(BF16)
        gather_send(1, block(cmix_s, me, c), cmix_s, c)

    def mlp(c):
        if c == 0:
            for copy in own_co:
                copy.wait()
            weight_wait(1, co_s)
        gather_wait(1, cmix_s, c)
        project_heads(cmix_s, co_s, c, res_s)
        if c == 0:
            down_load.wait()
        normed = rms_norm(res_s[CHUNK * c:CHUNK * (c + 1), :], norm_m_ref[...])
        for n in range(0, d_ff, 256):
            end = min(d_ff, n + 256)
            gate = dot(normed, gate_t[:, n:end])
            up = dot(normed, up_t[:, n:end])
            hid_s[:, n:end] = (jax.nn.gelu(gate, approximate=True) * up).astype(BF16)
        hidden = hid_s[...]
        for n in range(0, d_model, 512):
            part_s[c, :, n:n + 512] = dot(hidden, down_s[:, n:n + 512]).astype(BF16)
        give = pl.ds(pl.multiple_of((1 - core) * half, half), half)
        send(remote(part_s.at[c, give, :], near_s.at[c], sum_send.at[0, c], sum_recv.at[0, c], mate))

    keep = pl.ds(pl.multiple_of(core * half, half), half)

    def chip_sum(c):
        remote(near_s.at[c], near_s.at[c], sum_send.at[0, c], sum_recv.at[0, c], mate).wait_recv()
        chip_s[c] = (part_s[c, keep, :].astype(F32) + near_s[c].astype(F32)).astype(BF16)
        send(remote(chip_s.at[c], far_s.at[c], sum_send.at[1, c], sum_recv.at[1, c], over))

    def full_sum(c):
        remote(far_s.at[c], far_s.at[c], sum_send.at[1, c], sum_recv.at[1, c], over).wait_recv()
        mine = pl.ds(pl.multiple_of(CHUNK * c + core * half, half), half)
        done_s[mine, :] = (res_s[mine, :] + (chip_s[c].astype(F32) + far_s[c].astype(F32))).astype(BF16)
        send(remote(done_s.at[mine, :], done_s.at[mine, :], sum_send.at[2, c], sum_recv.at[2, c], mate))

    def store(c):
        other = pl.ds(pl.multiple_of(CHUNK * c + (1 - core) * half, half), half)
        remote(done_s.at[other, :], done_s.at[other, :], sum_send.at[2, c], sum_recv.at[2, c], mate).wait_recv()
        rows = pl.ds(CHUNK * c, CHUNK)
        copy = pltpu.make_async_copy(done_s.at[rows, :], out_ref.at[rows, :], out_sem.at[c])
        copy.start()
        return copy

    gate_load.wait()
    turn(gate_s, gate_t)
    gather_relay(0, mix_s, 0)
    up_load.wait()
    turn(up_s, up_t)
    cross_query(0)
    for c in range(1, chunks):
        gather_relay(0, mix_s, c)
    cross_start(1)
    cross_score(0)
    cross_mix(0)
    weight_send(1, co_ref, cox_ref, co_s)
    own_co = (load(co_ref, shard(co_s, me)), load(cox_ref, shard(co_s, over)))
    cross_start(2)
    cross_query(1)
    cross_score(1)
    cross_mix(1)
    down_load = load(down_ref, down_s)
    cross_start(3)
    cross_query(2)
    gather_relay(1, cmix_s, 0)
    cross_score(2)
    mlp(0)
    gather_relay(1, cmix_s, 1)
    cross_mix(2)
    chip_sum(0)
    cross_query(3)
    cross_score(3)
    cross_mix(3)
    mlp(1)
    gather_relay(1, cmix_s, 2)
    chip_sum(1)
    mlp(2)
    gather_relay(1, cmix_s, 3)
    full_sum(0)
    chip_sum(2)
    mlp(3)
    stores = [store(0)]
    full_sum(1)
    chip_sum(3)
    stores.append(store(1))
    full_sum(2)
    stores.append(store(2))
    full_sum(3)
    stores.append(store(3))
    for copy in stores:
        copy.wait()
    for copy in sends:
        copy.wait_send()


def rest_of_layer(x_in, mixed, w_o, w_o_over, cross_o, cross_o_over, cross_q, gate_t, up_t, w_down, norm_cross, norm_mlp, mask_t, cross_k, cross_v, heads):
    rows, d_model = x_in.shape
    flat = mixed.shape[1]
    d_ff = gate_t.shape[0]
    src_len = cross_k.shape[0]
    chunks = rows // CHUNK
    slots = 2
    anywhere = pl.BlockSpec(memory_space=pl.ANY)
    vmem = pl.BlockSpec(memory_space=pltpu.VMEM)
    dma = pltpu.SemaphoreType.DMA
    return pl.pallas_call(
        functools.partial(rest_kernel, heads, slots),
        in_specs=[anywhere] * 10 + [vmem, vmem] + [anywhere] * 3,
        out_specs=anywhere,
        out_shape=jax.ShapeDtypeStruct((rows, d_model), BF16),
        scratch_shapes=[
            pltpu.VMEM((rows, d_model), BF16),
            pltpu.VMEM((rows, d_model), F32),
            pltpu.VMEM((4, rows, flat), BF16),
            pltpu.VMEM((4, rows, flat), BF16),
            pltpu.VMEM((4 * flat, d_model), BF16),
            pltpu.VMEM((4 * flat, d_model), BF16),
            pltpu.VMEM((d_model, flat), BF16),
            pltpu.VMEM((d_ff, d_model), BF16),
            pltpu.VMEM((d_ff, d_model), BF16),
            pltpu.VMEM((d_model, d_ff), BF16),
            pltpu.VMEM((d_model, d_ff), BF16),
            pltpu.VMEM((d_ff, d_model), BF16),
            pltpu.VMEM((slots, src_len, flat, CHUNK), BF16),
            pltpu.VMEM((slots, src_len, flat, CHUNK), BF16),
            pltpu.VMEM((src_len, rows), jnp.int32),
            pltpu.VMEM((flat, CHUNK), F32),
            pltpu.VMEM((heads, src_len, CHUNK), F32),
            pltpu.VMEM((CHUNK, d_ff), BF16),
            pltpu.VMEM((chunks, CHUNK, d_model), BF16),
            pltpu.VMEM((chunks, CHUNK // 2, d_model), BF16),
            pltpu.VMEM((chunks, CHUNK // 2, d_model), BF16),
            pltpu.VMEM((chunks, CHUNK // 2, d_model), BF16),
            pltpu.VMEM((rows, d_model), BF16),
            dma((2, 3, chunks)), dma((2, 3, chunks)),
            dma((2, 2)), dma((2, 2)),
            dma((3, chunks)), dma((3, chunks)),
            dma((16,)), dma((2, slots)), dma((chunks,)),
        ],
        compiler_params=pltpu.CompilerParams(collective_id=0, has_side_effects=True, vmem_limit_bytes=VMEM_BYTES),
        cost_estimate=pl.CostEstimate(flops=2 * rows * d_model * (8 * flat + flat + 3 * d_ff), bytes_accessed=50_000_000, transcendentals=rows * d_ff),
        name='rest_of_layer',
    )(x_in, mixed, w_o, w_o_over, cross_o, cross_o_over, cross_q, gate_t, up_t, w_down, norm_cross, norm_mlp, mask_t, cross_k, cross_v)


def solution(mesh):
    def local_layer(x_in, tok_pos, self_k, self_v, cross_k, cross_v, enc_mask, rel_bias, w_q, w_k, w_v, w_o, cross_q, cross_o, w_gate, w_up, w_down, norm_self, norm_cross, norm_mlp):
        rows, t_len, heads, head_dim = self_k.shape
        flat = heads * head_dim
        to_kernel = lambda c: jnp.transpose(c, (0, 2, 3, 1)).reshape(rows, flat, t_len)
        from_kernel = lambda c: jnp.transpose(c.reshape(rows, heads, head_dim, t_len), (0, 3, 1, 2))
        cross_view = lambda c: jnp.transpose(c, (1, 2, 3, 0)).reshape(c.shape[1], flat, rows)
        swap = [(0, 2), (1, 3), (2, 0), (3, 1)]
        w_o_over = lax.ppermute(w_o, 'tp', swap)
        cross_o_over = lax.ppermute(cross_o, 'tp', swap)
        mixed_self, new_k, new_v = self_attention(tok_pos, rel_bias.T, x_in, w_q, w_k, w_v, norm_self, to_kernel(self_k), to_kernel(self_v), heads)
        x_out = rest_of_layer(x_in, mixed_self, w_o, w_o_over, cross_o, cross_o_over, cross_q, w_gate.T, w_up.T, w_down, norm_cross, norm_mlp,
                              enc_mask.T, cross_view(cross_k), cross_view(cross_v), heads)
        return x_out, from_kernel(new_k), from_kernel(new_v)

    cache_spec = P('dp', None, 'tp', None)
    split_cols = P(None, 'tp')
    split_rows = P('tp', None)
    in_specs = (P('dp', None), P('dp'), cache_spec, cache_spec, cache_spec, cache_spec, P('dp', None), split_cols, split_cols, split_cols, split_cols, split_rows, split_cols, split_rows, split_cols, split_cols, split_rows, P(None), P(None), P(None))
    out_specs = (P('dp', None), cache_spec, cache_spec)
    return jax.shard_map(local_layer, mesh=mesh, in_specs=in_specs, out_specs=out_specs, check_vma=False)
```

```python
import functools
import math
import jax
import jax.numpy as jnp
from jax import lax
from jax.experimental import pallas as pl
from jax.experimental.pallas import tpu as pltpu
from jax.sharding import PartitionSpec as P

BUCKET_EDGES = tuple(int(math.ceil(16.0 * 8.0 ** (bucket_step / 16.0))) for bucket_step in range(1, 16))
NEG_FILL = -1e30
STEP_ROWS = 32
SLOTS = 8
AHEAD = 4
VMEM_BYTES = 67043328
LANES = 128
F32 = jnp.float32
BF16 = jnp.bfloat16


def rms_norm(values, norm_scale):
    inv_rms = lax.rsqrt(jnp.mean(values * values, axis=-1, keepdims=True) + 1e-6)
    return (values * inv_rms * norm_scale.astype(F32)).astype(BF16)


def dot(a, b):
    return jnp.dot(a, b, preferred_element_type=F32)


def dot_nt(a, b):
    return lax.dot_general(a, b, (((1,), (1,)), ((), ())), preferred_element_type=F32)


def iota(shape, axis):
    return lax.broadcasted_iota(jnp.int32, shape, axis)


def self_kernel(heads, head_dim, pos_ref, bias_ref, x_ref, wq_ref, wk_ref, wv_ref, norm_ref, k_ref, v_ref,
                mixed_ref, ko_ref, vo_ref, x_s, wq_s, wk_s, wv_s, k_s, v_s, mixed_s, q_s, kt_s, vt_s, score_s, out_s,
                load_sem, in_sem, out_sem, mixed_sem):
    flat = heads * head_dim
    rows_total = x_ref.shape[0]
    n = STEP_ROWS
    steps = rows_total // n

    def rows_of(step):
        return pl.ds(pl.multiple_of(step * n, n), n)

    def fetch(step):
        slot = lax.rem(step, SLOTS)
        return (pltpu.make_async_copy(k_ref.at[rows_of(step)], k_s.at[slot], in_sem.at[0, slot]),
                pltpu.make_async_copy(v_ref.at[rows_of(step)], v_s.at[slot], in_sem.at[1, slot]))

    def write(step):
        slot = lax.rem(step, SLOTS)
        return (pltpu.make_async_copy(k_s.at[slot], ko_ref.at[rows_of(step)], out_sem.at[0, slot]),
                pltpu.make_async_copy(v_s.at[slot], vo_ref.at[rows_of(step)], out_sem.at[1, slot]))

    loads = [pltpu.make_async_copy(src, dst, load_sem.at[i])
             for i, (src, dst) in enumerate(((x_ref, x_s), (wq_ref, wq_s), (wk_ref, wk_s), (wv_ref, wv_s)))]
    for copy in loads:
        copy.start()
    for step in range(AHEAD):
        for copy in fetch(step):
            copy.start()

    lane = iota((4 * heads, LANES), 1)
    head_of = lax.rem(iota((4 * heads, LANES), 0), heads)
    far = jnp.full_like(lane, 16)
    for edge in BUCKET_EDGES:
        far = far + jnp.where(lane >= edge, 1, 0)
    bucket = jnp.where(lane < 16, lane, far)
    table = jnp.zeros((4 * heads, LANES), F32)
    for b in range(32):
        here = jnp.zeros((4 * heads, LANES), F32)
        for h in range(heads):
            here = jnp.where(head_of == h, bias_ref[h, b], here)
        table = jnp.where(bucket == b, here, table)

    for copy in loads:
        copy.wait()

    @pl.loop(0, rows_total // LANES)
    def _(g):
        rows = pl.ds(pl.multiple_of(g * LANES, LANES), LANES)
        normed = rms_norm(x_s[rows, :].astype(F32), norm_ref[...])
        q_s[rows, :] = dot(normed, wq_s[...]).astype(BF16)
        kt_s[g] = dot(normed, wk_s[...]).astype(BF16).astype(F32).T
        vt_s[g] = dot(normed, wv_s[...]).astype(BF16).astype(F32).T

    spread = jnp.where(iota((n * heads, n), 0) // heads == iota((n * heads, n), 1), 1.0, 0.0).astype(BF16)
    gather = jnp.where(iota((n, n * heads), 1) // heads == iota((n, n * heads), 0), 1.0, 0.0).astype(BF16)
    own_head = iota((n * heads, flat), 1) // head_dim == lax.rem(iota((n * heads, flat), 0), heads)
    lane_bf = iota((flat, LANES), 1).astype(F32).astype(BF16)
    quad_row = iota((4 * heads, LANES), 0)
    per = LANES // n

    @pl.loop(0, steps)
    def _(step):
        ahead = step + AHEAD

        @pl.when(ahead < steps)
        def _():
            @pl.when(ahead >= SLOTS)
            def _():
                for copy in write(ahead - SLOTS):
                    copy.wait()
            for copy in fetch(ahead):
                copy.start()

        first = pl.multiple_of(step * n, n)
        slot = lax.rem(step, SLOTS)
        group, part = step // per, lax.rem(step, per)
        shift = lax.rem(LANES - part * n, LANES)
        k_new = pltpu.roll(kt_s[group], shift, 1).astype(BF16)
        v_new = pltpu.roll(vt_s[group], shift, 1).astype(BF16)
        q_rows = jnp.where(own_head, dot(spread, q_s[pl.ds(first, n), :]), 0.0).astype(BF16)
        in_k, in_v = fetch(step)

        def update(cache, new_cols, b):
            at_pos = lane_bf == pos_ref[first + b].astype(F32).astype(BF16)
            col = jnp.broadcast_to(new_cols[:, b:b + 1], (flat, LANES))
            updated = jnp.where(at_pos, col, cache[slot, b])
            cache[slot, b] = updated
            return updated

        in_k.wait()
        for g in range(n // 4):
            lhs = q_rows[4 * heads * g:4 * heads * (g + 1), :]
            picked = None
            distance = None
            for half in range(2):
                b = 4 * g + 2 * half
                pair = jnp.concatenate([update(k_s, k_new, b), update(k_s, k_new, b + 1)], axis=1)
                both = dot(lhs, pair)
                for j in range(2):
                    mine = both[:, LANES * j:LANES * (j + 1)]
                    at = 2 * half + j
                    pos = pos_ref[first + 4 * g + at]
                    picked = mine if picked is None else jnp.where(quad_row >= heads * at, mine, picked)
                    distance = jnp.full((4 * heads, LANES), pos, jnp.int32) if distance is None else jnp.where(quad_row >= heads * at, pos, distance)
            distance = distance - iota((4 * heads, LANES), 1)
            bias = jnp.take_along_axis(table, jnp.maximum(distance, 0), axis=1)
            score_s[4 * heads * g:4 * heads * (g + 1), :] = jnp.where(distance >= 0, picked + bias, NEG_FILL)
        write(step)[0].start()

        scores = score_s[...]
        exps = jnp.exp(scores - jnp.max(scores, axis=1, keepdims=True))
        probs = exps * pl.reciprocal(jnp.sum(exps, axis=1, keepdims=True))

        in_v.wait()
        for g in range(n // 4):
            quad = probs[4 * heads * g:4 * heads * (g + 1), :]
            picked = None
            for half in range(2):
                b = 4 * g + 2 * half
                pair = jnp.concatenate([update(v_s, v_new, b), update(v_s, v_new, b + 1)], axis=1)
                low = jnp.where(quad_row // heads == 2 * half, quad, 0.0)
                high = jnp.where(quad_row // heads == 2 * half + 1, quad, 0.0)
                lhs = jnp.concatenate([low, high], axis=1).astype(BF16)
                both = dot_nt(lhs, pair)
                picked = both if half == 0 else jnp.where(iota(both.shape, 0) >= 2 * heads, both, picked)
            out_s[4 * heads * g:4 * heads * (g + 1), :] = picked
        write(step)[1].start()
        mixed_s[pl.ds(first, n), :] = dot(gather, jnp.where(own_head, out_s[...], 0.0).astype(BF16)).astype(BF16)

    mixed_copy = pltpu.make_async_copy(mixed_s, mixed_ref, mixed_sem)
    mixed_copy.start()
    for step in range(steps - SLOTS, steps):
        for copy in write(step):
            copy.wait()
    mixed_copy.wait()


def self_attention(tok_pos, bias_t, x_in, w_q, w_k, w_v, norm_self, keys, values, heads):
    rows, flat, t_len = keys.shape
    d_model = x_in.shape[1]
    n = STEP_ROWS
    smem = pl.BlockSpec(memory_space=pltpu.SMEM)
    anywhere = pl.BlockSpec(memory_space=pl.ANY)
    cache_shape = jax.ShapeDtypeStruct(keys.shape, BF16)
    return pl.pallas_call(
        functools.partial(self_kernel, heads, flat // heads),
        in_specs=[smem, smem] + [anywhere] * 4 + [pl.BlockSpec(memory_space=pltpu.VMEM)] + [anywhere] * 2,
        out_specs=[anywhere] * 3,
        out_shape=[jax.ShapeDtypeStruct((rows, flat), BF16), cache_shape, cache_shape],
        scratch_shapes=[
            pltpu.VMEM((rows, d_model), BF16),
            pltpu.VMEM((d_model, flat), BF16),
            pltpu.VMEM((d_model, flat), BF16),
            pltpu.VMEM((d_model, flat), BF16),
            pltpu.VMEM((SLOTS, n, flat, t_len), BF16),
            pltpu.VMEM((SLOTS, n, flat, t_len), BF16),
            pltpu.VMEM((rows, flat), BF16),
            pltpu.VMEM((rows, flat), BF16),
            pltpu.VMEM((rows // LANES, flat, LANES), F32),
            pltpu.VMEM((rows // LANES, flat, LANES), F32),
            pltpu.VMEM((n * heads, LANES), F32),
            pltpu.VMEM((n * heads, flat), F32),
            pltpu.SemaphoreType.DMA((4,)),
            pltpu.SemaphoreType.DMA((2, SLOTS)),
            pltpu.SemaphoreType.DMA((2, SLOTS)),
            pltpu.SemaphoreType.DMA,
        ],
        compiler_params=pltpu.CompilerParams(vmem_limit_bytes=VMEM_BYTES),
        cost_estimate=pl.CostEstimate(flops=4 * rows * flat * t_len * 16 + 6 * rows * d_model * flat, bytes_accessed=8 * rows * flat * t_len, transcendentals=rows * heads * t_len),
        name='self_attention',
    )(tok_pos, bias_t, x_in, w_q, w_k, w_v, norm_self, keys, values)


CHUNK = 128
MESH = pl.DeviceIdType.MESH


def rest_kernel(heads, n_cross_slots,
                x_ref, mixed_ref, wo_ref, wox_ref, wom_ref, co_ref, cox_ref, com_ref, cq_ref, gate_ref, up_ref, down_ref, norm_c_ref, norm_m_ref,
                mask_ref, ck_ref, cv_ref, out_ref,
                x_s, res_s, mix_s, cmix_s, wo_s, co_s, cq_s, gate_s, up_s, gate_t, up_t, down_s, k_s, v_s, mask_s,
                qt_s, score_s, hid_s, part_s, near_s, chip_s, far_s, done_s,
                ag_send, ag_recv, w_send, w_recv, sum_send, sum_recv, load_sem, cross_sem, out_sem):
    me = lax.axis_index('tp')
    core = lax.rem(me, 2)
    mate = me + 1 - 2 * core
    over = lax.rem(me + 2, 4)
    cater = lax.rem(mate + 2, 4)
    rows_total, d_model = x_ref.shape
    flat = mixed_ref.shape[1]
    head_dim = flat // heads
    src_len = ck_ref.shape[0]
    d_ff = gate_ref.shape[0]
    chunks = rows_total // CHUNK
    half = CHUNK // 2

    def remote(src, dst, send_sem, recv_sem, to):
        return pltpu.make_async_remote_copy(src_ref=src, dst_ref=dst, send_sem=send_sem, recv_sem=recv_sem,
                                            device_id={'tp': to}, device_id_type=MESH)

    def block(buf, who, c):
        return buf.at[who, pl.ds(CHUNK * c, CHUNK), :]

    def shard(buf, who):
        return buf.at[pl.ds(pl.multiple_of(who * flat, flat), flat), :]

    loads = []

    def load(src, dst):
        copy = pltpu.make_async_copy(src, dst, load_sem.at[len(loads)])
        copy.start()
        loads.append(copy)
        return copy

    def cross_load(c):
        slot = c % n_cross_slots
        cols = pl.ds(CHUNK * c, CHUNK)
        return (pltpu.make_async_copy(ck_ref.at[:, :, cols], k_s.at[slot], cross_sem.at[0, slot]),
                pltpu.make_async_copy(cv_ref.at[:, :, cols], v_s.at[slot], cross_sem.at[1, slot]))

    def cross_start(c):
        for copy in cross_load(c):
            copy.start()

    barrier = pltpu.get_barrier_semaphore()
    for peer in (mate, over):
        pl.semaphore_signal(barrier, inc=1, device_id={'tp': peer}, device_id_type=MESH)
    pl.semaphore_wait(barrier, 2)

    sends = []

    def send(copy):
        copy.start()
        sends.append(copy)

    def gather_send(stage, src, buf, c):
        send(remote(src, block(buf, me, c), ag_send.at[stage, 0, c], ag_recv.at[stage, 0, c], over))
        send(remote(src, block(buf, me, c), ag_send.at[stage, 1, c], ag_recv.at[stage, 1, c], mate))

    def gather_relay(stage, buf, c):
        remote(block(buf, over, c), block(buf, over, c), ag_send.at[stage, 0, c], ag_recv.at[stage, 0, c], over).wait_recv()
        send(remote(block(buf, over, c), block(buf, over, c), ag_send.at[stage, 2, c], ag_recv.at[stage, 2, c], mate))

    def gather_wait(stage, buf, c):
        remote(block(buf, mate, c), block(buf, mate, c), ag_send.at[stage, 1, c], ag_recv.at[stage, 1, c], mate).wait_recv()
        remote(block(buf, cater, c), block(buf, cater, c), ag_send.at[stage, 2, c], ag_recv.at[stage, 2, c], mate).wait_recv()

    def weight_send(which, ref_x, buf):
        send(remote(ref_x, shard(buf, over), w_send.at[which], w_recv.at[which], mate))

    def weight_wait(which, buf):
        remote(shard(buf, cater), shard(buf, cater), w_send.at[which], w_recv.at[which], mate).wait_recv()

    for c in range(chunks):
        gather_send(0, mixed_ref.at[pl.ds(CHUNK * c, CHUNK), :], mix_s, c)
    own_mixed = load(mixed_ref, mix_s.at[me])
    own_wo = (load(wo_ref, shard(wo_s, me)), load(wox_ref, shard(wo_s, over)), load(wom_ref, shard(wo_s, mate)))
    x_load = load(x_ref, x_s)
    q_load = load(cq_ref, cq_s)
    mask_load = load(mask_ref, mask_s)
    weight_send(0, wox_ref, wo_s)
    gate_load = load(gate_ref, gate_s)
    up_load = load(up_ref, up_s)
    cross_start(0)

    def turn(wide, tall):
        @pl.loop(0, d_model // CHUNK)
        def _(i):
            at = pl.ds(pl.multiple_of(i * CHUNK, CHUNK), CHUNK)
            tall[at, :] = wide[:, at].T

    def project_heads(buf, weight, c, add_to):
        lhs = jnp.concatenate([buf[i, CHUNK * c:CHUNK * (c + 1), :] for i in range(4)], axis=1)
        for n in range(0, d_model, 512):
            res_s[CHUNK * c:CHUNK * (c + 1), n:n + 512] = add_to[CHUNK * c:CHUNK * (c + 1), n:n + 512].astype(F32) + dot(lhs, weight[:, n:n + 512])

    def cross_query(c):
        if c == 0:
            own_mixed.wait()
            x_load.wait()
            for copy in own_wo:
                copy.wait()
        gather_wait(0, mix_s, c)
        if c == 0:
            weight_wait(0, wo_s)
            q_load.wait()
        project_heads(mix_s, wo_s, c, x_s)
        normed = rms_norm(res_s[CHUNK * c:CHUNK * (c + 1), :], norm_c_ref[...])
        qt_s[...] = dot(normed, cq_s[...]).astype(BF16).astype(F32).T

    def cross_score(c):
        slot = c % n_cross_slots
        for copy in cross_load(c):
            copy.wait()
        if c == 0:
            mask_load.wait()
        step = 8

        @pl.loop(0, src_len // step)
        def _(i):
            at = pl.ds(pl.multiple_of(i * step, step), step)
            for h in range(heads):
                d = slice(head_dim * h, head_dim * (h + 1))
                score_s[h, at, :] = jnp.sum(k_s[slot, at, d, :].astype(F32) * qt_s[d, :][None], axis=1)

    def cross_mix(c):
        slot = c % n_cross_slots
        step = 8
        valid = mask_s[:, CHUNK * c:CHUNK * (c + 1)] != 0
        for h in range(heads):
            scores = jnp.where(valid, score_s[h], NEG_FILL)
            exps = jnp.exp(scores - jnp.max(scores, axis=0, keepdims=True))
            probs = exps * pl.reciprocal(jnp.sum(exps, axis=0, keepdims=True))
            score_s[h] = probs.astype(BF16).astype(F32)

        def mix(i, acc):
            acc = list(acc)
            for j in range(step):
                s = i * step + j
                for h in range(heads):
                    d = slice(head_dim * h, head_dim * (h + 1))
                    acc[h] = acc[h] + v_s[slot, s, d, :].astype(F32) * score_s[h, pl.ds(s, 1), :]
            return tuple(acc)

        zero = jnp.zeros((head_dim, CHUNK), F32)
        acc = lax.fori_loop(0, src_len // step, mix, (zero,) * heads)
        cmix_s[me, CHUNK * c:CHUNK * (c + 1), :] = jnp.concatenate(acc, axis=0).T.astype(BF16)
        gather_send(1, block(cmix_s, me, c), cmix_s, c)

    def mlp(c):
        if c == 0:
            for copy in own_co:
                copy.wait()
            weight_wait(1, co_s)
        gather_wait(1, cmix_s, c)
        project_heads(cmix_s, co_s, c, res_s)
        if c == 0:
            down_load.wait()
        normed = rms_norm(res_s[CHUNK * c:CHUNK * (c + 1), :], norm_m_ref[...])
        for n in range(0, d_ff, 256):
            end = min(d_ff, n + 256)
            gate = dot(normed, gate_t[:, n:end])
            up = dot(normed, up_t[:, n:end])
            hid_s[:, n:end] = (jax.nn.gelu(gate, approximate=True) * up).astype(BF16)
        hidden = hid_s[...]
        for n in range(0, d_model, 512):
            part_s[c, :, n:n + 512] = dot(hidden, down_s[:, n:n + 512]).astype(BF16)
        give = pl.ds(pl.multiple_of((1 - core) * half, half), half)
        send(remote(part_s.at[c, give, :], near_s.at[c], sum_send.at[0, c], sum_recv.at[0, c], mate))

    keep = pl.ds(pl.multiple_of(core * half, half), half)

    def chip_sum(c):
        remote(near_s.at[c], near_s.at[c], sum_send.at[0, c], sum_recv.at[0, c], mate).wait_recv()
        chip_s[c] = (part_s[c, keep, :].astype(F32) + near_s[c].astype(F32)).astype(BF16)
        send(remote(chip_s.at[c], far_s.at[c], sum_send.at[1, c], sum_recv.at[1, c], over))

    def full_sum(c):
        remote(far_s.at[c], far_s.at[c], sum_send.at[1, c], sum_recv.at[1, c], over).wait_recv()
        mine = pl.ds(pl.multiple_of(CHUNK * c + core * half, half), half)
        done_s[mine, :] = (res_s[mine, :] + (chip_s[c].astype(F32) + far_s[c].astype(F32))).astype(BF16)
        send(remote(done_s.at[mine, :], done_s.at[mine, :], sum_send.at[2, c], sum_recv.at[2, c], mate))

    def store(c):
        other = pl.ds(pl.multiple_of(CHUNK * c + (1 - core) * half, half), half)
        remote(done_s.at[other, :], done_s.at[other, :], sum_send.at[2, c], sum_recv.at[2, c], mate).wait_recv()
        rows = pl.ds(CHUNK * c, CHUNK)
        copy = pltpu.make_async_copy(done_s.at[rows, :], out_ref.at[rows, :], out_sem.at[c])
        copy.start()
        return copy

    gate_load.wait()
    turn(gate_s, gate_t)
    gather_relay(0, mix_s, 0)
    up_load.wait()
    turn(up_s, up_t)
    cross_query(0)
    for c in range(1, chunks):
        gather_relay(0, mix_s, c)
    weight_send(1, cox_ref, co_s)
    cross_start(1)
    cross_score(0)
    cross_mix(0)
    own_co = (load(co_ref, shard(co_s, me)), load(cox_ref, shard(co_s, over)), load(com_ref, shard(co_s, mate)))
    cross_start(2)
    cross_query(1)
    cross_score(1)
    cross_mix(1)
    down_load = load(down_ref, down_s)
    cross_start(3)
    cross_query(2)
    gather_relay(1, cmix_s, 0)
    cross_score(2)
    mlp(0)
    gather_relay(1, cmix_s, 1)
    cross_mix(2)
    chip_sum(0)
    cross_query(3)
    cross_score(3)
    cross_mix(3)
    mlp(1)
    gather_relay(1, cmix_s, 2)
    chip_sum(1)
    mlp(2)
    gather_relay(1, cmix_s, 3)
    full_sum(0)
    chip_sum(2)
    mlp(3)
    stores = [store(0)]
    full_sum(1)
    chip_sum(3)
    stores.append(store(1))
    full_sum(2)
    stores.append(store(2))
    full_sum(3)
    stores.append(store(3))
    for copy in stores:
        copy.wait()
    for copy in sends:
        copy.wait_send()


def rest_of_layer(x_in, mixed, w_o, w_o_over, w_o_mate, cross_o, cross_o_over, cross_o_mate, cross_q, gate_t, up_t, w_down, norm_cross, norm_mlp, mask_t, cross_k, cross_v, heads):
    rows, d_model = x_in.shape
    flat = mixed.shape[1]
    d_ff = gate_t.shape[0]
    src_len = cross_k.shape[0]
    chunks = rows // CHUNK
    slots = 2
    anywhere = pl.BlockSpec(memory_space=pl.ANY)
    vmem = pl.BlockSpec(memory_space=pltpu.VMEM)
    dma = pltpu.SemaphoreType.DMA
    return pl.pallas_call(
        functools.partial(rest_kernel, heads, slots),
        in_specs=[anywhere] * 12 + [vmem, vmem] + [anywhere] * 3,
        out_specs=anywhere,
        out_shape=jax.ShapeDtypeStruct((rows, d_model), BF16),
        scratch_shapes=[
            pltpu.VMEM((rows, d_model), BF16),
            pltpu.VMEM((rows, d_model), F32),
            pltpu.VMEM((4, rows, flat), BF16),
            pltpu.VMEM((4, rows, flat), BF16),
            pltpu.VMEM((4 * flat, d_model), BF16),
            pltpu.VMEM((4 * flat, d_model), BF16),
            pltpu.VMEM((d_model, flat), BF16),
            pltpu.VMEM((d_ff, d_model), BF16),
            pltpu.VMEM((d_ff, d_model), BF16),
            pltpu.VMEM((d_model, d_ff), BF16),
            pltpu.VMEM((d_model, d_ff), BF16),
            pltpu.VMEM((d_ff, d_model), BF16),
            pltpu.VMEM((slots, src_len, flat, CHUNK), BF16),
            pltpu.VMEM((slots, src_len, flat, CHUNK), BF16),
            pltpu.VMEM((src_len, rows), jnp.int32),
            pltpu.VMEM((flat, CHUNK), F32),
            pltpu.VMEM((heads, src_len, CHUNK), F32),
            pltpu.VMEM((CHUNK, d_ff), BF16),
            pltpu.VMEM((chunks, CHUNK, d_model), BF16),
            pltpu.VMEM((chunks, CHUNK // 2, d_model), BF16),
            pltpu.VMEM((chunks, CHUNK // 2, d_model), BF16),
            pltpu.VMEM((chunks, CHUNK // 2, d_model), BF16),
            pltpu.VMEM((rows, d_model), BF16),
            dma((2, 3, chunks)), dma((2, 3, chunks)),
            dma((2,)), dma((2,)),
            dma((3, chunks)), dma((3, chunks)),
            dma((16,)), dma((2, slots)), dma((chunks,)),
        ],
        compiler_params=pltpu.CompilerParams(collective_id=0, has_side_effects=True, vmem_limit_bytes=VMEM_BYTES),
        cost_estimate=pl.CostEstimate(flops=2 * rows * d_model * (8 * flat + flat + 3 * d_ff), bytes_accessed=50_000_000, transcendentals=rows * d_ff),
        name='rest_of_layer',
    )(x_in, mixed, w_o, w_o_over, w_o_mate, cross_o, cross_o_over, cross_o_mate, cross_q, gate_t, up_t, w_down, norm_cross, norm_mlp, mask_t, cross_k, cross_v)


def solution(mesh):
    def local_layer(x_in, tok_pos, self_k, self_v, cross_k, cross_v, enc_mask, rel_bias, w_q, w_k, w_v, w_o, cross_q, cross_o, w_gate, w_up, w_down, norm_self, norm_cross, norm_mlp):
        rows, t_len, heads, head_dim = self_k.shape
        flat = heads * head_dim
        to_kernel = lambda c: jnp.transpose(c, (0, 2, 3, 1)).reshape(rows, flat, t_len)
        from_kernel = lambda c: jnp.transpose(c.reshape(rows, heads, head_dim, t_len), (0, 3, 1, 2))
        cross_view = lambda c: jnp.transpose(c, (1, 2, 3, 0)).reshape(c.shape[1], flat, rows)
        swap = [(0, 2), (1, 3), (2, 0), (3, 1)]
        w_o_over = lax.ppermute(w_o, 'tp', swap)
        cross_o_over = lax.ppermute(cross_o, 'tp', swap)
        mates = [(0, 1), (1, 0), (2, 3), (3, 2)]
        w_o_mate = lax.ppermute(w_o, 'tp', mates)
        cross_o_mate = lax.ppermute(cross_o, 'tp', mates)
        mixed_self, new_k, new_v = self_attention(tok_pos, rel_bias.T, x_in, w_q, w_k, w_v, norm_self, to_kernel(self_k), to_kernel(self_v), heads)
        x_out = rest_of_layer(x_in, mixed_self, w_o, w_o_over, w_o_mate, cross_o, cross_o_over, cross_o_mate, cross_q, w_gate.T, w_up.T, w_down, norm_cross, norm_mlp,
                              enc_mask.T, cross_view(cross_k), cross_view(cross_v), heads)
        return x_out, from_kernel(new_k), from_kernel(new_v)

    cache_spec = P('dp', None, 'tp', None)
    split_cols = P(None, 'tp')
    split_rows = P('tp', None)
    in_specs = (P('dp', None), P('dp'), cache_spec, cache_spec, cache_spec, cache_spec, P('dp', None), split_cols, split_cols, split_cols, split_cols, split_rows, split_cols, split_rows, split_cols, split_cols, split_rows, P(None), P(None), P(None))
    out_specs = (P('dp', None), cache_spec, cache_spec)
    return jax.shard_map(local_layer, mesh=mesh, in_specs=in_specs, out_specs=out_specs, check_vma=False)
```

```python
import functools
import math
import jax
import jax.numpy as jnp
from jax import lax
from jax.experimental import pallas as pl
from jax.experimental.pallas import tpu as pltpu
from jax.sharding import PartitionSpec as P

BUCKET_EDGES = tuple(int(math.ceil(16.0 * 8.0 ** (bucket_step / 16.0))) for bucket_step in range(1, 16))
NEG_FILL = -1e30
STEP_ROWS = 32
BLOCK_ROWS = 64
SLOTS = 6
AHEAD = 3
VMEM_BYTES = 67043328
LANES = 128
F32 = jnp.float32
BF16 = jnp.bfloat16


def rms_norm(values, norm_scale):
    inv_rms = lax.rsqrt(jnp.mean(values * values, axis=-1, keepdims=True) + 1e-6)
    return (values * inv_rms * norm_scale.astype(F32)).astype(BF16)


def dot(a, b):
    return jnp.dot(a, b, preferred_element_type=F32)


def dot_nt(a, b):
    return lax.dot_general(a, b, (((1,), (1,)), ((), ())), preferred_element_type=F32)


def iota(shape, axis):
    return lax.broadcasted_iota(jnp.int32, shape, axis)


def self_kernel(heads, head_dim, pos_ref, bias_ref, x_ref, wq_ref, wk_ref, wv_ref, norm_ref, k_ref, v_ref,
                mixed_ref, ko_ref, vo_ref, x_s, wq_s, wk_s, wv_s, k_s, v_s, mixed_s, q_s, kt_s, vt_s, score_s, out_s,
                load_sem, in_sem, out_sem, mixed_sem):
    flat = heads * head_dim
    rows_total = x_ref.shape[0]
    n = STEP_ROWS
    parts = BLOCK_ROWS // n
    steps = rows_total // BLOCK_ROWS

    def rows_of(step):
        return pl.ds(pl.multiple_of(step * BLOCK_ROWS, BLOCK_ROWS), BLOCK_ROWS)

    def fetch(step):
        slot = lax.rem(step, SLOTS)
        return (pltpu.make_async_copy(k_ref.at[rows_of(step)], k_s.at[slot], in_sem.at[0, slot]),
                pltpu.make_async_copy(v_ref.at[rows_of(step)], v_s.at[slot], in_sem.at[1, slot]))

    def write(step):
        slot = lax.rem(step, SLOTS)
        return (pltpu.make_async_copy(k_s.at[slot], ko_ref.at[rows_of(step)], out_sem.at[0, slot]),
                pltpu.make_async_copy(v_s.at[slot], vo_ref.at[rows_of(step)], out_sem.at[1, slot]))

    def write_part(part):
        slot = (steps - 1) % SLOTS
        here = pl.ds(pl.multiple_of(part * n, n), n)
        there = pl.ds(pl.multiple_of(BLOCK_ROWS * (steps - 1) + part * n, n), n)
        return (pltpu.make_async_copy(k_s.at[slot, here], ko_ref.at[there], out_sem.at[0, slot]),
                pltpu.make_async_copy(v_s.at[slot, here], vo_ref.at[there], out_sem.at[1, slot]))

    loads = [pltpu.make_async_copy(src, dst, load_sem.at[i])
             for i, (src, dst) in enumerate(((x_ref, x_s), (wq_ref, wq_s), (wk_ref, wk_s), (wv_ref, wv_s)))]
    for copy in loads:
        copy.start()
    for step in range(AHEAD):
        for copy in fetch(step):
            copy.start()

    lane = iota((4 * heads, LANES), 1)
    head_of = lax.rem(iota((4 * heads, LANES), 0), heads)
    far = jnp.full_like(lane, 16)
    for edge in BUCKET_EDGES:
        far = far + jnp.where(lane >= edge, 1, 0)
    bucket = jnp.where(lane < 16, lane, far)
    table = jnp.zeros((4 * heads, LANES), F32)
    for b in range(32):
        here = jnp.zeros((4 * heads, LANES), F32)
        for h in range(heads):
            here = jnp.where(head_of == h, bias_ref[h, b], here)
        table = jnp.where(bucket == b, here, table)

    for copy in loads:
        copy.wait()

    @pl.loop(0, rows_total // LANES)
    def _(g):
        rows = pl.ds(pl.multiple_of(g * LANES, LANES), LANES)
        normed = rms_norm(x_s[rows, :].astype(F32), norm_ref[...])
        q_s[rows, :] = dot(normed, wq_s[...]).astype(BF16)
        kt_s[g] = dot(normed, wk_s[...]).astype(BF16).astype(F32).T
        vt_s[g] = dot(normed, wv_s[...]).astype(BF16).astype(F32).T

    spread = jnp.where(iota((n * heads, n), 0) // heads == iota((n * heads, n), 1), 1.0, 0.0).astype(BF16)
    gather = jnp.where(iota((n, n * heads), 1) // heads == iota((n, n * heads), 0), 1.0, 0.0).astype(BF16)
    own_head = iota((n * heads, flat), 1) // head_dim == lax.rem(iota((n * heads, flat), 0), heads)
    lane_bf = iota((flat, LANES), 1).astype(F32).astype(BF16)
    quad_row = iota((4 * heads, LANES), 0)
    per = LANES // n

    @pl.loop(0, steps)
    def _(step):
        ahead = step + AHEAD

        @pl.when(ahead < steps)
        def _():
            @pl.when(ahead >= SLOTS)
            def _():
                for copy in write(ahead - SLOTS):
                    copy.wait()
            for copy in fetch(ahead):
                copy.start()

        slot = lax.rem(step, SLOTS)
        for copy in fetch(step):
            copy.wait()

        @pl.loop(0, parts)
        def _(sub):
            base = pl.multiple_of(sub * n, n)
            first = pl.multiple_of(step * BLOCK_ROWS + base, n)
            group, part = first // LANES, lax.rem(first // n, per)
            shift = lax.rem(LANES - part * n, LANES)
            k_new = pltpu.roll(kt_s[group], shift, 1)
            v_new = pltpu.roll(vt_s[group], shift, 1)
            q_rows = jnp.where(own_head, dot(spread, q_s[pl.ds(first, n), :]), 0.0).astype(BF16)

            def update(cache, new_cols, b):
                at_pos = lane_bf == pos_ref[first + b].astype(F32).astype(BF16)
                col = jnp.broadcast_to(new_cols[:, b:b + 1], (flat, LANES)).astype(BF16)
                updated = jnp.where(at_pos, col, cache[slot, base + b])
                cache[slot, base + b] = updated
                return updated

            for g in range(n // 4):
                lhs = q_rows[4 * heads * g:4 * heads * (g + 1), :]
                picked = None
                distance = None
                for half in range(2):
                    b = 4 * g + 2 * half
                    pair = jnp.concatenate([update(k_s, k_new, b), update(k_s, k_new, b + 1)], axis=1)
                    both = dot(lhs, pair)
                    for j in range(2):
                        mine = both[:, LANES * j:LANES * (j + 1)]
                        at = 2 * half + j
                        pos = pos_ref[first + 4 * g + at]
                        picked = mine if picked is None else jnp.where(quad_row >= heads * at, mine, picked)
                        distance = jnp.full((4 * heads, LANES), pos, jnp.int32) if distance is None else jnp.where(quad_row >= heads * at, pos, distance)
                distance = distance - iota((4 * heads, LANES), 1)
                bias = jnp.take_along_axis(table, jnp.maximum(distance, 0), axis=1)
                score_s[4 * heads * g:4 * heads * (g + 1), :] = jnp.where(distance >= 0, picked + bias, NEG_FILL)

            scores = score_s[...]
            exps = jnp.exp(scores - jnp.max(scores, axis=1, keepdims=True))
            probs = exps * pl.reciprocal(jnp.sum(exps, axis=1, keepdims=True))

            for g in range(n // 4):
                quad = probs[4 * heads * g:4 * heads * (g + 1), :]
                picked = None
                for half in range(2):
                    b = 4 * g + 2 * half
                    pair = jnp.concatenate([update(v_s, v_new, b), update(v_s, v_new, b + 1)], axis=1)
                    low = jnp.where(quad_row // heads == 2 * half, quad, 0.0)
                    high = jnp.where(quad_row // heads == 2 * half + 1, quad, 0.0)
                    lhs = jnp.concatenate([low, high], axis=1).astype(BF16)
                    both = dot_nt(lhs, pair)
                    picked = both if half == 0 else jnp.where(iota(both.shape, 0) >= 2 * heads, both, picked)
                out_s[4 * heads * g:4 * heads * (g + 1), :] = picked
            mixed_s[pl.ds(first, n), :] = dot(gather, jnp.where(own_head, out_s[...], 0.0).astype(BF16)).astype(BF16)

            @pl.when(step == steps - 1)
            def _():
                for copy in write_part(sub):
                    copy.start()

        @pl.when(step < steps - 1)
        def _():
            for copy in write(step):
                copy.start()

    mixed_copy = pltpu.make_async_copy(mixed_s, mixed_ref, mixed_sem)
    mixed_copy.start()
    for step in range(steps - SLOTS, steps):
        for copy in write(step):
            copy.wait()
    mixed_copy.wait()


def self_attention(tok_pos, bias_t, x_in, w_q, w_k, w_v, norm_self, keys, values, heads):
    rows, flat, t_len = keys.shape
    d_model = x_in.shape[1]
    n = STEP_ROWS
    smem = pl.BlockSpec(memory_space=pltpu.SMEM)
    anywhere = pl.BlockSpec(memory_space=pl.ANY)
    cache_shape = jax.ShapeDtypeStruct(keys.shape, BF16)
    return pl.pallas_call(
        functools.partial(self_kernel, heads, flat // heads),
        in_specs=[smem, smem] + [anywhere] * 4 + [pl.BlockSpec(memory_space=pltpu.VMEM)] + [anywhere] * 2,
        out_specs=[anywhere] * 3,
        out_shape=[jax.ShapeDtypeStruct((rows, flat), BF16), cache_shape, cache_shape],
        scratch_shapes=[
            pltpu.VMEM((rows, d_model), BF16),
            pltpu.VMEM((d_model, flat), BF16),
            pltpu.VMEM((d_model, flat), BF16),
            pltpu.VMEM((d_model, flat), BF16),
            pltpu.VMEM((SLOTS, BLOCK_ROWS, flat, t_len), BF16),
            pltpu.VMEM((SLOTS, BLOCK_ROWS, flat, t_len), BF16),
            pltpu.VMEM((rows, flat), BF16),
            pltpu.VMEM((rows, flat), BF16),
            pltpu.VMEM((rows // LANES, flat, LANES), F32),
            pltpu.VMEM((rows // LANES, flat, LANES), F32),
            pltpu.VMEM((n * heads, LANES), F32),
            pltpu.VMEM((n * heads, flat), F32),
            pltpu.SemaphoreType.DMA((4,)),
            pltpu.SemaphoreType.DMA((2, SLOTS)),
            pltpu.SemaphoreType.DMA((2, SLOTS)),
            pltpu.SemaphoreType.DMA,
        ],
        compiler_params=pltpu.CompilerParams(vmem_limit_bytes=VMEM_BYTES),
        cost_estimate=pl.CostEstimate(flops=4 * rows * flat * t_len * 16 + 6 * rows * d_model * flat, bytes_accessed=8 * rows * flat * t_len, transcendentals=rows * heads * t_len),
        name='self_attention',
    )(tok_pos, bias_t, x_in, w_q, w_k, w_v, norm_self, keys, values)


CHUNK = 128
SOURCE = 16
MESH = pl.DeviceIdType.MESH


def rest_kernel(heads,
                x_ref, mixed_ref, wo_ref, wox_ref, wom_ref, co_ref, cox_ref, com_ref, cq_ref, gate_ref, up_ref, down_ref, norm_c_ref, norm_m_ref,
                mask_ref, ck_ref, cv_ref, out_ref,
                x_s, res_s, mix_s, cmix_s, wo_s, co_s, cq_s, gate_s, up_s, down_s, k_s, v_s, mask_s,
                qt_s, score_s, hid_s, part_s, near_s, chip_s, far_s, done_s,
                ag_send, ag_recv, w_send, w_recv, sum_send, sum_recv, load_sem, cross_sem, out_sem):
    me = lax.axis_index('tp')
    core = lax.rem(me, 2)
    mate = me + 1 - 2 * core
    over = lax.rem(me + 2, 4)
    cater = lax.rem(mate + 2, 4)
    rows_total, d_model = x_ref.shape
    flat = mixed_ref.shape[1]
    head_dim = flat // heads
    src_len = ck_ref.shape[0]
    d_ff = gate_ref.shape[0]
    chunks = rows_total // CHUNK
    half = CHUNK // 2

    def remote(src, dst, send_sem, recv_sem, to):
        return pltpu.make_async_remote_copy(src_ref=src, dst_ref=dst, send_sem=send_sem, recv_sem=recv_sem,
                                            device_id={'tp': to}, device_id_type=MESH)

    def block(buf, who, c):
        return buf.at[who, pl.ds(CHUNK * c, CHUNK), :]

    def shard(buf, who):
        return buf.at[pl.ds(pl.multiple_of(who * flat, flat), flat), :]

    loads = []

    def load(src, dst):
        copy = pltpu.make_async_copy(src, dst, load_sem.at[len(loads)])
        copy.start()
        loads.append(copy)
        return copy

    def cross_part(which, i):
        at = pl.ds(i * SOURCE, SOURCE)
        src, dst = ((ck_ref, k_s), (cv_ref, v_s))[which]
        return pltpu.make_async_copy(src.at[at], dst.at[at], cross_sem.at[which, i])

    barrier = pltpu.get_barrier_semaphore()
    for peer in (mate, over):
        pl.semaphore_signal(barrier, inc=1, device_id={'tp': peer}, device_id_type=MESH)
    own_mixed = load(mixed_ref, mix_s.at[me])
    own_wo = (load(wo_ref, shard(wo_s, me)), load(wox_ref, shard(wo_s, over)), load(wom_ref, shard(wo_s, mate)))
    x_load = load(x_ref, x_s)
    q_load = load(cq_ref, cq_s)
    mask_load = load(mask_ref, mask_s)
    for which in range(2):
        for i in range(src_len // SOURCE):
            cross_part(which, i).start()
    pl.semaphore_wait(barrier, 2)

    sends = []

    def send(copy):
        copy.start()
        sends.append(copy)

    def gather_send(stage, src, buf, c):
        send(remote(src, block(buf, me, c), ag_send.at[stage, 0, c], ag_recv.at[stage, 0, c], over))
        send(remote(src, block(buf, me, c), ag_send.at[stage, 1, c], ag_recv.at[stage, 1, c], mate))

    def gather_relay(stage, buf, c):
        remote(block(buf, over, c), block(buf, over, c), ag_send.at[stage, 0, c], ag_recv.at[stage, 0, c], over).wait_recv()
        send(remote(block(buf, over, c), block(buf, over, c), ag_send.at[stage, 2, c], ag_recv.at[stage, 2, c], mate))

    def gather_wait(stage, buf, c):
        remote(block(buf, mate, c), block(buf, mate, c), ag_send.at[stage, 1, c], ag_recv.at[stage, 1, c], mate).wait_recv()
        remote(block(buf, cater, c), block(buf, cater, c), ag_send.at[stage, 2, c], ag_recv.at[stage, 2, c], mate).wait_recv()

    def weight_send(which, ref_x, buf):
        send(remote(ref_x, shard(buf, over), w_send.at[which], w_recv.at[which], mate))

    def weight_wait(which, buf):
        remote(shard(buf, cater), shard(buf, cater), w_send.at[which], w_recv.at[which], mate).wait_recv()

    for c in range(chunks):
        gather_send(0, mixed_ref.at[pl.ds(CHUNK * c, CHUNK), :], mix_s, c)
    weight_send(0, wox_ref, wo_s)
    own_co = (load(co_ref, shard(co_s, me)), load(cox_ref, shard(co_s, over)), load(com_ref, shard(co_s, mate)))
    mlp_loads = (load(gate_ref, gate_s), load(up_ref, up_s), load(down_ref, down_s))

    def project_heads(buf, weight, c, add_to):
        lhs = jnp.concatenate([buf[i, CHUNK * c:CHUNK * (c + 1), :] for i in range(4)], axis=1)
        for n in range(0, d_model, 512):
            res_s[CHUNK * c:CHUNK * (c + 1), n:n + 512] = add_to[CHUNK * c:CHUNK * (c + 1), n:n + 512].astype(F32) + dot(lhs, weight[:, n:n + 512])

    def cross_query(c):
        if c == 0:
            own_mixed.wait()
            x_load.wait()
            for copy in own_wo:
                copy.wait()
        gather_wait(0, mix_s, c)
        if c == 0:
            weight_wait(0, wo_s)
            q_load.wait()
        project_heads(mix_s, wo_s, c, x_s)
        normed = rms_norm(res_s[CHUNK * c:CHUNK * (c + 1), :], norm_c_ref[...])
        qt_s[...] = dot(normed, cq_s[...]).astype(BF16).astype(F32).T

    def cross_score(c):
        if c == 0:
            mask_load.wait()
            for i in range(src_len // SOURCE):
                cross_part(0, i).wait()
        step = 8

        @pl.loop(0, src_len // step)
        def _(i):
            at = pl.ds(pl.multiple_of(i * step, step), step)
            for h in range(heads):
                d = slice(head_dim * h, head_dim * (h + 1))
                score_s[h, at, :] = jnp.sum(k_s[at, d, CHUNK * c:CHUNK * (c + 1)].astype(F32) * qt_s[d, :][None], axis=1)

    def cross_mix(c):
        step = 8
        valid = mask_s[:, CHUNK * c:CHUNK * (c + 1)] != 0
        for h in range(heads):
            scores = jnp.where(valid, score_s[h], NEG_FILL)
            exps = jnp.exp(scores - jnp.max(scores, axis=0, keepdims=True))
            probs = exps * pl.reciprocal(jnp.sum(exps, axis=0, keepdims=True))
            score_s[h] = probs.astype(BF16).astype(F32)

        def mix(i, acc):
            acc = list(acc)
            for j in range(step):
                s = i * step + j
                for h in range(heads):
                    d = slice(head_dim * h, head_dim * (h + 1))
                    acc[h] = acc[h] + v_s[s, d, CHUNK * c:CHUNK * (c + 1)].astype(F32) * score_s[h, pl.ds(s, 1), :]
            return tuple(acc)

        acc = (jnp.zeros((head_dim, CHUNK), F32),) * heads
        if c == 0:
            for i in range(src_len // SOURCE):
                cross_part(1, i).wait()
        acc = lax.fori_loop(0, src_len // step, mix, acc)
        cmix_s[me, CHUNK * c:CHUNK * (c + 1), :] = jnp.concatenate(acc, axis=0).T.astype(BF16)
        gather_send(1, block(cmix_s, me, c), cmix_s, c)

    def mlp(c):
        if c == 0:
            for copy in own_co:
                copy.wait()
            weight_wait(1, co_s)
        gather_wait(1, cmix_s, c)
        project_heads(cmix_s, co_s, c, res_s)
        if c == 0:
            for copy in mlp_loads:
                copy.wait()
        normed = rms_norm(res_s[CHUNK * c:CHUNK * (c + 1), :], norm_m_ref[...])
        for n in range(0, d_ff, 256):
            end = min(d_ff, n + 256)
            gate = dot_nt(normed, gate_s[n:end, :])
            up = dot_nt(normed, up_s[n:end, :])
            hid_s[:, n:end] = (jax.nn.gelu(gate, approximate=True) * up).astype(BF16)
        hidden = hid_s[...]
        for n in range(0, d_model, 512):
            part_s[c, :, n:n + 512] = dot(hidden, down_s[:, n:n + 512]).astype(BF16)
        give = pl.ds(pl.multiple_of((1 - core) * half, half), half)
        send(remote(part_s.at[c, give, :], near_s.at[c], sum_send.at[0, c], sum_recv.at[0, c], mate))

    keep = pl.ds(pl.multiple_of(core * half, half), half)

    def chip_sum(c):
        remote(near_s.at[c], near_s.at[c], sum_send.at[0, c], sum_recv.at[0, c], mate).wait_recv()
        chip_s[c] = (part_s[c, keep, :].astype(F32) + near_s[c].astype(F32)).astype(BF16)
        send(remote(chip_s.at[c], far_s.at[c], sum_send.at[1, c], sum_recv.at[1, c], over))

    def full_sum(c):
        remote(far_s.at[c], far_s.at[c], sum_send.at[1, c], sum_recv.at[1, c], over).wait_recv()
        mine = pl.ds(pl.multiple_of(CHUNK * c + core * half, half), half)
        done_s[mine, :] = (res_s[mine, :] + (chip_s[c].astype(F32) + far_s[c].astype(F32))).astype(BF16)
        send(remote(done_s.at[mine, :], done_s.at[mine, :], sum_send.at[2, c], sum_recv.at[2, c], mate))

    def store(c):
        other = pl.ds(pl.multiple_of(CHUNK * c + (1 - core) * half, half), half)
        remote(done_s.at[other, :], done_s.at[other, :], sum_send.at[2, c], sum_recv.at[2, c], mate).wait_recv()
        rows = pl.ds(CHUNK * c, CHUNK)
        copy = pltpu.make_async_copy(done_s.at[rows, :], out_ref.at[rows, :], out_sem.at[c])
        copy.start()
        return copy

    gather_relay(0, mix_s, 0)
    cross_query(0)
    for c in range(1, chunks):
        gather_relay(0, mix_s, c)
    weight_send(1, cox_ref, co_s)
    cross_score(0)
    cross_query(1)
    cross_mix(0)
    cross_score(1)
    cross_mix(1)
    cross_query(2)
    cross_score(2)
    gather_relay(1, cmix_s, 0)
    cross_mix(2)
    mlp(0)
    gather_relay(1, cmix_s, 1)
    cross_query(3)
    chip_sum(0)
    cross_score(3)
    cross_mix(3)
    mlp(1)
    gather_relay(1, cmix_s, 2)
    chip_sum(1)
    mlp(2)
    gather_relay(1, cmix_s, 3)
    full_sum(0)
    chip_sum(2)
    mlp(3)
    stores = [store(0)]
    full_sum(1)
    chip_sum(3)
    stores.append(store(1))
    full_sum(2)
    stores.append(store(2))
    full_sum(3)
    stores.append(store(3))
    for copy in stores:
        copy.wait()
    for copy in sends:
        copy.wait_send()


def rest_of_layer(x_in, mixed, w_o, w_o_over, w_o_mate, cross_o, cross_o_over, cross_o_mate, cross_q, gate_t, up_t, w_down, norm_cross, norm_mlp, mask_t, cross_k, cross_v, heads):
    rows, d_model = x_in.shape
    flat = mixed.shape[1]
    d_ff = gate_t.shape[0]
    src_len = cross_k.shape[0]
    chunks = rows // CHUNK
    anywhere = pl.BlockSpec(memory_space=pl.ANY)
    vmem = pl.BlockSpec(memory_space=pltpu.VMEM)
    dma = pltpu.SemaphoreType.DMA
    return pl.pallas_call(
        functools.partial(rest_kernel, heads),
        in_specs=[anywhere] * 12 + [vmem, vmem] + [anywhere] * 3,
        out_specs=anywhere,
        out_shape=jax.ShapeDtypeStruct((rows, d_model), BF16),
        scratch_shapes=[
            pltpu.VMEM((rows, d_model), BF16),
            pltpu.VMEM((rows, d_model), F32),
            pltpu.VMEM((4, rows, flat), BF16),
            pltpu.VMEM((4, rows, flat), BF16),
            pltpu.VMEM((4 * flat, d_model), BF16),
            pltpu.VMEM((4 * flat, d_model), BF16),
            pltpu.VMEM((d_model, flat), BF16),
            pltpu.VMEM((d_ff, d_model), BF16),
            pltpu.VMEM((d_ff, d_model), BF16),
            pltpu.VMEM((d_ff, d_model), BF16),
            pltpu.VMEM((src_len, flat, rows), BF16),
            pltpu.VMEM((src_len, flat, rows), BF16),
            pltpu.VMEM((src_len, rows), jnp.int32),
            pltpu.VMEM((flat, CHUNK), F32),
            pltpu.VMEM((heads, src_len, CHUNK), F32),
            pltpu.VMEM((CHUNK, d_ff), BF16),
            pltpu.VMEM((chunks, CHUNK, d_model), BF16),
            pltpu.VMEM((chunks, CHUNK // 2, d_model), BF16),
            pltpu.VMEM((chunks, CHUNK // 2, d_model), BF16),
            pltpu.VMEM((chunks, CHUNK // 2, d_model), BF16),
            pltpu.VMEM((rows, d_model), BF16),
            dma((2, 3, chunks)), dma((2, 3, chunks)),
            dma((2,)), dma((2,)),
            dma((3, chunks)), dma((3, chunks)),
            dma((16,)), dma((2, src_len // SOURCE)), dma((chunks,)),
        ],
        compiler_params=pltpu.CompilerParams(collective_id=0, has_side_effects=True, vmem_limit_bytes=VMEM_BYTES),
        cost_estimate=pl.CostEstimate(flops=2 * rows * d_model * (8 * flat + flat + 3 * d_ff), bytes_accessed=50_000_000, transcendentals=rows * d_ff),
        name='rest_of_layer',
    )(x_in, mixed, w_o, w_o_over, w_o_mate, cross_o, cross_o_over, cross_o_mate, cross_q, gate_t, up_t, w_down, norm_cross, norm_mlp, mask_t, cross_k, cross_v)


def solution(mesh):
    def local_layer(x_in, tok_pos, self_k, self_v, cross_k, cross_v, enc_mask, rel_bias, w_q, w_k, w_v, w_o, cross_q, cross_o, w_gate, w_up, w_down, norm_self, norm_cross, norm_mlp):
        rows, t_len, heads, head_dim = self_k.shape
        flat = heads * head_dim
        to_kernel = lambda c: jnp.transpose(c, (0, 2, 3, 1)).reshape(rows, flat, t_len)
        from_kernel = lambda c: jnp.transpose(c.reshape(rows, heads, head_dim, t_len), (0, 3, 1, 2))
        cross_view = lambda c: jnp.transpose(c, (1, 2, 3, 0)).reshape(c.shape[1], flat, rows)
        swap = [(0, 2), (1, 3), (2, 0), (3, 1)]
        w_o_over = lax.ppermute(w_o, 'tp', swap)
        cross_o_over = lax.ppermute(cross_o, 'tp', swap)
        mates = [(0, 1), (1, 0), (2, 3), (3, 2)]
        w_o_mate = lax.ppermute(w_o, 'tp', mates)
        cross_o_mate = lax.ppermute(cross_o, 'tp', mates)
        mixed_self, new_k, new_v = self_attention(tok_pos, rel_bias.T, x_in, w_q, w_k, w_v, norm_self, to_kernel(self_k), to_kernel(self_v), heads)
        x_out = rest_of_layer(x_in, mixed_self, w_o, w_o_over, w_o_mate, cross_o, cross_o_over, cross_o_mate, cross_q, w_gate.T, w_up.T, w_down, norm_cross, norm_mlp,
                              enc_mask.T, cross_view(cross_k), cross_view(cross_v), heads)
        return x_out, from_kernel(new_k), from_kernel(new_v)

    cache_spec = P('dp', None, 'tp', None)
    split_cols = P(None, 'tp')
    split_rows = P('tp', None)
    in_specs = (P('dp', None), P('dp'), cache_spec, cache_spec, cache_spec, cache_spec, P('dp', None), split_cols, split_cols, split_cols, split_cols, split_rows, split_cols, split_rows, split_cols, split_cols, split_rows, P(None), P(None), P(None))
    out_specs = (P('dp', None), cache_spec, cache_spec)
    return jax.shard_map(local_layer, mesh=mesh, in_specs=in_specs, out_specs=out_specs, check_vma=False)
```

```python
import functools
import math
import jax
import jax.numpy as jnp
from jax import lax
from jax.experimental import pallas as pl
from jax.experimental.pallas import tpu as pltpu
from jax.sharding import PartitionSpec as P

BUCKET_EDGES = tuple(int(math.ceil(16.0 * 8.0 ** (bucket_step / 16.0))) for bucket_step in range(1, 16))
NEG_FILL = -1e30
STEP_ROWS = 32
SLOTS = 8
AHEAD = 4
VMEM_BYTES = 67043328
LANES = 128
F32 = jnp.float32
BF16 = jnp.bfloat16


def rms_norm(values, norm_scale):
    inv_rms = lax.rsqrt(jnp.mean(values * values, axis=-1, keepdims=True) + 1e-6)
    return (values * inv_rms * norm_scale.astype(F32)).astype(BF16)


def dot(a, b):
    return jnp.dot(a, b, preferred_element_type=F32)


def dot_nt(a, b):
    return lax.dot_general(a, b, (((1,), (1,)), ((), ())), preferred_element_type=F32)


def iota(shape, axis):
    return lax.broadcasted_iota(jnp.int32, shape, axis)


def self_kernel(heads, head_dim, pos_ref, bias_ref, x_ref, wq_ref, wk_ref, wv_ref, norm_ref, k_ref, v_ref,
                mixed_ref, ko_ref, vo_ref, x_s, wq_s, wk_s, wv_s, k_s, v_s, mixed_s, q_s, kt_s, vt_s, score_s, out_s,
                load_sem, in_sem, out_sem, mixed_sem):
    flat = heads * head_dim
    rows_total = x_ref.shape[0]
    n = STEP_ROWS
    steps = rows_total // n

    def rows_of(step):
        return pl.ds(pl.multiple_of(step * n, n), n)

    def fetch(step):
        slot = lax.rem(step, SLOTS)
        return (pltpu.make_async_copy(k_ref.at[rows_of(step)], k_s.at[slot], in_sem.at[0, slot]),
                pltpu.make_async_copy(v_ref.at[rows_of(step)], v_s.at[slot], in_sem.at[1, slot]))

    def write(step):
        slot = lax.rem(step, SLOTS)
        return (pltpu.make_async_copy(k_s.at[slot], ko_ref.at[rows_of(step)], out_sem.at[0, slot]),
                pltpu.make_async_copy(v_s.at[slot], vo_ref.at[rows_of(step)], out_sem.at[1, slot]))

    loads = [pltpu.make_async_copy(src, dst, load_sem.at[i])
             for i, (src, dst) in enumerate(((x_ref, x_s), (wq_ref, wq_s), (wk_ref, wk_s), (wv_ref, wv_s)))]
    for copy in loads:
        copy.start()
    for step in range(AHEAD):
        for copy in fetch(step):
            copy.start()

    lane = iota((4 * heads, LANES), 1)
    head_of = lax.rem(iota((4 * heads, LANES), 0), heads)
    far = jnp.full_like(lane, 16)
    for edge in BUCKET_EDGES:
        far = far + jnp.where(lane >= edge, 1, 0)
    bucket = jnp.where(lane < 16, lane, far)
    table = jnp.zeros((4 * heads, LANES), F32)
    for b in range(32):
        here = jnp.zeros((4 * heads, LANES), F32)
        for h in range(heads):
            here = jnp.where(head_of == h, bias_ref[h, b], here)
        table = jnp.where(bucket == b, here, table)

    for copy in loads:
        copy.wait()

    @pl.loop(0, rows_total // LANES)
    def _(g):
        rows = pl.ds(pl.multiple_of(g * LANES, LANES), LANES)
        normed = rms_norm(x_s[rows, :].astype(F32), norm_ref[...])
        q_s[rows, :] = dot(normed, wq_s[...]).astype(BF16)
        kt_s[g] = dot(normed, wk_s[...]).astype(BF16).astype(F32).T
        vt_s[g] = dot(normed, wv_s[...]).astype(BF16).astype(F32).T

    spread = jnp.where(iota((n * heads, n), 0) // heads == iota((n * heads, n), 1), 1.0, 0.0).astype(BF16)
    gather = jnp.where(iota((n, n * heads), 1) // heads == iota((n, n * heads), 0), 1.0, 0.0).astype(BF16)
    own_head = iota((n * heads, flat), 1) // head_dim == lax.rem(iota((n * heads, flat), 0), heads)
    lane_bf = iota((flat, LANES), 1).astype(F32).astype(BF16)
    quad_row = iota((4 * heads, LANES), 0)
    per = LANES // n

    @pl.loop(0, steps)
    def _(step):
        ahead = step + AHEAD

        @pl.when(ahead < steps)
        def _():
            @pl.when(ahead >= SLOTS)
            def _():
                for copy in write(ahead - SLOTS):
                    copy.wait()
            for copy in fetch(ahead):
                copy.start()

        first = pl.multiple_of(step * n, n)
        slot = lax.rem(step, SLOTS)
        group, part = step // per, lax.rem(step, per)
        shift = lax.rem(LANES - part * n, LANES)
        k_new = pltpu.roll(kt_s[group], shift, 1).astype(BF16)
        v_new = pltpu.roll(vt_s[group], shift, 1).astype(BF16)
        q_rows = jnp.where(own_head, dot(spread, q_s[pl.ds(first, n), :]), 0.0).astype(BF16)
        in_k, in_v = fetch(step)

        def update(cache, new_cols, b):
            at_pos = lane_bf == pos_ref[first + b].astype(F32).astype(BF16)
            col = jnp.broadcast_to(new_cols[:, b:b + 1], (flat, LANES))
            updated = jnp.where(at_pos, col, cache[slot, b])
            cache[slot, b] = updated
            return updated

        in_k.wait()
        for g in range(n // 4):
            lhs = q_rows[4 * heads * g:4 * heads * (g + 1), :]
            picked = None
            distance = None
            for half in range(2):
                b = 4 * g + 2 * half
                pair = jnp.concatenate([update(k_s, k_new, b), update(k_s, k_new, b + 1)], axis=1)
                both = dot(lhs, pair)
                for j in range(2):
                    mine = both[:, LANES * j:LANES * (j + 1)]
                    at = 2 * half + j
                    pos = pos_ref[first + 4 * g + at]
                    picked = mine if picked is None else jnp.where(quad_row >= heads * at, mine, picked)
                    distance = jnp.full((4 * heads, LANES), pos, jnp.int32) if distance is None else jnp.where(quad_row >= heads * at, pos, distance)
            distance = distance - iota((4 * heads, LANES), 1)
            bias = jnp.take_along_axis(table, jnp.maximum(distance, 0), axis=1)
            score_s[4 * heads * g:4 * heads * (g + 1), :] = jnp.where(distance >= 0, picked + bias, NEG_FILL)
        write(step)[0].start()

        scores = score_s[...]
        exps = jnp.exp(scores - jnp.max(scores, axis=1, keepdims=True))
        probs = exps * pl.reciprocal(jnp.sum(exps, axis=1, keepdims=True))

        in_v.wait()
        for g in range(n // 4):
            quad = probs[4 * heads * g:4 * heads * (g + 1), :]
            picked = None
            for half in range(2):
                b = 4 * g + 2 * half
                pair = jnp.concatenate([update(v_s, v_new, b), update(v_s, v_new, b + 1)], axis=1)
                low = jnp.where(quad_row // heads == 2 * half, quad, 0.0)
                high = jnp.where(quad_row // heads == 2 * half + 1, quad, 0.0)
                lhs = jnp.concatenate([low, high], axis=1).astype(BF16)
                both = dot_nt(lhs, pair)
                picked = both if half == 0 else jnp.where(iota(both.shape, 0) >= 2 * heads, both, picked)
            out_s[4 * heads * g:4 * heads * (g + 1), :] = picked
        write(step)[1].start()
        mixed_s[pl.ds(first, n), :] = dot(gather, jnp.where(own_head, out_s[...], 0.0).astype(BF16)).astype(BF16)

    mixed_copy = pltpu.make_async_copy(mixed_s, mixed_ref, mixed_sem)
    mixed_copy.start()
    for step in range(steps - SLOTS, steps):
        for copy in write(step):
            copy.wait()
    mixed_copy.wait()


def self_attention(tok_pos, bias_t, x_in, w_q, w_k, w_v, norm_self, keys, values, heads):
    rows, flat, t_len = keys.shape
    d_model = x_in.shape[1]
    n = STEP_ROWS
    smem = pl.BlockSpec(memory_space=pltpu.SMEM)
    anywhere = pl.BlockSpec(memory_space=pl.ANY)
    cache_shape = jax.ShapeDtypeStruct(keys.shape, BF16)
    return pl.pallas_call(
        functools.partial(self_kernel, heads, flat // heads),
        in_specs=[smem, smem] + [anywhere] * 4 + [pl.BlockSpec(memory_space=pltpu.VMEM)] + [anywhere] * 2,
        out_specs=[anywhere] * 3,
        out_shape=[jax.ShapeDtypeStruct((rows, flat), BF16), cache_shape, cache_shape],
        scratch_shapes=[
            pltpu.VMEM((rows, d_model), BF16),
            pltpu.VMEM((d_model, flat), BF16),
            pltpu.VMEM((d_model, flat), BF16),
            pltpu.VMEM((d_model, flat), BF16),
            pltpu.VMEM((SLOTS, n, flat, t_len), BF16),
            pltpu.VMEM((SLOTS, n, flat, t_len), BF16),
            pltpu.VMEM((rows, flat), BF16),
            pltpu.VMEM((rows, flat), BF16),
            pltpu.VMEM((rows // LANES, flat, LANES), F32),
            pltpu.VMEM((rows // LANES, flat, LANES), F32),
            pltpu.VMEM((n * heads, LANES), F32),
            pltpu.VMEM((n * heads, flat), F32),
            pltpu.SemaphoreType.DMA((4,)),
            pltpu.SemaphoreType.DMA((2, SLOTS)),
            pltpu.SemaphoreType.DMA((2, SLOTS)),
            pltpu.SemaphoreType.DMA,
        ],
        compiler_params=pltpu.CompilerParams(vmem_limit_bytes=VMEM_BYTES),
        cost_estimate=pl.CostEstimate(flops=4 * rows * flat * t_len * 16 + 6 * rows * d_model * flat, bytes_accessed=8 * rows * flat * t_len, transcendentals=rows * heads * t_len),
        name='self_attention',
    )(tok_pos, bias_t, x_in, w_q, w_k, w_v, norm_self, keys, values)


CHUNK = 128
MESH = pl.DeviceIdType.MESH


def rest_kernel(heads, n_cross_slots,
                x_ref, mixed_ref, wo_ref, wox_ref, wom_ref, co_ref, cox_ref, com_ref, cq_ref, gate_ref, up_ref, down_ref, norm_c_ref, norm_m_ref,
                mask_ref, ck_ref, cv_ref, out_ref,
                x_s, res_s, part_f, mix_s, cmix_s, wo_s, co_s, cq_s, gate_s, up_s, gate_t, up_t, down_s, k_s, v_s, mask_s,
                qt_s, score_s, hid_s, part_s, near_s, chip_s, far_s, done_s,
                ag_send, ag_recv, w_send, w_recv, sum_send, sum_recv, load_sem, cross_sem, out_sem):
    me = lax.axis_index('tp')
    core = lax.rem(me, 2)
    mate = me + 1 - 2 * core
    over = lax.rem(me + 2, 4)
    cater = lax.rem(mate + 2, 4)
    rows_total, d_model = x_ref.shape
    flat = mixed_ref.shape[1]
    head_dim = flat // heads
    src_len = ck_ref.shape[0]
    d_ff = gate_ref.shape[0]
    chunks = rows_total // CHUNK
    half = CHUNK // 2

    def remote(src, dst, send_sem, recv_sem, to):
        return pltpu.make_async_remote_copy(src_ref=src, dst_ref=dst, send_sem=send_sem, recv_sem=recv_sem,
                                            device_id={'tp': to}, device_id_type=MESH)

    def block(buf, who, c):
        return buf.at[who, pl.ds(CHUNK * c, CHUNK), :]

    def shard(buf, who):
        return buf.at[pl.ds(pl.multiple_of(who * flat, flat), flat), :]

    loads = []

    def load(src, dst):
        copy = pltpu.make_async_copy(src, dst, load_sem.at[len(loads)])
        copy.start()
        loads.append(copy)
        return copy

    def cross_load(c):
        slot = c % n_cross_slots
        cols = pl.ds(CHUNK * c, CHUNK)
        return (pltpu.make_async_copy(ck_ref.at[:, :, cols], k_s.at[slot], cross_sem.at[0, slot]),
                pltpu.make_async_copy(cv_ref.at[:, :, cols], v_s.at[slot], cross_sem.at[1, slot]))

    def cross_start(c):
        for copy in cross_load(c):
            copy.start()

    barrier = pltpu.get_barrier_semaphore()
    for peer in (mate, over):
        pl.semaphore_signal(barrier, inc=1, device_id={'tp': peer}, device_id_type=MESH)
    pl.semaphore_wait(barrier, 2)

    sends = []

    def send(copy):
        copy.start()
        sends.append(copy)

    def gather_send(stage, src, buf, c):
        send(remote(src, block(buf, me, c), ag_send.at[stage, 0, c], ag_recv.at[stage, 0, c], over))
        send(remote(src, block(buf, me, c), ag_send.at[stage, 1, c], ag_recv.at[stage, 1, c], mate))

    def gather_relay(stage, buf, c):
        remote(block(buf, over, c), block(buf, over, c), ag_send.at[stage, 0, c], ag_recv.at[stage, 0, c], over).wait_recv()
        send(remote(block(buf, over, c), block(buf, over, c), ag_send.at[stage, 2, c], ag_recv.at[stage, 2, c], mate))

    def gather_near(stage, buf, c):
        remote(block(buf, mate, c), block(buf, mate, c), ag_send.at[stage, 1, c], ag_recv.at[stage, 1, c], mate).wait_recv()

    def gather_far(stage, buf, c):
        remote(block(buf, cater, c), block(buf, cater, c), ag_send.at[stage, 2, c], ag_recv.at[stage, 2, c], mate).wait_recv()

    def weight_send(which, ref_x, buf):
        send(remote(ref_x, shard(buf, over), w_send.at[which], w_recv.at[which], mate))

    def weight_wait(which, buf):
        remote(shard(buf, cater), shard(buf, cater), w_send.at[which], w_recv.at[which], mate).wait_recv()

    for c in range(chunks):
        gather_send(0, mixed_ref.at[pl.ds(CHUNK * c, CHUNK), :], mix_s, c)
    own_mixed = load(mixed_ref, mix_s.at[me])
    own_wo = (load(wo_ref, shard(wo_s, me)), load(wox_ref, shard(wo_s, over)), load(wom_ref, shard(wo_s, mate)))
    x_load = load(x_ref, x_s)
    q_load = load(cq_ref, cq_s)
    mask_load = load(mask_ref, mask_s)
    weight_send(0, wox_ref, wo_s)
    gate_load = load(gate_ref, gate_s)
    up_load = load(up_ref, up_s)
    cross_start(0)

    def turn(wide, tall):
        @pl.loop(0, d_model // CHUNK)
        def _(i):
            at = pl.ds(pl.multiple_of(i * CHUNK, CHUNK), CHUNK)
            tall[at, :] = wide[:, at].T

    def chip_dot(buf, weight, first, c, n):
        lhs = jnp.concatenate([buf[first, CHUNK * c:CHUNK * (c + 1), :], buf[first + 1, CHUNK * c:CHUNK * (c + 1), :]], axis=1)
        return dot(lhs, weight[pl.ds(pl.multiple_of(first * flat, flat), 2 * flat), n:n + 512])

    def chip_product(buf, weight, c):
        for n in range(0, d_model, 512):
            part_f[CHUNK * c:CHUNK * (c + 1), n:n + 512] = chip_dot(buf, weight, me - core, c, n)

    def add_other_chip(buf, weight, c, add_to):
        rows = slice(CHUNK * c, CHUNK * (c + 1))
        for n in range(0, d_model, 512):
            both = part_f[rows, n:n + 512] + chip_dot(buf, weight, over - core, c, n)
            res_s[rows, n:n + 512] = add_to[rows, n:n + 512].astype(F32) + both

    def early_product(c):
        if c == 0:
            own_mixed.wait()
            for copy in own_wo:
                copy.wait()
        gather_near(0, mix_s, c)
        chip_product(mix_s, wo_s, c)

    def cross_query(c):
        if c == 0:
            x_load.wait()
        gather_far(0, mix_s, c)
        if c == 0:
            weight_wait(0, wo_s)
            q_load.wait()
        add_other_chip(mix_s, wo_s, c, x_s)
        normed = rms_norm(res_s[CHUNK * c:CHUNK * (c + 1), :], norm_c_ref[...])
        qt_s[...] = dot(normed, cq_s[...]).astype(BF16).astype(F32).T

    def cross_score(c):
        slot = c % n_cross_slots
        for copy in cross_load(c):
            copy.wait()
        if c == 0:
            mask_load.wait()
        step = 8

        @pl.loop(0, src_len // step)
        def _(i):
            at = pl.ds(pl.multiple_of(i * step, step), step)
            for h in range(heads):
                d = slice(head_dim * h, head_dim * (h + 1))
                score_s[h, at, :] = jnp.sum(k_s[slot, at, d, :].astype(F32) * qt_s[d, :][None], axis=1)

    def cross_mix(c):
        slot = c % n_cross_slots
        step = 8
        valid = mask_s[:, CHUNK * c:CHUNK * (c + 1)] != 0
        for h in range(heads):
            scores = jnp.where(valid, score_s[h], NEG_FILL)
            exps = jnp.exp(scores - jnp.max(scores, axis=0, keepdims=True))
            probs = exps * pl.reciprocal(jnp.sum(exps, axis=0, keepdims=True))
            score_s[h] = probs.astype(BF16).astype(F32)

        def mix(i, acc):
            acc = list(acc)
            for j in range(step):
                s = i * step + j
                for h in range(heads):
                    d = slice(head_dim * h, head_dim * (h + 1))
                    acc[h] = acc[h] + v_s[slot, s, d, :].astype(F32) * score_s[h, pl.ds(s, 1), :]
            return tuple(acc)

        zero = jnp.zeros((head_dim, CHUNK), F32)
        acc = lax.fori_loop(0, src_len // step, mix, (zero,) * heads)
        cmix_s[me, CHUNK * c:CHUNK * (c + 1), :] = jnp.concatenate(acc, axis=0).T.astype(BF16)
        gather_send(1, block(cmix_s, me, c), cmix_s, c)

    def mlp_up(c):
        if c == 0:
            for copy in own_co:
                copy.wait()
        gather_near(1, cmix_s, c)
        chip_product(cmix_s, co_s, c)
        if c == 0:
            weight_wait(1, co_s)
        gather_far(1, cmix_s, c)
        add_other_chip(cmix_s, co_s, c, res_s)
        normed = rms_norm(res_s[CHUNK * c:CHUNK * (c + 1), :], norm_m_ref[...])
        for n in range(0, d_ff, 256):
            end = min(d_ff, n + 256)
            gate = dot(normed, gate_t[:, n:end])
            up = dot(normed, up_t[:, n:end])
            hid_s[:, n:end] = (jax.nn.gelu(gate, approximate=True) * up).astype(BF16)

    def mlp_down(c):
        hidden = hid_s[...]
        if c == 0:
            down_load.wait()
        for n in range(0, d_model, 512):
            part_s[c, :, n:n + 512] = dot(hidden, down_s[:, n:n + 512]).astype(BF16)
        give = pl.ds(pl.multiple_of((1 - core) * half, half), half)
        send(remote(part_s.at[c, give, :], near_s.at[c], sum_send.at[0, c], sum_recv.at[0, c], mate))

    keep = pl.ds(pl.multiple_of(core * half, half), half)

    def chip_sum(c):
        remote(near_s.at[c], near_s.at[c], sum_send.at[0, c], sum_recv.at[0, c], mate).wait_recv()
        chip_s[c] = (part_s[c, keep, :].astype(F32) + near_s[c].astype(F32)).astype(BF16)
        send(remote(chip_s.at[c], far_s.at[c], sum_send.at[1, c], sum_recv.at[1, c], over))

    def full_sum(c):
        remote(far_s.at[c], far_s.at[c], sum_send.at[1, c], sum_recv.at[1, c], over).wait_recv()
        mine = pl.ds(pl.multiple_of(CHUNK * c + core * half, half), half)
        done_s[mine, :] = (res_s[mine, :] + (chip_s[c].astype(F32) + far_s[c].astype(F32))).astype(BF16)
        send(remote(done_s.at[mine, :], done_s.at[mine, :], sum_send.at[2, c], sum_recv.at[2, c], mate))

    def store(c):
        other = pl.ds(pl.multiple_of(CHUNK * c + (1 - core) * half, half), half)
        remote(done_s.at[other, :], done_s.at[other, :], sum_send.at[2, c], sum_recv.at[2, c], mate).wait_recv()
        rows = pl.ds(CHUNK * c, CHUNK)
        copy = pltpu.make_async_copy(done_s.at[rows, :], out_ref.at[rows, :], out_sem.at[c])
        copy.start()
        return copy

    for c in range(chunks):
        early_product(c)
    gate_load.wait()
    turn(gate_s, gate_t)
    gather_relay(0, mix_s, 0)
    up_load.wait()
    turn(up_s, up_t)
    cross_query(0)
    for c in range(1, chunks):
        gather_relay(0, mix_s, c)
    weight_send(1, cox_ref, co_s)
    cross_start(1)
    cross_score(0)
    cross_mix(0)
    own_co = (load(co_ref, shard(co_s, me)), load(cox_ref, shard(co_s, over)), load(com_ref, shard(co_s, mate)))
    cross_start(2)
    cross_query(1)
    cross_score(1)
    gather_relay(1, cmix_s, 0)
    cross_mix(1)
    down_load = load(down_ref, down_s)
    cross_start(3)
    mlp_up(0)
    mlp_down(0)
    gather_relay(1, cmix_s, 1)
    cross_query(2)
    chip_sum(0)
    cross_score(2)
    cross_mix(2)
    cross_query(3)
    cross_score(3)
    gather_relay(1, cmix_s, 2)
    cross_mix(3)
    mlp_up(1)
    mlp_down(1)
    mlp_up(2)
    chip_sum(1)
    mlp_down(2)
    gather_relay(1, cmix_s, 3)
    full_sum(0)
    mlp_up(3)
    chip_sum(2)
    mlp_down(3)
    stores = [store(0)]
    full_sum(1)
    chip_sum(3)
    stores.append(store(1))
    full_sum(2)
    stores.append(store(2))
    full_sum(3)
    stores.append(store(3))
    for copy in stores:
        copy.wait()
    for copy in sends:
        copy.wait_send()


def rest_of_layer(x_in, mixed, w_o, w_o_over, w_o_mate, cross_o, cross_o_over, cross_o_mate, cross_q, gate_t, up_t, w_down, norm_cross, norm_mlp, mask_t, cross_k, cross_v, heads):
    rows, d_model = x_in.shape
    flat = mixed.shape[1]
    d_ff = gate_t.shape[0]
    src_len = cross_k.shape[0]
    chunks = rows // CHUNK
    slots = 2
    anywhere = pl.BlockSpec(memory_space=pl.ANY)
    vmem = pl.BlockSpec(memory_space=pltpu.VMEM)
    dma = pltpu.SemaphoreType.DMA
    return pl.pallas_call(
        functools.partial(rest_kernel, heads, slots),
        in_specs=[anywhere] * 12 + [vmem, vmem] + [anywhere] * 3,
        out_specs=anywhere,
        out_shape=jax.ShapeDtypeStruct((rows, d_model), BF16),
        scratch_shapes=[
            pltpu.VMEM((rows, d_model), BF16),
            pltpu.VMEM((rows, d_model), F32),
            pltpu.VMEM((rows, d_model), F32),
            pltpu.VMEM((4, rows, flat), BF16),
            pltpu.VMEM((4, rows, flat), BF16),
            pltpu.VMEM((4 * flat, d_model), BF16),
            pltpu.VMEM((4 * flat, d_model), BF16),
            pltpu.VMEM((d_model, flat), BF16),
            pltpu.VMEM((d_ff, d_model), BF16),
            pltpu.VMEM((d_ff, d_model), BF16),
            pltpu.VMEM((d_model, d_ff), BF16),
            pltpu.VMEM((d_model, d_ff), BF16),
            pltpu.VMEM((d_ff, d_model), BF16),
            pltpu.VMEM((slots, src_len, flat, CHUNK), BF16),
            pltpu.VMEM((slots, src_len, flat, CHUNK), BF16),
            pltpu.VMEM((src_len, rows), jnp.int32),
            pltpu.VMEM((flat, CHUNK), F32),
            pltpu.VMEM((heads, src_len, CHUNK), F32),
            pltpu.VMEM((CHUNK, d_ff), BF16),
            pltpu.VMEM((chunks, CHUNK, d_model), BF16),
            pltpu.VMEM((chunks, CHUNK // 2, d_model), BF16),
            pltpu.VMEM((chunks, CHUNK // 2, d_model), BF16),
            pltpu.VMEM((chunks, CHUNK // 2, d_model), BF16),
            pltpu.VMEM((rows, d_model), BF16),
            dma((2, 3, chunks)), dma((2, 3, chunks)),
            dma((2,)), dma((2,)),
            dma((3, chunks)), dma((3, chunks)),
            dma((16,)), dma((2, slots)), dma((chunks,)),
        ],
        compiler_params=pltpu.CompilerParams(collective_id=0, has_side_effects=True, vmem_limit_bytes=VMEM_BYTES),
        cost_estimate=pl.CostEstimate(flops=2 * rows * d_model * (8 * flat + flat + 3 * d_ff), bytes_accessed=50_000_000, transcendentals=rows * d_ff),
        name='rest_of_layer',
    )(x_in, mixed, w_o, w_o_over, w_o_mate, cross_o, cross_o_over, cross_o_mate, cross_q, gate_t, up_t, w_down, norm_cross, norm_mlp, mask_t, cross_k, cross_v)


def solution(mesh):
    def local_layer(x_in, tok_pos, self_k, self_v, cross_k, cross_v, enc_mask, rel_bias, w_q, w_k, w_v, w_o, cross_q, cross_o, w_gate, w_up, w_down, norm_self, norm_cross, norm_mlp):
        rows, t_len, heads, head_dim = self_k.shape
        flat = heads * head_dim
        to_kernel = lambda c: jnp.transpose(c, (0, 2, 3, 1)).reshape(rows, flat, t_len)
        from_kernel = lambda c: jnp.transpose(c.reshape(rows, heads, head_dim, t_len), (0, 3, 1, 2))
        cross_view = lambda c: jnp.transpose(c, (1, 2, 3, 0)).reshape(c.shape[1], flat, rows)
        swap = [(0, 2), (1, 3), (2, 0), (3, 1)]
        w_o_over = lax.ppermute(w_o, 'tp', swap)
        cross_o_over = lax.ppermute(cross_o, 'tp', swap)
        mates = [(0, 1), (1, 0), (2, 3), (3, 2)]
        w_o_mate = lax.ppermute(w_o, 'tp', mates)
        cross_o_mate = lax.ppermute(cross_o, 'tp', mates)
        mixed_self, new_k, new_v = self_attention(tok_pos, rel_bias.T, x_in, w_q, w_k, w_v, norm_self, to_kernel(self_k), to_kernel(self_v), heads)
        x_out = rest_of_layer(x_in, mixed_self, w_o, w_o_over, w_o_mate, cross_o, cross_o_over, cross_o_mate, cross_q, w_gate.T, w_up.T, w_down, norm_cross, norm_mlp,
                              enc_mask.T, cross_view(cross_k), cross_view(cross_v), heads)
        return x_out, from_kernel(new_k), from_kernel(new_v)

    cache_spec = P('dp', None, 'tp', None)
    split_cols = P(None, 'tp')
    split_rows = P('tp', None)
    in_specs = (P('dp', None), P('dp'), cache_spec, cache_spec, cache_spec, cache_spec, P('dp', None), split_cols, split_cols, split_cols, split_cols, split_rows, split_cols, split_rows, split_cols, split_cols, split_rows, P(None), P(None), P(None))
    out_specs = (P('dp', None), cache_spec, cache_spec)
    return jax.shard_map(local_layer, mesh=mesh, in_specs=in_specs, out_specs=out_specs, check_vma=False)
```

```python
import functools
import math
import jax
import jax.numpy as jnp
from jax import lax
from jax.experimental import pallas as pl
from jax.experimental.pallas import tpu as pltpu
from jax.sharding import PartitionSpec as P

BUCKET_EDGES = tuple(int(math.ceil(16.0 * 8.0 ** (bucket_step / 16.0))) for bucket_step in range(1, 16))
NEG_FILL = -1e30
STEP_ROWS = 32
SLOTS = 8
AHEAD = 4
VMEM_BYTES = 67043328
LANES = 128
F32 = jnp.float32
BF16 = jnp.bfloat16


def rms_norm(values, norm_scale):
    inv_rms = lax.rsqrt(jnp.mean(values * values, axis=-1, keepdims=True) + 1e-6)
    return (values * inv_rms * norm_scale.astype(F32)).astype(BF16)


def dot(a, b):
    return jnp.dot(a, b, preferred_element_type=F32)


def dot_nt(a, b):
    return lax.dot_general(a, b, (((1,), (1,)), ((), ())), preferred_element_type=F32)


def iota(shape, axis):
    return lax.broadcasted_iota(jnp.int32, shape, axis)


def self_kernel(heads, head_dim, pos_ref, bias_ref, x_ref, wq_ref, wk_ref, wv_ref, norm_ref, k_ref, v_ref,
                mixed_ref, ko_ref, vo_ref, x_s, wq_s, wk_s, wv_s, k_s, v_s, mixed_s, q_s, kt_s, vt_s, score_s, out_s,
                load_sem, in_sem, out_sem, mixed_sem):
    flat = heads * head_dim
    rows_total = x_ref.shape[0]
    n = STEP_ROWS
    steps = rows_total // n

    def rows_of(step):
        return pl.ds(pl.multiple_of(step * n, n), n)

    def fetch(step):
        slot = lax.rem(step, SLOTS)
        return (pltpu.make_async_copy(k_ref.at[rows_of(step)], k_s.at[slot], in_sem.at[0, slot]),
                pltpu.make_async_copy(v_ref.at[rows_of(step)], v_s.at[slot], in_sem.at[1, slot]))

    def write(step):
        slot = lax.rem(step, SLOTS)
        return (pltpu.make_async_copy(k_s.at[slot], ko_ref.at[rows_of(step)], out_sem.at[0, slot]),
                pltpu.make_async_copy(v_s.at[slot], vo_ref.at[rows_of(step)], out_sem.at[1, slot]))

    loads = [pltpu.make_async_copy(src, dst, load_sem.at[i])
             for i, (src, dst) in enumerate(((x_ref, x_s), (wq_ref, wq_s), (wk_ref, wk_s), (wv_ref, wv_s)))]
    for copy in loads:
        copy.start()
    for step in range(AHEAD):
        for copy in fetch(step):
            copy.start()

    lane = iota((4 * heads, LANES), 1)
    head_of = lax.rem(iota((4 * heads, LANES), 0), heads)
    far = jnp.full_like(lane, 16)
    for edge in BUCKET_EDGES:
        far = far + jnp.where(lane >= edge, 1, 0)
    bucket = jnp.where(lane < 16, lane, far)
    table = jnp.zeros((4 * heads, LANES), F32)
    for b in range(32):
        here = jnp.zeros((4 * heads, LANES), F32)
        for h in range(heads):
            here = jnp.where(head_of == h, bias_ref[h, b], here)
        table = jnp.where(bucket == b, here, table)

    for copy in loads:
        copy.wait()

    @pl.loop(0, rows_total // LANES)
    def _(g):
        rows = pl.ds(pl.multiple_of(g * LANES, LANES), LANES)
        normed = rms_norm(x_s[rows, :].astype(F32), norm_ref[...])
        q_s[rows, :] = dot(normed, wq_s[...]).astype(BF16)
        kt_s[g] = dot(normed, wk_s[...]).astype(BF16).astype(F32).T
        vt_s[g] = dot(normed, wv_s[...]).astype(BF16).astype(F32).T

    spread = jnp.where(iota((n * heads, n), 0) // heads == iota((n * heads, n), 1), 1.0, 0.0).astype(BF16)
    gather = jnp.where(iota((n, n * heads), 1) // heads == iota((n, n * heads), 0), 1.0, 0.0).astype(BF16)
    own_head = iota((n * heads, flat), 1) // head_dim == lax.rem(iota((n * heads, flat), 0), heads)
    lane_bf = iota((flat, LANES), 1).astype(F32).astype(BF16)
    quad_row = iota((4 * heads, LANES), 0)
    per = LANES // n

    @pl.loop(0, steps)
    def _(step):
        ahead = step + AHEAD

        @pl.when(ahead < steps)
        def _():
            @pl.when(ahead >= SLOTS)
            def _():
                for copy in write(ahead - SLOTS):
                    copy.wait()
            for copy in fetch(ahead):
                copy.start()

        first = pl.multiple_of(step * n, n)
        slot = lax.rem(step, SLOTS)
        group, part = step // per, lax.rem(step, per)
        shift = lax.rem(LANES - part * n, LANES)
        k_new = pltpu.roll(kt_s[group], shift, 1).astype(BF16)
        v_new = pltpu.roll(vt_s[group], shift, 1).astype(BF16)
        q_rows = jnp.where(own_head, dot(spread, q_s[pl.ds(first, n), :]), 0.0).astype(BF16)
        in_k, in_v = fetch(step)

        def update(cache, new_cols, b):
            at_pos = lane_bf == pos_ref[first + b].astype(F32).astype(BF16)
            col = jnp.broadcast_to(new_cols[:, b:b + 1], (flat, LANES))
            updated = jnp.where(at_pos, col, cache[slot, b])
            cache[slot, b] = updated
            return updated

        in_k.wait()
        for g in range(n // 4):
            lhs = q_rows[4 * heads * g:4 * heads * (g + 1), :]
            picked = None
            distance = None
            for half in range(2):
                b = 4 * g + 2 * half
                pair = jnp.concatenate([update(k_s, k_new, b), update(k_s, k_new, b + 1)], axis=1)
                both = dot(lhs, pair)
                for j in range(2):
                    mine = both[:, LANES * j:LANES * (j + 1)]
                    at = 2 * half + j
                    pos = pos_ref[first + 4 * g + at]
                    picked = mine if picked is None else jnp.where(quad_row >= heads * at, mine, picked)
                    distance = jnp.full((4 * heads, LANES), pos, jnp.int32) if distance is None else jnp.where(quad_row >= heads * at, pos, distance)
            distance = distance - iota((4 * heads, LANES), 1)
            bias = jnp.take_along_axis(table, jnp.maximum(distance, 0), axis=1)
            score_s[4 * heads * g:4 * heads * (g + 1), :] = jnp.where(distance >= 0, picked + bias, NEG_FILL)
        write(step)[0].start()

        scores = score_s[...]
        exps = jnp.exp(scores - jnp.max(scores, axis=1, keepdims=True))
        probs = exps * pl.reciprocal(jnp.sum(exps, axis=1, keepdims=True))

        in_v.wait()
        for g in range(n // 4):
            quad = probs[4 * heads * g:4 * heads * (g + 1), :]
            picked = None
            for half in range(2):
                b = 4 * g + 2 * half
                pair = jnp.concatenate([update(v_s, v_new, b), update(v_s, v_new, b + 1)], axis=1)
                low = jnp.where(quad_row // heads == 2 * half, quad, 0.0)
                high = jnp.where(quad_row // heads == 2 * half + 1, quad, 0.0)
                lhs = jnp.concatenate([low, high], axis=1).astype(BF16)
                both = dot_nt(lhs, pair)
                picked = both if half == 0 else jnp.where(iota(both.shape, 0) >= 2 * heads, both, picked)
            out_s[4 * heads * g:4 * heads * (g + 1), :] = picked
        write(step)[1].start()
        mixed_s[pl.ds(first, n), :] = dot(gather, jnp.where(own_head, out_s[...], 0.0).astype(BF16)).astype(BF16)

    mixed_copy = pltpu.make_async_copy(mixed_s, mixed_ref, mixed_sem)
    mixed_copy.start()
    for step in range(steps - SLOTS, steps):
        for copy in write(step):
            copy.wait()
    mixed_copy.wait()


def self_attention(tok_pos, bias_t, x_in, w_q, w_k, w_v, norm_self, keys, values, heads):
    rows, flat, t_len = keys.shape
    d_model = x_in.shape[1]
    n = STEP_ROWS
    smem = pl.BlockSpec(memory_space=pltpu.SMEM)
    anywhere = pl.BlockSpec(memory_space=pl.ANY)
    cache_shape = jax.ShapeDtypeStruct(keys.shape, BF16)
    return pl.pallas_call(
        functools.partial(self_kernel, heads, flat // heads),
        in_specs=[smem, smem] + [anywhere] * 4 + [pl.BlockSpec(memory_space=pltpu.VMEM)] + [anywhere] * 2,
        out_specs=[anywhere] * 3,
        out_shape=[jax.ShapeDtypeStruct((rows, flat), BF16), cache_shape, cache_shape],
        scratch_shapes=[
            pltpu.VMEM((rows, d_model), BF16),
            pltpu.VMEM((d_model, flat), BF16),
            pltpu.VMEM((d_model, flat), BF16),
            pltpu.VMEM((d_model, flat), BF16),
            pltpu.VMEM((SLOTS, n, flat, t_len), BF16),
            pltpu.VMEM((SLOTS, n, flat, t_len), BF16),
            pltpu.VMEM((rows, flat), BF16),
            pltpu.VMEM((rows, flat), BF16),
            pltpu.VMEM((rows // LANES, flat, LANES), F32),
            pltpu.VMEM((rows // LANES, flat, LANES), F32),
            pltpu.VMEM((n * heads, LANES), F32),
            pltpu.VMEM((n * heads, flat), F32),
            pltpu.SemaphoreType.DMA((4,)),
            pltpu.SemaphoreType.DMA((2, SLOTS)),
            pltpu.SemaphoreType.DMA((2, SLOTS)),
            pltpu.SemaphoreType.DMA,
        ],
        compiler_params=pltpu.CompilerParams(vmem_limit_bytes=VMEM_BYTES),
        cost_estimate=pl.CostEstimate(flops=4 * rows * flat * t_len * 16 + 6 * rows * d_model * flat, bytes_accessed=8 * rows * flat * t_len, transcendentals=rows * heads * t_len),
        name='self_attention',
    )(tok_pos, bias_t, x_in, w_q, w_k, w_v, norm_self, keys, values)


CHUNK = 128
MESH = pl.DeviceIdType.MESH


def rest_kernel(heads, n_cross_slots,
                x_ref, mixed_ref, wo_ref, wox_ref, co_ref, cox_ref, cq_ref, gate_ref, up_ref, down_ref, norm_c_ref, norm_m_ref,
                mask_ref, ck_ref, cv_ref, out_ref,
                x_s, res_s, mix_s, cmix_s, wo_s, co_s, cq_s, gate_s, up_s, gate_t, down_s, k_s, v_s, mask_s,
                qt_s, score_s, hid_s, part_s, near_s, chip_s, far_s, done_s,
                ag_send, ag_recv, w_send, w_recv, sum_send, sum_recv, load_sem, cross_sem, out_sem):
    me = lax.axis_index('tp')
    core = lax.rem(me, 2)
    mate = me + 1 - 2 * core
    over = lax.rem(me + 2, 4)
    cater = lax.rem(mate + 2, 4)
    rows_total, d_model = x_ref.shape
    flat = mixed_ref.shape[1]
    head_dim = flat // heads
    src_len = ck_ref.shape[0]
    d_ff = gate_ref.shape[0]
    chunks = rows_total // CHUNK
    half = CHUNK // 2

    def remote(src, dst, send_sem, recv_sem, to):
        return pltpu.make_async_remote_copy(src_ref=src, dst_ref=dst, send_sem=send_sem, recv_sem=recv_sem,
                                            device_id={'tp': to}, device_id_type=MESH)

    def block(buf, who, c):
        return buf.at[who, pl.ds(CHUNK * c, CHUNK), :]

    def shard(buf, who):
        return buf.at[pl.ds(pl.multiple_of(who * flat, flat), flat), :]

    loads = []

    def load(src, dst):
        copy = pltpu.make_async_copy(src, dst, load_sem.at[len(loads)])
        copy.start()
        loads.append(copy)
        return copy

    def cross_load(c):
        slot = c % n_cross_slots
        cols = pl.ds(CHUNK * c, CHUNK)
        return (pltpu.make_async_copy(ck_ref.at[:, :, cols], k_s.at[slot], cross_sem.at[0, slot]),
                pltpu.make_async_copy(cv_ref.at[:, :, cols], v_s.at[slot], cross_sem.at[1, slot]))

    def cross_start(c):
        for copy in cross_load(c):
            copy.start()

    barrier = pltpu.get_barrier_semaphore()
    for peer in (mate, over):
        pl.semaphore_signal(barrier, inc=1, device_id={'tp': peer}, device_id_type=MESH)
    pl.semaphore_wait(barrier, 2)

    sends = []

    def send(copy):
        copy.start()
        sends.append(copy)

    def gather_send(stage, src, buf, c):
        send(remote(src, block(buf, me, c), ag_send.at[stage, 0, c], ag_recv.at[stage, 0, c], over))
        send(remote(src, block(buf, me, c), ag_send.at[stage, 1, c], ag_recv.at[stage, 1, c], mate))

    def gather_relay(stage, buf, c):
        remote(block(buf, over, c), block(buf, over, c), ag_send.at[stage, 0, c], ag_recv.at[stage, 0, c], over).wait_recv()
        send(remote(block(buf, over, c), block(buf, over, c), ag_send.at[stage, 2, c], ag_recv.at[stage, 2, c], mate))

    def gather_wait(stage, buf, c):
        remote(block(buf, mate, c), block(buf, mate, c), ag_send.at[stage, 1, c], ag_recv.at[stage, 1, c], mate).wait_recv()
        remote(block(buf, cater, c), block(buf, cater, c), ag_send.at[stage, 2, c], ag_recv.at[stage, 2, c], mate).wait_recv()

    def weight_send(which, ref, ref_x, buf):
        send(remote(ref, shard(buf, me), w_send.at[which, 0], w_recv.at[which, 0], mate))
        send(remote(ref_x, shard(buf, over), w_send.at[which, 1], w_recv.at[which, 1], mate))

    def weight_wait(which, buf):
        remote(shard(buf, mate), shard(buf, mate), w_send.at[which, 0], w_recv.at[which, 0], mate).wait_recv()
        remote(shard(buf, cater), shard(buf, cater), w_send.at[which, 1], w_recv.at[which, 1], mate).wait_recv()

    for c in range(chunks):
        gather_send(0, mixed_ref.at[pl.ds(CHUNK * c, CHUNK), :], mix_s, c)
    own_mixed = load(mixed_ref, mix_s.at[me])
    own_wo = (load(wo_ref, shard(wo_s, me)), load(wox_ref, shard(wo_s, over)))
    x_load = load(x_ref, x_s)
    q_load = load(cq_ref, cq_s)
    mask_load = load(mask_ref, mask_s)
    weight_send(0, wo_ref, wox_ref, wo_s)
    gate_load = load(gate_ref, gate_s)
    up_load = load(up_ref, up_s)
    cross_start(0)

    def turn(wide, tall):
        @pl.loop(0, d_model // CHUNK)
        def _(i):
            at = pl.ds(pl.multiple_of(i * CHUNK, CHUNK), CHUNK)
            tall[at, :] = wide[:, at].T

    def project_heads(buf, weight, c, add_to):
        lhs = jnp.concatenate([buf[i, CHUNK * c:CHUNK * (c + 1), :] for i in range(4)], axis=1)
        for n in range(0, d_model, 512):
            res_s[CHUNK * c:CHUNK * (c + 1), n:n + 512] = add_to[CHUNK * c:CHUNK * (c + 1), n:n + 512].astype(F32) + dot(lhs, weight[:, n:n + 512])

    def cross_query(c):
        if c == 0:
            own_mixed.wait()
            x_load.wait()
            for copy in own_wo:
                copy.wait()
        gather_wait(0, mix_s, c)
        if c == 0:
            weight_wait(0, wo_s)
            q_load.wait()
        project_heads(mix_s, wo_s, c, x_s)
        normed = rms_norm(res_s[CHUNK * c:CHUNK * (c + 1), :], norm_c_ref[...])
        qt_s[...] = dot(normed, cq_s[...]).astype(BF16).astype(F32).T

    sub = iota((8, CHUNK), 0)
    masks = [lax.rem(sub, 2 * w) < w for w in (4, 2, 1)]

    def turned(x, w):
        return jnp.concatenate([x[w:], x[:w]], axis=0)

    def fold(parts):
        for w, mask in zip((4, 2, 1), masks):
            folded = []
            for j in range(w):
                a, b = parts[j], parts[j + w]
                keep = jnp.where(mask, a, b)
                give = jnp.where(mask, turned(a, w), turned(b, 8 - w))
                folded.append(keep + give)
            parts = folded
        return parts[0]

    def cross_score(c):
        slot = c % n_cross_slots
        for copy in cross_load(c):
            copy.wait()
        if c == 0:
            mask_load.wait()
        step = 8

        @pl.loop(0, src_len // step)
        def _(i):
            at = pl.ds(pl.multiple_of(i * step, step), step)
            for h in range(heads):
                d = slice(head_dim * h, head_dim * (h + 1))
                parts = []
                for j in range(step):
                    prod = k_s[slot, i * step + j, d, :].astype(F32) * qt_s[d, :]
                    parts.append(jnp.sum(prod.reshape(head_dim // 8, 8, CHUNK), axis=0))
                score_s[h, at, :] = fold(parts)

    def cross_mix(c):
        slot = c % n_cross_slots
        step = 8
        valid = mask_s[:, CHUNK * c:CHUNK * (c + 1)] != 0
        for h in range(heads):
            scores = jnp.where(valid, score_s[h], NEG_FILL)
            exps = jnp.exp(scores - jnp.max(scores, axis=0, keepdims=True))
            probs = exps * pl.reciprocal(jnp.sum(exps, axis=0, keepdims=True))
            score_s[h] = probs.astype(BF16).astype(F32)

        def mix(i, acc):
            acc = list(acc)
            for j in range(step):
                s = i * step + j
                for h in range(heads):
                    d = slice(head_dim * h, head_dim * (h + 1))
                    acc[h] = acc[h] + v_s[slot, s, d, :].astype(F32) * score_s[h, pl.ds(s, 1), :]
            return tuple(acc)

        zero = jnp.zeros((head_dim, CHUNK), F32)
        acc = lax.fori_loop(0, src_len // step, mix, (zero,) * heads)
        cmix_s[me, CHUNK * c:CHUNK * (c + 1), :] = jnp.concatenate(acc, axis=0).T.astype(BF16)
        gather_send(1, block(cmix_s, me, c), cmix_s, c)

    def mlp(c):
        if c == 0:
            for copy in own_co:
                copy.wait()
            weight_wait(1, co_s)
        gather_wait(1, cmix_s, c)
        project_heads(cmix_s, co_s, c, res_s)
        if c == 0:
            up_load.wait()
            down_load.wait()
        normed = rms_norm(res_s[CHUNK * c:CHUNK * (c + 1), :], norm_m_ref[...])
        for n in range(0, d_ff, 256):
            end = min(d_ff, n + 256)
            gate = dot(normed, gate_t[:, n:end])
            up = dot_nt(normed, up_s[n:end, :])
            hid_s[:, n:end] = (jax.nn.gelu(gate, approximate=True) * up).astype(BF16)
        hidden = hid_s[...]
        for n in range(0, d_model, 512):
            part_s[c, :, n:n + 512] = dot(hidden, down_s[:, n:n + 512]).astype(BF16)
        give = pl.ds(pl.multiple_of((1 - core) * half, half), half)
        send(remote(part_s.at[c, give, :], near_s.at[c], sum_send.at[0, c], sum_recv.at[0, c], mate))

    pieces = [(c, 0, half) for c in range(chunks - 1)] + [(chunks - 1, 0, half // 2), (chunks - 1, half // 2, half // 2)]

    def chip_sum(p):
        c, at, size = pieces[p]
        if at == 0:
            remote(near_s.at[c], near_s.at[c], sum_send.at[0, c], sum_recv.at[0, c], mate).wait_recv()
        keep = pl.ds(pl.multiple_of(core * half + at, size), size)
        piece = pl.ds(at, size)
        chip_s[c, piece, :] = (part_s[c, keep, :].astype(F32) + near_s[c, piece, :].astype(F32)).astype(BF16)
        send(remote(chip_s.at[c, piece, :], far_s.at[c, piece, :], sum_send.at[1, p], sum_recv.at[1, p], over))

    def full_sum(p):
        c, at, size = pieces[p]
        piece = pl.ds(at, size)
        remote(far_s.at[c, piece, :], far_s.at[c, piece, :], sum_send.at[1, p], sum_recv.at[1, p], over).wait_recv()
        mine = pl.ds(pl.multiple_of(CHUNK * c + core * half + at, size), size)
        done_s[mine, :] = (res_s[mine, :] + (chip_s[c, piece, :].astype(F32) + far_s[c, piece, :].astype(F32))).astype(BF16)
        send(remote(done_s.at[mine, :], done_s.at[mine, :], sum_send.at[2, p], sum_recv.at[2, p], mate))
        copy = pltpu.make_async_copy(done_s.at[mine, :], out_ref.at[mine, :], out_sem.at[0, p])
        copy.start()
        stores.append(copy)

    def store(p):
        c, at, size = pieces[p]
        other = pl.ds(pl.multiple_of(CHUNK * c + (1 - core) * half + at, size), size)
        remote(done_s.at[other, :], done_s.at[other, :], sum_send.at[2, p], sum_recv.at[2, p], mate).wait_recv()
        copy = pltpu.make_async_copy(done_s.at[other, :], out_ref.at[other, :], out_sem.at[1, p])
        copy.start()
        stores.append(copy)

    stores = []
    gate_load.wait()
    turn(gate_s, gate_t)
    gather_relay(0, mix_s, 0)
    cross_query(0)
    for c in range(1, chunks):
        gather_relay(0, mix_s, c)
    cross_start(1)
    cross_score(0)
    cross_mix(0)
    weight_send(1, co_ref, cox_ref, co_s)
    own_co = (load(co_ref, shard(co_s, me)), load(cox_ref, shard(co_s, over)))
    cross_start(2)
    cross_query(1)
    cross_score(1)
    cross_mix(1)
    down_load = load(down_ref, down_s)
    cross_start(3)
    cross_query(2)
    gather_relay(1, cmix_s, 0)
    cross_score(2)
    mlp(0)
    gather_relay(1, cmix_s, 1)
    cross_mix(2)
    chip_sum(0)
    cross_query(3)
    cross_score(3)
    cross_mix(3)
    mlp(1)
    gather_relay(1, cmix_s, 2)
    chip_sum(1)
    mlp(2)
    gather_relay(1, cmix_s, 3)
    full_sum(0)
    chip_sum(2)
    mlp(3)
    store(0)
    full_sum(1)
    chip_sum(3)
    chip_sum(4)
    store(1)
    full_sum(2)
    store(2)
    full_sum(3)
    store(3)
    full_sum(4)
    store(4)
    for copy in stores:
        copy.wait()
    for copy in sends:
        copy.wait_send()


def rest_of_layer(x_in, mixed, w_o, w_o_over, cross_o, cross_o_over, cross_q, gate_t, up_t, w_down, norm_cross, norm_mlp, mask_t, cross_k, cross_v, heads):
    rows, d_model = x_in.shape
    flat = mixed.shape[1]
    d_ff = gate_t.shape[0]
    src_len = cross_k.shape[0]
    chunks = rows // CHUNK
    slots = 2
    anywhere = pl.BlockSpec(memory_space=pl.ANY)
    vmem = pl.BlockSpec(memory_space=pltpu.VMEM)
    dma = pltpu.SemaphoreType.DMA
    return pl.pallas_call(
        functools.partial(rest_kernel, heads, slots),
        in_specs=[anywhere] * 10 + [vmem, vmem] + [anywhere] * 3,
        out_specs=anywhere,
        out_shape=jax.ShapeDtypeStruct((rows, d_model), BF16),
        scratch_shapes=[
            pltpu.VMEM((rows, d_model), BF16),
            pltpu.VMEM((rows, d_model), F32),
            pltpu.VMEM((4, rows, flat), BF16),
            pltpu.VMEM((4, rows, flat), BF16),
            pltpu.VMEM((4 * flat, d_model), BF16),
            pltpu.VMEM((4 * flat, d_model), BF16),
            pltpu.VMEM((d_model, flat), BF16),
            pltpu.VMEM((d_ff, d_model), BF16),
            pltpu.VMEM((d_ff, d_model), BF16),
            pltpu.VMEM((d_model, d_ff), BF16),
            pltpu.VMEM((d_ff, d_model), BF16),
            pltpu.VMEM((slots, src_len, flat, CHUNK), BF16),
            pltpu.VMEM((slots, src_len, flat, CHUNK), BF16),
            pltpu.VMEM((src_len, rows), jnp.int32),
            pltpu.VMEM((flat, CHUNK), F32),
            pltpu.VMEM((heads, src_len, CHUNK), F32),
            pltpu.VMEM((CHUNK, d_ff), BF16),
            pltpu.VMEM((chunks, CHUNK, d_model), BF16),
            pltpu.VMEM((chunks, CHUNK // 2, d_model), BF16),
            pltpu.VMEM((chunks, CHUNK // 2, d_model), BF16),
            pltpu.VMEM((chunks, CHUNK // 2, d_model), BF16),
            pltpu.VMEM((rows, d_model), BF16),
            dma((2, 3, chunks)), dma((2, 3, chunks)),
            dma((2, 2)), dma((2, 2)),
            dma((3, chunks + 1)), dma((3, chunks + 1)),
            dma((16,)), dma((2, slots)), dma((2, chunks + 1)),
        ],
        compiler_params=pltpu.CompilerParams(collective_id=0, has_side_effects=True, vmem_limit_bytes=VMEM_BYTES),
        cost_estimate=pl.CostEstimate(flops=2 * rows * d_model * (8 * flat + flat + 3 * d_ff), bytes_accessed=50_000_000, transcendentals=rows * d_ff),
        name='rest_of_layer',
    )(x_in, mixed, w_o, w_o_over, cross_o, cross_o_over, cross_q, gate_t, up_t, w_down, norm_cross, norm_mlp, mask_t, cross_k, cross_v)


def solution(mesh):
    def local_layer(x_in, tok_pos, self_k, self_v, cross_k, cross_v, enc_mask, rel_bias, w_q, w_k, w_v, w_o, cross_q, cross_o, w_gate, w_up, w_down, norm_self, norm_cross, norm_mlp):
        rows, t_len, heads, head_dim = self_k.shape
        flat = heads * head_dim
        to_kernel = lambda c: jnp.transpose(c, (0, 2, 3, 1)).reshape(rows, flat, t_len)
        from_kernel = lambda c: jnp.transpose(c.reshape(rows, heads, head_dim, t_len), (0, 3, 1, 2))
        cross_view = lambda c: jnp.transpose(c, (1, 2, 3, 0)).reshape(c.shape[1], flat, rows)
        swap = [(0, 2), (1, 3), (2, 0), (3, 1)]
        w_o_over = lax.ppermute(w_o, 'tp', swap)
        cross_o_over = lax.ppermute(cross_o, 'tp', swap)
        mixed_self, new_k, new_v = self_attention(tok_pos, rel_bias.T, x_in, w_q, w_k, w_v, norm_self, to_kernel(self_k), to_kernel(self_v), heads)
        x_out = rest_of_layer(x_in, mixed_self, w_o, w_o_over, cross_o, cross_o_over, cross_q, w_gate.T, w_up.T, w_down, norm_cross, norm_mlp,
                              enc_mask.T, cross_view(cross_k), cross_view(cross_v), heads)
        return x_out, from_kernel(new_k), from_kernel(new_v)

    cache_spec = P('dp', None, 'tp', None)
    split_cols = P(None, 'tp')
    split_rows = P('tp', None)
    in_specs = (P('dp', None), P('dp'), cache_spec, cache_spec, cache_spec, cache_spec, P('dp', None), split_cols, split_cols, split_cols, split_cols, split_rows, split_cols, split_rows, split_cols, split_cols, split_rows, P(None), P(None), P(None))
    out_specs = (P('dp', None), cache_spec, cache_spec)
    return jax.shard_map(local_layer, mesh=mesh, in_specs=in_specs, out_specs=out_specs, check_vma=False)
```

```python
import functools
import math
import jax
import jax.numpy as jnp
from jax import lax
from jax.experimental import pallas as pl
from jax.experimental.pallas import tpu as pltpu
from jax.sharding import PartitionSpec as P

BUCKET_EDGES = tuple(int(math.ceil(16.0 * 8.0 ** (bucket_step / 16.0))) for bucket_step in range(1, 16))
NEG_FILL = -1e30
STEP_ROWS = 32
SLOTS = 11
AHEAD = 6
VMEM_BYTES = 67043328
LANES = 128
F32 = jnp.float32
BF16 = jnp.bfloat16


def rms_norm(values, norm_scale):
    inv_rms = lax.rsqrt(jnp.mean(values * values, axis=-1, keepdims=True) + 1e-6)
    return (values * inv_rms * norm_scale.astype(F32)).astype(BF16)


def dot(a, b):
    return jnp.dot(a, b, preferred_element_type=F32)


def dot_nt(a, b):
    return lax.dot_general(a, b, (((1,), (1,)), ((), ())), preferred_element_type=F32)


def iota(shape, axis):
    return lax.broadcasted_iota(jnp.int32, shape, axis)


def self_kernel(heads, head_dim, pos_ref, bias_ref, x_ref, wq_ref, wk_ref, wv_ref, norm_ref, k_ref, v_ref,
                mixed_ref, ko_ref, vo_ref, x_s, wq_s, wk_s, wv_s, k_s, v_s, mixed_s, q_s, kt_s, vt_s, score_s, out_s,
                load_sem, in_sem, out_sem, mixed_sem):
    flat = heads * head_dim
    rows_total = x_ref.shape[0]
    n = STEP_ROWS
    steps = rows_total // n

    def rows_of(step):
        return pl.ds(pl.multiple_of(step * n, n), n)

    def fetch(step):
        slot = lax.rem(step, SLOTS)
        return (pltpu.make_async_copy(k_ref.at[rows_of(step)], k_s.at[slot], in_sem.at[0, slot]),
                pltpu.make_async_copy(v_ref.at[rows_of(step)], v_s.at[slot], in_sem.at[1, slot]))

    def write(step):
        slot = lax.rem(step, SLOTS)
        return (pltpu.make_async_copy(k_s.at[slot], ko_ref.at[rows_of(step)], out_sem.at[0, slot]),
                pltpu.make_async_copy(v_s.at[slot], vo_ref.at[rows_of(step)], out_sem.at[1, slot]))

    loads = [pltpu.make_async_copy(src, dst, load_sem.at[i])
             for i, (src, dst) in enumerate(((x_ref, x_s), (wq_ref, wq_s), (wk_ref, wk_s), (wv_ref, wv_s)))]
    for copy in loads:
        copy.start()
    for step in range(AHEAD):
        for copy in fetch(step):
            copy.start()

    lane = iota((4 * heads, LANES), 1)
    head_of = lax.rem(iota((4 * heads, LANES), 0), heads)
    far = jnp.full_like(lane, 16)
    for edge in BUCKET_EDGES:
        far = far + jnp.where(lane >= edge, 1, 0)
    bucket = jnp.where(lane < 16, lane, far)
    table = jnp.zeros((4 * heads, LANES), F32)
    for b in range(32):
        here = jnp.zeros((4 * heads, LANES), F32)
        for h in range(heads):
            here = jnp.where(head_of == h, bias_ref[h, b], here)
        table = jnp.where(bucket == b, here, table)

    for copy in loads:
        copy.wait()

    @pl.loop(0, rows_total // LANES)
    def _(g):
        rows = pl.ds(pl.multiple_of(g * LANES, LANES), LANES)
        normed = rms_norm(x_s[rows, :].astype(F32), norm_ref[...])
        q_s[rows, :] = dot(normed, wq_s[...]).astype(BF16)
        kt_s[g] = dot(normed, wk_s[...]).astype(BF16).astype(F32).T
        vt_s[g] = dot(normed, wv_s[...]).astype(BF16).astype(F32).T

    spread = jnp.where(iota((n * heads, n), 0) // heads == iota((n * heads, n), 1), 1.0, 0.0).astype(BF16)
    gather = jnp.where(iota((n, n * heads), 1) // heads == iota((n, n * heads), 0), 1.0, 0.0).astype(BF16)
    own_head = iota((n * heads, flat), 1) // head_dim == lax.rem(iota((n * heads, flat), 0), heads)
    lane_bf = iota((flat, LANES), 1).astype(F32).astype(BF16)
    quad_row = iota((4 * heads, LANES), 0)
    per = LANES // n

    @pl.loop(0, steps)
    def _(step):
        ahead = step + AHEAD

        @pl.when(ahead < steps)
        def _():
            @pl.when(ahead >= SLOTS)
            def _():
                for copy in write(ahead - SLOTS):
                    copy.wait()
            for copy in fetch(ahead):
                copy.start()

        first = pl.multiple_of(step * n, n)
        slot = lax.rem(step, SLOTS)
        group, part = step // per, lax.rem(step, per)
        shift = lax.rem(LANES - part * n, LANES)
        k_new = pltpu.roll(kt_s[group], shift, 1).astype(BF16)
        v_new = pltpu.roll(vt_s[group], shift, 1).astype(BF16)
        q_rows = jnp.where(own_head, dot(spread, q_s[pl.ds(first, n), :]), 0.0).astype(BF16)
        in_k, in_v = fetch(step)

        def update(cache, new_cols, b):
            at_pos = lane_bf == pos_ref[first + b].astype(F32).astype(BF16)
            col = jnp.broadcast_to(new_cols[:, b:b + 1], (flat, LANES))
            updated = jnp.where(at_pos, col, cache[slot, b])
            cache[slot, b] = updated
            return updated

        in_k.wait()
        for g in range(n // 4):
            lhs = q_rows[4 * heads * g:4 * heads * (g + 1), :]
            picked = None
            distance = None
            for half in range(2):
                b = 4 * g + 2 * half
                pair = jnp.concatenate([update(k_s, k_new, b), update(k_s, k_new, b + 1)], axis=1)
                both = dot(lhs, pair)
                for j in range(2):
                    mine = both[:, LANES * j:LANES * (j + 1)]
                    at = 2 * half + j
                    pos = pos_ref[first + 4 * g + at]
                    picked = mine if picked is None else jnp.where(quad_row >= heads * at, mine, picked)
                    distance = jnp.full((4 * heads, LANES), pos, jnp.int32) if distance is None else jnp.where(quad_row >= heads * at, pos, distance)
            distance = distance - iota((4 * heads, LANES), 1)
            bias = jnp.take_along_axis(table, jnp.maximum(distance, 0), axis=1)
            score_s[4 * heads * g:4 * heads * (g + 1), :] = jnp.where(distance >= 0, picked + bias, NEG_FILL)
        write(step)[0].start()

        scores = score_s[...]
        exps = jnp.exp(scores - jnp.max(scores, axis=1, keepdims=True))
        probs = exps * pl.reciprocal(jnp.sum(exps, axis=1, keepdims=True))

        in_v.wait()
        for g in range(n // 4):
            quad = probs[4 * heads * g:4 * heads * (g + 1), :]
            picked = None
            for half in range(2):
                b = 4 * g + 2 * half
                pair = jnp.concatenate([update(v_s, v_new, b), update(v_s, v_new, b + 1)], axis=1)
                low = jnp.where(quad_row // heads == 2 * half, quad, 0.0)
                high = jnp.where(quad_row // heads == 2 * half + 1, quad, 0.0)
                lhs = jnp.concatenate([low, high], axis=1).astype(BF16)
                both = dot_nt(lhs, pair)
                picked = both if half == 0 else jnp.where(iota(both.shape, 0) >= 2 * heads, both, picked)
            out_s[4 * heads * g:4 * heads * (g + 1), :] = picked
        write(step)[1].start()
        mixed_s[pl.ds(first, n), :] = dot(gather, jnp.where(own_head, out_s[...], 0.0).astype(BF16)).astype(BF16)

    mixed_copy = pltpu.make_async_copy(mixed_s, mixed_ref, mixed_sem)
    mixed_copy.start()
    for step in range(steps - SLOTS, steps):
        for copy in write(step):
            copy.wait()
    mixed_copy.wait()


def self_attention(tok_pos, bias_t, x_in, w_q, w_k, w_v, norm_self, keys, values, heads):
    rows, flat, t_len = keys.shape
    d_model = x_in.shape[1]
    n = STEP_ROWS
    smem = pl.BlockSpec(memory_space=pltpu.SMEM)
    anywhere = pl.BlockSpec(memory_space=pl.ANY)
    cache_shape = jax.ShapeDtypeStruct(keys.shape, BF16)
    return pl.pallas_call(
        functools.partial(self_kernel, heads, flat // heads),
        in_specs=[smem, smem] + [anywhere] * 4 + [pl.BlockSpec(memory_space=pltpu.VMEM)] + [anywhere] * 2,
        out_specs=[anywhere] * 3,
        out_shape=[jax.ShapeDtypeStruct((rows, flat), BF16), cache_shape, cache_shape],
        scratch_shapes=[
            pltpu.VMEM((rows, d_model), BF16),
            pltpu.VMEM((d_model, flat), BF16),
            pltpu.VMEM((d_model, flat), BF16),
            pltpu.VMEM((d_model, flat), BF16),
            pltpu.VMEM((SLOTS, n, flat, t_len), BF16),
            pltpu.VMEM((SLOTS, n, flat, t_len), BF16),
            pltpu.VMEM((rows, flat), BF16),
            pltpu.VMEM((rows, flat), BF16),
            pltpu.VMEM((rows // LANES, flat, LANES), F32),
            pltpu.VMEM((rows // LANES, flat, LANES), F32),
            pltpu.VMEM((n * heads, LANES), F32),
            pltpu.VMEM((n * heads, flat), F32),
            pltpu.SemaphoreType.DMA((4,)),
            pltpu.SemaphoreType.DMA((2, SLOTS)),
            pltpu.SemaphoreType.DMA((2, SLOTS)),
            pltpu.SemaphoreType.DMA,
        ],
        compiler_params=pltpu.CompilerParams(vmem_limit_bytes=VMEM_BYTES),
        cost_estimate=pl.CostEstimate(flops=4 * rows * flat * t_len * 16 + 6 * rows * d_model * flat, bytes_accessed=8 * rows * flat * t_len, transcendentals=rows * heads * t_len),
        name='self_attention',
    )(tok_pos, bias_t, x_in, w_q, w_k, w_v, norm_self, keys, values)


CHUNK = 128
MESH = pl.DeviceIdType.MESH


def rest_kernel(heads, n_cross_slots,
                x_ref, mixed_ref, wo_ref, wox_ref, co_ref, cox_ref, cq_ref, gate_ref, up_ref, down_ref, norm_c_ref, norm_m_ref,
                mask_ref, ck_ref, cv_ref, out_ref,
                x_s, res_s, mix_s, cmix_s, wo_s, co_s, cq_s, gate_s, up_s, gate_t, down_s, k_s, v_s, mask_s,
                qt_s, score_s, hid_s, part_s, near_s, chip_s, far_s, done_s,
                ag_send, ag_recv, w_send, w_recv, sum_send, sum_recv, load_sem, cross_sem, out_sem):
    me = lax.axis_index('tp')
    core = lax.rem(me, 2)
    mate = me + 1 - 2 * core
    over = lax.rem(me + 2, 4)
    cater = lax.rem(mate + 2, 4)
    rows_total, d_model = x_ref.shape
    flat = mixed_ref.shape[1]
    head_dim = flat // heads
    src_len = ck_ref.shape[0]
    d_ff = gate_ref.shape[0]
    chunks = rows_total // CHUNK
    half = CHUNK // 2

    def remote(src, dst, send_sem, recv_sem, to):
        return pltpu.make_async_remote_copy(src_ref=src, dst_ref=dst, send_sem=send_sem, recv_sem=recv_sem,
                                            device_id={'tp': to}, device_id_type=MESH)

    def block(buf, who, c):
        return buf.at[who, pl.ds(CHUNK * c, CHUNK), :]

    def shard(buf, who):
        return buf.at[pl.ds(pl.multiple_of(who * flat, flat), flat), :]

    loads = []

    def load(src, dst):
        copy = pltpu.make_async_copy(src, dst, load_sem.at[len(loads)])
        copy.start()
        loads.append(copy)
        return copy

    def cross_load(c):
        slot = c % n_cross_slots
        cols = pl.ds(CHUNK * c, CHUNK)
        return (pltpu.make_async_copy(ck_ref.at[:, :, cols], k_s.at[slot], cross_sem.at[0, slot]),
                pltpu.make_async_copy(cv_ref.at[:, :, cols], v_s.at[slot], cross_sem.at[1, slot]))

    def cross_start(c):
        for copy in cross_load(c):
            copy.start()

    barrier = pltpu.get_barrier_semaphore()
    for peer in (mate, over):
        pl.semaphore_signal(barrier, inc=1, device_id={'tp': peer}, device_id_type=MESH)
    pl.semaphore_wait(barrier, 2)

    sends = []

    def send(copy):
        copy.start()
        sends.append(copy)

    def gather_send(stage, src, buf, c):
        send(remote(src, block(buf, me, c), ag_send.at[stage, 0, c], ag_recv.at[stage, 0, c], over))
        send(remote(src, block(buf, me, c), ag_send.at[stage, 1, c], ag_recv.at[stage, 1, c], mate))

    def gather_relay(stage, buf, c):
        remote(block(buf, over, c), block(buf, over, c), ag_send.at[stage, 0, c], ag_recv.at[stage, 0, c], over).wait_recv()
        send(remote(block(buf, over, c), block(buf, over, c), ag_send.at[stage, 2, c], ag_recv.at[stage, 2, c], mate))

    def gather_wait(stage, buf, c):
        remote(block(buf, mate, c), block(buf, mate, c), ag_send.at[stage, 1, c], ag_recv.at[stage, 1, c], mate).wait_recv()
        remote(block(buf, cater, c), block(buf, cater, c), ag_send.at[stage, 2, c], ag_recv.at[stage, 2, c], mate).wait_recv()

    def weight_send(which, ref, ref_x, buf):
        send(remote(ref, shard(buf, me), w_send.at[which, 0], w_recv.at[which, 0], mate))
        send(remote(ref_x, shard(buf, over), w_send.at[which, 1], w_recv.at[which, 1], mate))

    def weight_wait(which, buf):
        remote(shard(buf, mate), shard(buf, mate), w_send.at[which, 0], w_recv.at[which, 0], mate).wait_recv()
        remote(shard(buf, cater), shard(buf, cater), w_send.at[which, 1], w_recv.at[which, 1], mate).wait_recv()

    for c in range(chunks):
        gather_send(0, mixed_ref.at[pl.ds(CHUNK * c, CHUNK), :], mix_s, c)
    own_mixed = load(mixed_ref, mix_s.at[me])
    own_wo = (load(wo_ref, shard(wo_s, me)), load(wox_ref, shard(wo_s, over)))
    x_load = load(x_ref, x_s)
    q_load = load(cq_ref, cq_s)
    mask_load = load(mask_ref, mask_s)
    weight_send(0, wo_ref, wox_ref, wo_s)
    gate_load = load(gate_ref, gate_s)
    up_load = load(up_ref, up_s)
    cross_start(0)

    def turn(wide, tall):
        @pl.loop(0, d_model // CHUNK)
        def _(i):
            at = pl.ds(pl.multiple_of(i * CHUNK, CHUNK), CHUNK)
            tall[at, :] = wide[:, at].T

    def project_heads(buf, weight, c, add_to):
        lhs = jnp.concatenate([buf[i, CHUNK * c:CHUNK * (c + 1), :] for i in range(4)], axis=1)
        for n in range(0, d_model, 512):
            res_s[CHUNK * c:CHUNK * (c + 1), n:n + 512] = add_to[CHUNK * c:CHUNK * (c + 1), n:n + 512].astype(F32) + dot(lhs, weight[:, n:n + 512])

    def cross_query(c):
        if c == 0:
            own_mixed.wait()
            x_load.wait()
            for copy in own_wo:
                copy.wait()
        gather_wait(0, mix_s, c)
        if c == 0:
            weight_wait(0, wo_s)
            q_load.wait()
        project_heads(mix_s, wo_s, c, x_s)
        normed = rms_norm(res_s[CHUNK * c:CHUNK * (c + 1), :], norm_c_ref[...])
        qt_s[...] = dot(normed, cq_s[...]).astype(BF16).astype(F32).T

    sub = iota((8, CHUNK), 0)
    masks = [lax.rem(sub, 2 * w) < w for w in (4, 2, 1)]

    def turned(x, w):
        return jnp.concatenate([x[w:], x[:w]], axis=0)

    def fold(parts):
        for w, mask in zip((4, 2, 1), masks):
            folded = []
            for j in range(w):
                a, b = parts[j], parts[j + w]
                keep = jnp.where(mask, a, b)
                give = jnp.where(mask, turned(a, w), turned(b, 8 - w))
                folded.append(keep + give)
            parts = folded
        return parts[0]

    def cross_score(c):
        slot = c % n_cross_slots
        for copy in cross_load(c):
            copy.wait()
        if c == 0:
            mask_load.wait()
        step = 8

        @pl.loop(0, src_len // step)
        def _(i):
            at = pl.ds(pl.multiple_of(i * step, step), step)
            for h in range(heads):
                d = slice(head_dim * h, head_dim * (h + 1))
                parts = []
                for j in range(step):
                    prod = k_s[slot, i * step + j, d, :].astype(F32) * qt_s[d, :]
                    parts.append(jnp.sum(prod.reshape(head_dim // 8, 8, CHUNK), axis=0))
                score_s[h, at, :] = fold(parts)

    def cross_mix(c):
        slot = c % n_cross_slots
        step = 8
        valid = mask_s[:, CHUNK * c:CHUNK * (c + 1)] != 0
        for h in range(heads):
            scores = jnp.where(valid, score_s[h], NEG_FILL)
            exps = jnp.exp(scores - jnp.max(scores, axis=0, keepdims=True))
            probs = exps * pl.reciprocal(jnp.sum(exps, axis=0, keepdims=True))
            score_s[h] = probs.astype(BF16).astype(F32)

        def mix(i, acc):
            acc = list(acc)
            for j in range(step):
                s = i * step + j
                for h in range(heads):
                    d = slice(head_dim * h, head_dim * (h + 1))
                    acc[h] = acc[h] + v_s[slot, s, d, :].astype(F32) * score_s[h, pl.ds(s, 1), :]
            return tuple(acc)

        zero = jnp.zeros((head_dim, CHUNK), F32)
        acc = lax.fori_loop(0, src_len // step, mix, (zero,) * heads)
        cmix_s[me, CHUNK * c:CHUNK * (c + 1), :] = jnp.concatenate(acc, axis=0).T.astype(BF16)
        gather_send(1, block(cmix_s, me, c), cmix_s, c)

    def mlp(c):
        if c == 0:
            for copy in own_co:
                copy.wait()
            weight_wait(1, co_s)
        gather_wait(1, cmix_s, c)
        project_heads(cmix_s, co_s, c, res_s)
        if c == 0:
            up_load.wait()
            down_load.wait()
        normed = rms_norm(res_s[CHUNK * c:CHUNK * (c + 1), :], norm_m_ref[...])
        for n in range(0, d_ff, 256):
            end = min(d_ff, n + 256)
            gate = dot(normed, gate_t[:, n:end])
            up = dot_nt(normed, up_s[n:end, :])
            hid_s[:, n:end] = (jax.nn.gelu(gate, approximate=True) * up).astype(BF16)
        hidden = hid_s[...]
        for n in range(0, d_model, 512):
            part_s[c, :, n:n + 512] = dot(hidden, down_s[:, n:n + 512]).astype(BF16)
        give = pl.ds(pl.multiple_of((1 - core) * half, half), half)
        send(remote(part_s.at[c, give, :], near_s.at[c], sum_send.at[0, c], sum_recv.at[0, c], mate))

    pieces = [(c, 0, half) for c in range(chunks - 1)] + [(chunks - 1, 0, half // 2), (chunks - 1, half // 2, half // 2)]

    def chip_sum(p):
        c, at, size = pieces[p]
        if at == 0:
            remote(near_s.at[c], near_s.at[c], sum_send.at[0, c], sum_recv.at[0, c], mate).wait_recv()
        keep = pl.ds(pl.multiple_of(core * half + at, size), size)
        piece = pl.ds(at, size)
        chip_s[c, piece, :] = (part_s[c, keep, :].astype(F32) + near_s[c, piece, :].astype(F32)).astype(BF16)
        send(remote(chip_s.at[c, piece, :], far_s.at[c, piece, :], sum_send.at[1, p], sum_recv.at[1, p], over))

    def full_sum(p):
        c, at, size = pieces[p]
        piece = pl.ds(at, size)
        remote(far_s.at[c, piece, :], far_s.at[c, piece, :], sum_send.at[1, p], sum_recv.at[1, p], over).wait_recv()
        mine = pl.ds(pl.multiple_of(CHUNK * c + core * half + at, size), size)
        done_s[mine, :] = (res_s[mine, :] + (chip_s[c, piece, :].astype(F32) + far_s[c, piece, :].astype(F32))).astype(BF16)
        send(remote(done_s.at[mine, :], done_s.at[mine, :], sum_send.at[2, p], sum_recv.at[2, p], mate))
        copy = pltpu.make_async_copy(done_s.at[mine, :], out_ref.at[mine, :], out_sem.at[0, p])
        copy.start()
        stores.append(copy)

    def store(p):
        c, at, size = pieces[p]
        other = pl.ds(pl.multiple_of(CHUNK * c + (1 - core) * half + at, size), size)
        remote(done_s.at[other, :], done_s.at[other, :], sum_send.at[2, p], sum_recv.at[2, p], mate).wait_recv()
        copy = pltpu.make_async_copy(done_s.at[other, :], out_ref.at[other, :], out_sem.at[1, p])
        copy.start()
        stores.append(copy)

    stores = []
    gate_load.wait()
    turn(gate_s, gate_t)
    gather_relay(0, mix_s, 0)
    cross_query(0)
    for c in range(1, chunks):
        gather_relay(0, mix_s, c)
    cross_start(1)
    cross_score(0)
    cross_mix(0)
    weight_send(1, co_ref, cox_ref, co_s)
    own_co = (load(co_ref, shard(co_s, me)), load(cox_ref, shard(co_s, over)))
    cross_start(2)
    cross_query(1)
    cross_score(1)
    cross_mix(1)
    down_load = load(down_ref, down_s)
    cross_start(3)
    cross_query(2)
    gather_relay(1, cmix_s, 0)
    cross_score(2)
    mlp(0)
    gather_relay(1, cmix_s, 1)
    cross_mix(2)
    chip_sum(0)
    cross_query(3)
    cross_score(3)
    cross_mix(3)
    mlp(1)
    gather_relay(1, cmix_s, 2)
    chip_sum(1)
    mlp(2)
    gather_relay(1, cmix_s, 3)
    full_sum(0)
    chip_sum(2)
    mlp(3)
    store(0)
    full_sum(1)
    chip_sum(3)
    chip_sum(4)
    store(1)
    full_sum(2)
    store(2)
    full_sum(3)
    store(3)
    full_sum(4)
    store(4)
    for copy in stores:
        copy.wait()
    for copy in sends:
        copy.wait_send()


def rest_of_layer(x_in, mixed, w_o, w_o_over, cross_o, cross_o_over, cross_q, gate_t, up_t, w_down, norm_cross, norm_mlp, mask_t, cross_k, cross_v, heads):
    rows, d_model = x_in.shape
    flat = mixed.shape[1]
    d_ff = gate_t.shape[0]
    src_len = cross_k.shape[0]
    chunks = rows // CHUNK
    slots = 2
    anywhere = pl.BlockSpec(memory_space=pl.ANY)
    vmem = pl.BlockSpec(memory_space=pltpu.VMEM)
    dma = pltpu.SemaphoreType.DMA
    return pl.pallas_call(
        functools.partial(rest_kernel, heads, slots),
        in_specs=[anywhere] * 10 + [vmem, vmem] + [anywhere] * 3,
        out_specs=anywhere,
        out_shape=jax.ShapeDtypeStruct((rows, d_model), BF16),
        scratch_shapes=[
            pltpu.VMEM((rows, d_model), BF16),
            pltpu.VMEM((rows, d_model), F32),
            pltpu.VMEM((4, rows, flat), BF16),
            pltpu.VMEM((4, rows, flat), BF16),
            pltpu.VMEM((4 * flat, d_model), BF16),
            pltpu.VMEM((4 * flat, d_model), BF16),
            pltpu.VMEM((d_model, flat), BF16),
            pltpu.VMEM((d_ff, d_model), BF16),
            pltpu.VMEM((d_ff, d_model), BF16),
            pltpu.VMEM((d_model, d_ff), BF16),
            pltpu.VMEM((d_ff, d_model), BF16),
            pltpu.VMEM((slots, src_len, flat, CHUNK), BF16),
            pltpu.VMEM((slots, src_len, flat, CHUNK), BF16),
            pltpu.VMEM((src_len, rows), jnp.int32),
            pltpu.VMEM((flat, CHUNK), F32),
            pltpu.VMEM((heads, src_len, CHUNK), F32),
            pltpu.VMEM((CHUNK, d_ff), BF16),
            pltpu.VMEM((chunks, CHUNK, d_model), BF16),
            pltpu.VMEM((chunks, CHUNK // 2, d_model), BF16),
            pltpu.VMEM((chunks, CHUNK // 2, d_model), BF16),
            pltpu.VMEM((chunks, CHUNK // 2, d_model), BF16),
            pltpu.VMEM((rows, d_model), BF16),
            dma((2, 3, chunks)), dma((2, 3, chunks)),
            dma((2, 2)), dma((2, 2)),
            dma((3, chunks + 1)), dma((3, chunks + 1)),
            dma((16,)), dma((2, slots)), dma((2, chunks + 1)),
        ],
        compiler_params=pltpu.CompilerParams(collective_id=0, has_side_effects=True, vmem_limit_bytes=VMEM_BYTES),
        cost_estimate=pl.CostEstimate(flops=2 * rows * d_model * (8 * flat + flat + 3 * d_ff), bytes_accessed=50_000_000, transcendentals=rows * d_ff),
        name='rest_of_layer',
    )(x_in, mixed, w_o, w_o_over, cross_o, cross_o_over, cross_q, gate_t, up_t, w_down, norm_cross, norm_mlp, mask_t, cross_k, cross_v)


HAND_PIECES = 4


def hand_out(x_out):
    rows = x_out.shape[0] // HAND_PIECES

    def kernel(x_ref, out_ref, held, in_sem, out_sem):
        part = [pl.ds(rows * i, rows) for i in range(HAND_PIECES)]
        ins = [pltpu.make_async_copy(x_ref.at[p], held.at[p], in_sem.at[i]) for i, p in enumerate(part)]
        outs = [pltpu.make_async_copy(held.at[p], out_ref.at[p], out_sem.at[i]) for i, p in enumerate(part)]
        for copy in ins:
            copy.start()
        for arrived, copy in zip(ins, outs):
            arrived.wait()
            copy.start()
        for copy in outs:
            copy.wait()

    return pl.pallas_call(
        kernel,
        in_specs=[pl.BlockSpec(memory_space=pl.ANY)],
        out_specs=pl.BlockSpec(memory_space=pl.ANY),
        out_shape=jax.ShapeDtypeStruct(x_out.shape, x_out.dtype),
        scratch_shapes=[pltpu.VMEM(x_out.shape, x_out.dtype), pltpu.SemaphoreType.DMA((HAND_PIECES,)), pltpu.SemaphoreType.DMA((HAND_PIECES,))],
        compiler_params=pltpu.CompilerParams(vmem_limit_bytes=VMEM_BYTES),
        name='hand_out',
    )(x_out)


def solution(mesh):
    def local_layer(x_in, tok_pos, self_k, self_v, cross_k, cross_v, enc_mask, rel_bias, w_q, w_k, w_v, w_o, cross_q, cross_o, w_gate, w_up, w_down, norm_self, norm_cross, norm_mlp):
        rows, t_len, heads, head_dim = self_k.shape
        flat = heads * head_dim
        to_kernel = lambda c: jnp.transpose(c, (0, 2, 3, 1)).reshape(rows, flat, t_len)
        from_kernel = lambda c: jnp.transpose(c.reshape(rows, heads, head_dim, t_len), (0, 3, 1, 2))
        cross_view = lambda c: jnp.transpose(c, (1, 2, 3, 0)).reshape(c.shape[1], flat, rows)
        swap = [(0, 2), (1, 3), (2, 0), (3, 1)]
        w_o_over = lax.ppermute(w_o, 'tp', swap)
        cross_o_over = lax.ppermute(cross_o, 'tp', swap)
        mixed_self, new_k, new_v = self_attention(tok_pos, rel_bias.T, x_in, w_q, w_k, w_v, norm_self, to_kernel(self_k), to_kernel(self_v), heads)
        x_out = rest_of_layer(x_in, mixed_self, w_o, w_o_over, cross_o, cross_o_over, cross_q, w_gate.T, w_up.T, w_down, norm_cross, norm_mlp,
                              enc_mask.T, cross_view(cross_k), cross_view(cross_v), heads)
        return hand_out(x_out), from_kernel(new_k), from_kernel(new_v)

    cache_spec = P('dp', None, 'tp', None)
    split_cols = P(None, 'tp')
    split_rows = P('tp', None)
    in_specs = (P('dp', None), P('dp'), cache_spec, cache_spec, cache_spec, cache_spec, P('dp', None), split_cols, split_cols, split_cols, split_cols, split_rows, split_cols, split_rows, split_cols, split_cols, split_rows, P(None), P(None), P(None))
    out_specs = (P('dp', None), cache_spec, cache_spec)
    return jax.shard_map(local_layer, mesh=mesh, in_specs=in_specs, out_specs=out_specs, check_vma=False)
```

```python
import functools
import math
import jax
import jax.numpy as jnp
from jax import lax
from jax.experimental import pallas as pl
from jax.experimental.pallas import tpu as pltpu
from jax.sharding import PartitionSpec as P

BUCKET_EDGES = tuple(int(math.ceil(16.0 * 8.0 ** (bucket_step / 16.0))) for bucket_step in range(1, 16))
NEG_FILL = -1e30
STEP_ROWS = 32
SLOTS = 8
AHEAD = 2
VMEM_BYTES = 67043328
LANES = 128
F32 = jnp.float32
BF16 = jnp.bfloat16


def rms_norm(values, norm_scale):
    inv_rms = lax.rsqrt(jnp.mean(values * values, axis=-1, keepdims=True) + 1e-6)
    return (values * inv_rms * norm_scale.astype(F32)).astype(BF16)


def dot(a, b):
    return jnp.dot(a, b, preferred_element_type=F32)


def dot_nt(a, b):
    return lax.dot_general(a, b, (((1,), (1,)), ((), ())), preferred_element_type=F32)


def iota(shape, axis):
    return lax.broadcasted_iota(jnp.int32, shape, axis)


def self_kernel(heads, head_dim, pos_ref, bias_ref, x_ref, wq_ref, wk_ref, wv_ref, norm_ref, k_ref, v_ref,
                mixed_ref, ko_ref, vo_ref, x_s, wq_s, wk_s, wv_s, k_s, v_s, mixed_s, q_s, kt_s, vt_s, score_s, out_s,
                load_sem, in_sem, out_sem, mixed_sem):
    flat = heads * head_dim
    rows_total = x_ref.shape[0]
    n = STEP_ROWS
    steps = rows_total // n

    def rows_of(step):
        return pl.ds(pl.multiple_of(step * n, n), n)

    def fetch(step):
        slot = lax.rem(step, SLOTS)
        return (pltpu.make_async_copy(k_ref.at[rows_of(step)], k_s.at[slot], in_sem.at[0, slot]),
                pltpu.make_async_copy(v_ref.at[rows_of(step)], v_s.at[slot], in_sem.at[1, slot]))

    def write(step):
        slot = lax.rem(step, SLOTS)
        return (pltpu.make_async_copy(k_s.at[slot], ko_ref.at[rows_of(step)], out_sem.at[0, slot]),
                pltpu.make_async_copy(v_s.at[slot], vo_ref.at[rows_of(step)], out_sem.at[1, slot]))

    loads = [pltpu.make_async_copy(src, dst, load_sem.at[i])
             for i, (src, dst) in enumerate(((x_ref, x_s), (wq_ref, wq_s), (wk_ref, wk_s), (wv_ref, wv_s)))]
    for copy in loads:
        copy.start()
    for step in range(AHEAD):
        for copy in fetch(step):
            copy.start()

    lane = iota((4 * heads, LANES), 1)
    head_of = lax.rem(iota((4 * heads, LANES), 0), heads)
    far = jnp.full_like(lane, 16)
    for edge in BUCKET_EDGES:
        far = far + jnp.where(lane >= edge, 1, 0)
    bucket = jnp.where(lane < 16, lane, far)
    table = jnp.zeros((4 * heads, LANES), F32)
    for b in range(32):
        here = jnp.zeros((4 * heads, LANES), F32)
        for h in range(heads):
            here = jnp.where(head_of == h, bias_ref[h, b], here)
        table = jnp.where(bucket == b, here, table)

    for copy in loads:
        copy.wait()

    @pl.loop(0, rows_total // LANES)
    def _(g):
        rows = pl.ds(pl.multiple_of(g * LANES, LANES), LANES)
        normed = rms_norm(x_s[rows, :].astype(F32), norm_ref[...])
        q_s[rows, :] = dot(normed, wq_s[...]).astype(BF16)
        kt_s[g] = dot(normed, wk_s[...]).astype(BF16).astype(F32).T
        vt_s[g] = dot(normed, wv_s[...]).astype(BF16).astype(F32).T

    spread = jnp.where(iota((n * heads, n), 0) // heads == iota((n * heads, n), 1), 1.0, 0.0).astype(BF16)
    gather = jnp.where(iota((n, n * heads), 1) // heads == iota((n, n * heads), 0), 1.0, 0.0).astype(BF16)
    own_head = iota((n * heads, flat), 1) // head_dim == lax.rem(iota((n * heads, flat), 0), heads)
    lane_bf = iota((flat, LANES), 1).astype(F32).astype(BF16)
    quad_row = iota((4 * heads, LANES), 0)
    per = LANES // n

    @pl.loop(0, steps)
    def _(step):
        ahead = step + AHEAD

        @pl.when(ahead < steps)
        def _():
            @pl.when(ahead >= SLOTS)
            def _():
                for copy in write(ahead - SLOTS):
                    copy.wait()
            for copy in fetch(ahead):
                copy.start()

        first = pl.multiple_of(step * n, n)
        slot = lax.rem(step, SLOTS)
        group, part = step // per, lax.rem(step, per)
        shift = lax.rem(LANES - part * n, LANES)
        k_new = pltpu.roll(kt_s[group], shift, 1).astype(BF16)
        v_new = pltpu.roll(vt_s[group], shift, 1).astype(BF16)
        q_rows = jnp.where(own_head, dot(spread, q_s[pl.ds(first, n), :]), 0.0).astype(BF16)
        in_k, in_v = fetch(step)

        def update(cache, new_cols, b):
            at_pos = lane_bf == pos_ref[first + b].astype(F32).astype(BF16)
            col = jnp.broadcast_to(new_cols[:, b:b + 1], (flat, LANES))
            updated = jnp.where(at_pos, col, cache[slot, b])
            cache[slot, b] = updated
            return updated

        in_k.wait()
        for g in range(n // 4):
            lhs = q_rows[4 * heads * g:4 * heads * (g + 1), :]
            picked = None
            distance = None
            for half in range(2):
                b = 4 * g + 2 * half
                pair = jnp.concatenate([update(k_s, k_new, b), update(k_s, k_new, b + 1)], axis=1)
                both = dot(lhs, pair)
                for j in range(2):
                    mine = both[:, LANES * j:LANES * (j + 1)]
                    at = 2 * half + j
                    pos = pos_ref[first + 4 * g + at]
                    picked = mine if picked is None else jnp.where(quad_row >= heads * at, mine, picked)
                    distance = jnp.full((4 * heads, LANES), pos, jnp.int32) if distance is None else jnp.where(quad_row >= heads * at, pos, distance)
            distance = distance - iota((4 * heads, LANES), 1)
            bias = jnp.take_along_axis(table, jnp.maximum(distance, 0), axis=1)
            score_s[4 * heads * g:4 * heads * (g + 1), :] = jnp.where(distance >= 0, picked + bias, NEG_FILL)
        write(step)[0].start()

        scores = score_s[...]
        exps = jnp.exp(scores - jnp.max(scores, axis=1, keepdims=True))
        probs = exps * pl.reciprocal(jnp.sum(exps, axis=1, keepdims=True))

        in_v.wait()
        for g in range(n // 4):
            quad = probs[4 * heads * g:4 * heads * (g + 1), :]
            picked = None
            for half in range(2):
                b = 4 * g + 2 * half
                pair = jnp.concatenate([update(v_s, v_new, b), update(v_s, v_new, b + 1)], axis=1)
                low = jnp.where(quad_row // heads == 2 * half, quad, 0.0)
                high = jnp.where(quad_row // heads == 2 * half + 1, quad, 0.0)
                lhs = jnp.concatenate([low, high], axis=1).astype(BF16)
                both = dot_nt(lhs, pair)
                picked = both if half == 0 else jnp.where(iota(both.shape, 0) >= 2 * heads, both, picked)
            out_s[4 * heads * g:4 * heads * (g + 1), :] = picked
        write(step)[1].start()
        mixed_s[pl.ds(first, n), :] = dot(gather, jnp.where(own_head, out_s[...], 0.0).astype(BF16)).astype(BF16)

    mixed_copy = pltpu.make_async_copy(mixed_s, mixed_ref, mixed_sem)
    mixed_copy.start()
    for step in range(steps - SLOTS, steps):
        for copy in write(step):
            copy.wait()
    mixed_copy.wait()


def self_attention(tok_pos, bias_t, x_in, w_q, w_k, w_v, norm_self, keys, values, heads):
    rows, flat, t_len = keys.shape
    d_model = x_in.shape[1]
    n = STEP_ROWS
    smem = pl.BlockSpec(memory_space=pltpu.SMEM)
    anywhere = pl.BlockSpec(memory_space=pl.ANY)
    cache_shape = jax.ShapeDtypeStruct(keys.shape, BF16)
    return pl.pallas_call(
        functools.partial(self_kernel, heads, flat // heads),
        in_specs=[smem, smem] + [anywhere] * 4 + [pl.BlockSpec(memory_space=pltpu.VMEM)] + [anywhere] * 2,
        out_specs=[anywhere] * 3,
        out_shape=[jax.ShapeDtypeStruct((rows, flat), BF16), cache_shape, cache_shape],
        scratch_shapes=[
            pltpu.VMEM((rows, d_model), BF16),
            pltpu.VMEM((d_model, flat), BF16),
            pltpu.VMEM((d_model, flat), BF16),
            pltpu.VMEM((d_model, flat), BF16),
            pltpu.VMEM((SLOTS, n, flat, t_len), BF16),
            pltpu.VMEM((SLOTS, n, flat, t_len), BF16),
            pltpu.VMEM((rows, flat), BF16),
            pltpu.VMEM((rows, flat), BF16),
            pltpu.VMEM((rows // LANES, flat, LANES), F32),
            pltpu.VMEM((rows // LANES, flat, LANES), F32),
            pltpu.VMEM((n * heads, LANES), F32),
            pltpu.VMEM((n * heads, flat), F32),
            pltpu.SemaphoreType.DMA((4,)),
            pltpu.SemaphoreType.DMA((2, SLOTS)),
            pltpu.SemaphoreType.DMA((2, SLOTS)),
            pltpu.SemaphoreType.DMA,
        ],
        compiler_params=pltpu.CompilerParams(vmem_limit_bytes=VMEM_BYTES),
        cost_estimate=pl.CostEstimate(flops=4 * rows * flat * t_len * 16 + 6 * rows * d_model * flat, bytes_accessed=8 * rows * flat * t_len, transcendentals=rows * heads * t_len),
        name='self_attention',
    )(tok_pos, bias_t, x_in, w_q, w_k, w_v, norm_self, keys, values)


CHUNK = 128
MESH = pl.DeviceIdType.MESH


def rest_kernel(heads, n_cross_slots,
                x_ref, mixed_ref, wo_ref, wox_ref, co_ref, cox_ref, cq_ref, gate_ref, up_ref, down_ref, norm_c_ref, norm_m_ref,
                mask_ref, ck_ref, cv_ref, out_ref,
                x_s, res_s, mix_s, cmix_s, wo_s, co_s, cq_s, gate_s, up_s, gate_t, down_s, k_s, v_s, mask_s,
                qt_s, score_s, hid_s, part_s, near_s, chip_s, far_s, done_s,
                ag_send, ag_recv, w_send, w_recv, sum_send, sum_recv, load_sem, cross_sem, out_sem):
    me = lax.axis_index('tp')
    core = lax.rem(me, 2)
    mate = me + 1 - 2 * core
    over = lax.rem(me + 2, 4)
    cater = lax.rem(mate + 2, 4)
    rows_total, d_model = x_ref.shape
    flat = mixed_ref.shape[1]
    head_dim = flat // heads
    src_len = ck_ref.shape[0]
    d_ff = gate_ref.shape[0]
    chunks = rows_total // CHUNK
    half = CHUNK // 2

    def remote(src, dst, send_sem, recv_sem, to):
        return pltpu.make_async_remote_copy(src_ref=src, dst_ref=dst, send_sem=send_sem, recv_sem=recv_sem,
                                            device_id={'tp': to}, device_id_type=MESH)

    def block(buf, who, c):
        return buf.at[who, pl.ds(CHUNK * c, CHUNK), :]

    def shard(buf, who):
        return buf.at[pl.ds(pl.multiple_of(who * flat, flat), flat), :]

    loads = []

    def load(src, dst):
        copy = pltpu.make_async_copy(src, dst, load_sem.at[len(loads)])
        copy.start()
        loads.append(copy)
        return copy

    def cross_load(c):
        slot = c % n_cross_slots
        cols = pl.ds(CHUNK * c, CHUNK)
        return (pltpu.make_async_copy(ck_ref.at[:, :, cols], k_s.at[slot], cross_sem.at[0, slot]),
                pltpu.make_async_copy(cv_ref.at[:, :, cols], v_s.at[slot], cross_sem.at[1, slot]))

    def cross_start(c):
        for copy in cross_load(c):
            copy.start()

    barrier = pltpu.get_barrier_semaphore()
    for peer in (mate, over):
        pl.semaphore_signal(barrier, inc=1, device_id={'tp': peer}, device_id_type=MESH)
    pl.semaphore_wait(barrier, 2)

    sends = []

    def send(copy):
        copy.start()
        sends.append(copy)

    def gather_send(stage, src, buf, c):
        send(remote(src, block(buf, me, c), ag_send.at[stage, 0, c], ag_recv.at[stage, 0, c], over))
        send(remote(src, block(buf, me, c), ag_send.at[stage, 1, c], ag_recv.at[stage, 1, c], mate))

    def gather_relay(stage, buf, c):
        remote(block(buf, over, c), block(buf, over, c), ag_send.at[stage, 0, c], ag_recv.at[stage, 0, c], over).wait_recv()
        send(remote(block(buf, over, c), block(buf, over, c), ag_send.at[stage, 2, c], ag_recv.at[stage, 2, c], mate))

    def gather_wait(stage, buf, c):
        remote(block(buf, mate, c), block(buf, mate, c), ag_send.at[stage, 1, c], ag_recv.at[stage, 1, c], mate).wait_recv()
        remote(block(buf, cater, c), block(buf, cater, c), ag_send.at[stage, 2, c], ag_recv.at[stage, 2, c], mate).wait_recv()

    def weight_send(which, ref, ref_x, buf):
        send(remote(ref, shard(buf, me), w_send.at[which, 0], w_recv.at[which, 0], mate))
        send(remote(ref_x, shard(buf, over), w_send.at[which, 1], w_recv.at[which, 1], mate))

    def weight_wait(which, buf):
        remote(shard(buf, mate), shard(buf, mate), w_send.at[which, 0], w_recv.at[which, 0], mate).wait_recv()
        remote(shard(buf, cater), shard(buf, cater), w_send.at[which, 1], w_recv.at[which, 1], mate).wait_recv()

    for c in range(chunks):
        gather_send(0, mixed_ref.at[pl.ds(CHUNK * c, CHUNK), :], mix_s, c)
    own_mixed = load(mixed_ref, mix_s.at[me])
    own_wo = (load(wo_ref, shard(wo_s, me)), load(wox_ref, shard(wo_s, over)))
    x_load = load(x_ref, x_s)
    q_load = load(cq_ref, cq_s)
    mask_load = load(mask_ref, mask_s)
    weight_send(0, wo_ref, wox_ref, wo_s)
    gate_load = load(gate_ref, gate_s)
    up_load = load(up_ref, up_s)
    cross_start(0)

    def turn(wide, tall):
        @pl.loop(0, d_model // CHUNK)
        def _(i):
            at = pl.ds(pl.multiple_of(i * CHUNK, CHUNK), CHUNK)
            tall[at, :] = wide[:, at].T

    def project_heads(buf, weight, c, add_to):
        lhs = jnp.concatenate([buf[i, CHUNK * c:CHUNK * (c + 1), :] for i in range(4)], axis=1)
        for n in range(0, d_model, 512):
            res_s[CHUNK * c:CHUNK * (c + 1), n:n + 512] = add_to[CHUNK * c:CHUNK * (c + 1), n:n + 512].astype(F32) + dot(lhs, weight[:, n:n + 512])

    def cross_query(c):
        if c == 0:
            own_mixed.wait()
            x_load.wait()
            for copy in own_wo:
                copy.wait()
        gather_wait(0, mix_s, c)
        if c == 0:
            weight_wait(0, wo_s)
            q_load.wait()
        project_heads(mix_s, wo_s, c, x_s)
        normed = rms_norm(res_s[CHUNK * c:CHUNK * (c + 1), :], norm_c_ref[...])
        qt_s[...] = dot(normed, cq_s[...]).astype(BF16).astype(F32).T

    sub = iota((8, CHUNK), 0)
    masks = [lax.rem(sub, 2 * w) < w for w in (4, 2, 1)]

    def turned(x, w):
        return jnp.concatenate([x[w:], x[:w]], axis=0)

    def fold(parts):
        for w, mask in zip((4, 2, 1), masks):
            folded = []
            for j in range(w):
                a, b = parts[j], parts[j + w]
                keep = jnp.where(mask, a, b)
                give = jnp.where(mask, turned(a, w), turned(b, 8 - w))
                folded.append(keep + give)
            parts = folded
        return parts[0]

    def cross_score(c):
        slot = c % n_cross_slots
        for copy in cross_load(c):
            copy.wait()
        if c == 0:
            mask_load.wait()
        step = 8

        @pl.loop(0, src_len // step)
        def _(i):
            at = pl.ds(pl.multiple_of(i * step, step), step)
            for h in range(heads):
                d = slice(head_dim * h, head_dim * (h + 1))
                parts = []
                for j in range(step):
                    prod = k_s[slot, i * step + j, d, :].astype(F32) * qt_s[d, :]
                    parts.append(jnp.sum(prod.reshape(head_dim // 8, 8, CHUNK), axis=0))
                score_s[h, at, :] = fold(parts)

    def cross_mix(c):
        slot = c % n_cross_slots
        step = 8
        valid = mask_s[:, CHUNK * c:CHUNK * (c + 1)] != 0
        for h in range(heads):
            scores = jnp.where(valid, score_s[h], NEG_FILL)
            exps = jnp.exp(scores - jnp.max(scores, axis=0, keepdims=True))
            probs = exps * pl.reciprocal(jnp.sum(exps, axis=0, keepdims=True))
            score_s[h] = probs.astype(BF16).astype(F32)

        def mix(i, acc):
            acc = list(acc)
            for j in range(step):
                s = i * step + j
                for h in range(heads):
                    d = slice(head_dim * h, head_dim * (h + 1))
                    acc[h] = acc[h] + v_s[slot, s, d, :].astype(F32) * score_s[h, pl.ds(s, 1), :]
            return tuple(acc)

        zero = jnp.zeros((head_dim, CHUNK), F32)
        acc = lax.fori_loop(0, src_len // step, mix, (zero,) * heads)
        cmix_s[me, CHUNK * c:CHUNK * (c + 1), :] = jnp.concatenate(acc, axis=0).T.astype(BF16)
        gather_send(1, block(cmix_s, me, c), cmix_s, c)

    def mlp(c):
        if c == 0:
            for copy in own_co:
                copy.wait()
            weight_wait(1, co_s)
        gather_wait(1, cmix_s, c)
        project_heads(cmix_s, co_s, c, res_s)
        if c == 0:
            up_load.wait()
            down_load.wait()
        normed = rms_norm(res_s[CHUNK * c:CHUNK * (c + 1), :], norm_m_ref[...])
        for n in range(0, d_ff, 256):
            end = min(d_ff, n + 256)
            gate = dot(normed, gate_t[:, n:end])
            up = dot_nt(normed, up_s[n:end, :])
            hid_s[:, n:end] = (jax.nn.gelu(gate, approximate=True) * up).astype(BF16)
        hidden = hid_s[...]
        for n in range(0, d_model, 512):
            part_s[c, :, n:n + 512] = dot(hidden, down_s[:, n:n + 512]).astype(BF16)
        give = pl.ds(pl.multiple_of((1 - core) * half, half), half)
        send(remote(part_s.at[c, give, :], near_s.at[c], sum_send.at[0, c], sum_recv.at[0, c], mate))

    pieces = [(c, 0, half) for c in range(chunks - 1)] + [(chunks - 1, 0, half // 2), (chunks - 1, half // 2, half // 2)]

    def chip_sum(p):
        c, at, size = pieces[p]
        if at == 0:
            remote(near_s.at[c], near_s.at[c], sum_send.at[0, c], sum_recv.at[0, c], mate).wait_recv()
        keep = pl.ds(pl.multiple_of(core * half + at, size), size)
        piece = pl.ds(at, size)
        chip_s[c, piece, :] = (part_s[c, keep, :].astype(F32) + near_s[c, piece, :].astype(F32)).astype(BF16)
        send(remote(chip_s.at[c, piece, :], far_s.at[c, piece, :], sum_send.at[1, p], sum_recv.at[1, p], over))

    def full_sum(p):
        c, at, size = pieces[p]
        piece = pl.ds(at, size)
        remote(far_s.at[c, piece, :], far_s.at[c, piece, :], sum_send.at[1, p], sum_recv.at[1, p], over).wait_recv()
        mine = pl.ds(pl.multiple_of(CHUNK * c + core * half + at, size), size)
        done_s[mine, :] = (res_s[mine, :] + (chip_s[c, piece, :].astype(F32) + far_s[c, piece, :].astype(F32))).astype(BF16)
        send(remote(done_s.at[mine, :], done_s.at[mine, :], sum_send.at[2, p], sum_recv.at[2, p], mate))
        copy = pltpu.make_async_copy(done_s.at[mine, :], out_ref.at[mine, :], out_sem.at[0, p])
        copy.start()
        stores.append(copy)

    def store(p):
        c, at, size = pieces[p]
        other = pl.ds(pl.multiple_of(CHUNK * c + (1 - core) * half + at, size), size)
        remote(done_s.at[other, :], done_s.at[other, :], sum_send.at[2, p], sum_recv.at[2, p], mate).wait_recv()
        copy = pltpu.make_async_copy(done_s.at[other, :], out_ref.at[other, :], out_sem.at[1, p])
        copy.start()
        stores.append(copy)

    stores = []
    gate_load.wait()
    turn(gate_s, gate_t)
    gather_relay(0, mix_s, 0)
    cross_query(0)
    for c in range(1, chunks):
        gather_relay(0, mix_s, c)
    cross_start(1)
    cross_score(0)
    cross_mix(0)
    weight_send(1, co_ref, cox_ref, co_s)
    own_co = (load(co_ref, shard(co_s, me)), load(cox_ref, shard(co_s, over)))
    cross_start(2)
    cross_query(1)
    cross_score(1)
    cross_mix(1)
    down_load = load(down_ref, down_s)
    cross_start(3)
    cross_query(2)
    gather_relay(1, cmix_s, 0)
    cross_score(2)
    mlp(0)
    gather_relay(1, cmix_s, 1)
    cross_mix(2)
    chip_sum(0)
    cross_query(3)
    cross_score(3)
    cross_mix(3)
    mlp(1)
    gather_relay(1, cmix_s, 2)
    chip_sum(1)
    mlp(2)
    gather_relay(1, cmix_s, 3)
    full_sum(0)
    chip_sum(2)
    mlp(3)
    store(0)
    full_sum(1)
    chip_sum(3)
    chip_sum(4)
    store(1)
    full_sum(2)
    store(2)
    full_sum(3)
    store(3)
    full_sum(4)
    store(4)
    for copy in stores:
        copy.wait()
    for copy in sends:
        copy.wait_send()


def rest_of_layer(x_in, mixed, w_o, w_o_over, cross_o, cross_o_over, cross_q, gate_t, up_t, w_down, norm_cross, norm_mlp, mask_t, cross_k, cross_v, heads):
    rows, d_model = x_in.shape
    flat = mixed.shape[1]
    d_ff = gate_t.shape[0]
    src_len = cross_k.shape[0]
    chunks = rows // CHUNK
    slots = 2
    anywhere = pl.BlockSpec(memory_space=pl.ANY)
    vmem = pl.BlockSpec(memory_space=pltpu.VMEM)
    dma = pltpu.SemaphoreType.DMA
    return pl.pallas_call(
        functools.partial(rest_kernel, heads, slots),
        in_specs=[anywhere] * 10 + [vmem, vmem] + [anywhere] * 3,
        out_specs=anywhere,
        out_shape=jax.ShapeDtypeStruct((rows, d_model), BF16),
        scratch_shapes=[
            pltpu.VMEM((rows, d_model), BF16),
            pltpu.VMEM((rows, d_model), F32),
            pltpu.VMEM((4, rows, flat), BF16),
            pltpu.VMEM((4, rows, flat), BF16),
            pltpu.VMEM((4 * flat, d_model), BF16),
            pltpu.VMEM((4 * flat, d_model), BF16),
            pltpu.VMEM((d_model, flat), BF16),
            pltpu.VMEM((d_ff, d_model), BF16),
            pltpu.VMEM((d_ff, d_model), BF16),
            pltpu.VMEM((d_model, d_ff), BF16),
            pltpu.VMEM((d_ff, d_model), BF16),
            pltpu.VMEM((slots, src_len, flat, CHUNK), BF16),
            pltpu.VMEM((slots, src_len, flat, CHUNK), BF16),
            pltpu.VMEM((src_len, rows), jnp.int32),
            pltpu.VMEM((flat, CHUNK), F32),
            pltpu.VMEM((heads, src_len, CHUNK), F32),
            pltpu.VMEM((CHUNK, d_ff), BF16),
            pltpu.VMEM((chunks, CHUNK, d_model), BF16),
            pltpu.VMEM((chunks, CHUNK // 2, d_model), BF16),
            pltpu.VMEM((chunks, CHUNK // 2, d_model), BF16),
            pltpu.VMEM((chunks, CHUNK // 2, d_model), BF16),
            pltpu.VMEM((rows, d_model), BF16),
            dma((2, 3, chunks)), dma((2, 3, chunks)),
            dma((2, 2)), dma((2, 2)),
            dma((3, chunks + 1)), dma((3, chunks + 1)),
            dma((16,)), dma((2, slots)), dma((2, chunks + 1)),
        ],
        compiler_params=pltpu.CompilerParams(collective_id=0, has_side_effects=True, vmem_limit_bytes=VMEM_BYTES),
        cost_estimate=pl.CostEstimate(flops=2 * rows * d_model * (8 * flat + flat + 3 * d_ff), bytes_accessed=50_000_000, transcendentals=rows * d_ff),
        name='rest_of_layer',
    )(x_in, mixed, w_o, w_o_over, cross_o, cross_o_over, cross_q, gate_t, up_t, w_down, norm_cross, norm_mlp, mask_t, cross_k, cross_v)


HAND_PIECES = 4


def hand_out(x_out):
    rows = x_out.shape[0] // HAND_PIECES

    def kernel(x_ref, out_ref, held, in_sem, out_sem):
        part = [pl.ds(rows * i, rows) for i in range(HAND_PIECES)]
        ins = [pltpu.make_async_copy(x_ref.at[p], held.at[p], in_sem.at[i]) for i, p in enumerate(part)]
        outs = [pltpu.make_async_copy(held.at[p], out_ref.at[p], out_sem.at[i]) for i, p in enumerate(part)]
        for copy in ins:
            copy.start()
        for arrived, copy in zip(ins, outs):
            arrived.wait()
            copy.start()
        for copy in outs:
            copy.wait()

    return pl.pallas_call(
        kernel,
        in_specs=[pl.BlockSpec(memory_space=pl.ANY)],
        out_specs=pl.BlockSpec(memory_space=pl.ANY),
        out_shape=jax.ShapeDtypeStruct(x_out.shape, x_out.dtype),
        scratch_shapes=[pltpu.VMEM(x_out.shape, x_out.dtype), pltpu.SemaphoreType.DMA((HAND_PIECES,)), pltpu.SemaphoreType.DMA((HAND_PIECES,))],
        compiler_params=pltpu.CompilerParams(vmem_limit_bytes=VMEM_BYTES),
        name='hand_out',
    )(x_out)


def solution(mesh):
    def local_layer(x_in, tok_pos, self_k, self_v, cross_k, cross_v, enc_mask, rel_bias, w_q, w_k, w_v, w_o, cross_q, cross_o, w_gate, w_up, w_down, norm_self, norm_cross, norm_mlp):
        rows, t_len, heads, head_dim = self_k.shape
        flat = heads * head_dim
        to_kernel = lambda c: jnp.transpose(c, (0, 2, 3, 1)).reshape(rows, flat, t_len)
        from_kernel = lambda c: jnp.transpose(c.reshape(rows, heads, head_dim, t_len), (0, 3, 1, 2))
        cross_view = lambda c: jnp.transpose(c, (1, 2, 3, 0)).reshape(c.shape[1], flat, rows)
        swap = [(0, 2), (1, 3), (2, 0), (3, 1)]
        w_o_over = lax.ppermute(w_o, 'tp', swap)
        cross_o_over = lax.ppermute(cross_o, 'tp', swap)
        mixed_self, new_k, new_v = self_attention(tok_pos, rel_bias.T, x_in, w_q, w_k, w_v, norm_self, to_kernel(self_k), to_kernel(self_v), heads)
        x_out = rest_of_layer(x_in, mixed_self, w_o, w_o_over, cross_o, cross_o_over, cross_q, w_gate.T, w_up.T, w_down, norm_cross, norm_mlp,
                              enc_mask.T, cross_view(cross_k), cross_view(cross_v), heads)
        return hand_out(x_out), from_kernel(new_k), from_kernel(new_v)

    cache_spec = P('dp', None, 'tp', None)
    split_cols = P(None, 'tp')
    split_rows = P('tp', None)
    in_specs = (P('dp', None), P('dp'), cache_spec, cache_spec, cache_spec, cache_spec, P('dp', None), split_cols, split_cols, split_cols, split_cols, split_rows, split_cols, split_rows, split_cols, split_cols, split_rows, P(None), P(None), P(None))
    out_specs = (P('dp', None), cache_spec, cache_spec)
    return jax.shard_map(local_layer, mesh=mesh, in_specs=in_specs, out_specs=out_specs, check_vma=False)
```
